32 devices in a mesh: frame: 4 (over z), space: 8 (over y, x, core).
Axes of the slice: x: 2, y: 2, z: 4, core: 2. Of those that a mesh axis runs over, the one named last changes fastest.
Arguments:
- tokens: bfloat16 [32, 152, 1024], P('space', 'frame'), may hold values from -16 to 16
- tube_count: int32 [8], P('space'), may hold values from 1 to 4, as said below
- ln_gain: float32 [1024], replicated, may hold values from 0.25 to 1.75
- ln_bias: float32 [1024], replicated, may hold values from -3 to 3
- w_qkv: bfloat16 [1024, 1536], replicated, may hold values from -1.5 to 1.5
- w_out: bfloat16 [512, 1024], replicated, may hold values from -0.25 to 0.25
Outputs:
- mixed: bfloat16 [32, 152, 1024], P('space', 'frame')
The draws below stay inside these ranges and needn't reach their ends.
Inputs may be any that keep to these rules, and one draw needn't show every extreme that they name: tube_count[s] is how many of the 4 slots of space index s hold visible tubes; they are the first ones. Some index has all 4, some only 1.
All inputs are finite; a program needn't handle non-finite values.
Results may differ from the reference program's by a relative error of at most 0.005.
Values may be sent and summed in bfloat16 or wider, within the bound.
No kernel may reach another device: no remote copies, remote signals or barrier semaphores. Data moves between devices by JAX's collectives and lax.ppermute only.
A program may use at most 128 MiB of HBM per device.

```python
import math
import jax
import jax.numpy as jnp
from jax import lax

D = 1024
HEADS = 8
HD = 64
VIS = 4
TIME = 152
SLOTS = 32
N_SPACE = 8


def draw_tokens(key, part):
    noise_key = jax.random.fold_in(jax.random.fold_in(key, 11), 0)
    drawn = jax.random.normal(noise_key, (SLOTS, TIME, D), jnp.float32)
    return jnp.clip(drawn, -16.0, 16.0).astype(jnp.bfloat16)


def draw_w_qkv(key, part):
    first_key = jax.random.fold_in(jax.random.fold_in(key, 23), 0)
    drawn = jax.random.normal(first_key, (D, 3 * HEADS * HD), jnp.float32) / math.sqrt(D)
    return jnp.clip(drawn, -1.5, 1.5).astype(jnp.bfloat16)


def draw_tube_count(key, part):
    first_key, second_key, third_key, fourth_key = jax.random.split(jax.random.fold_in(key, 37), 4)
    many = jax.random.randint(first_key, (N_SPACE,), 2, VIS + 1)
    chosen = jax.random.randint(second_key, (N_SPACE,), 0, 3) == 0
    counts = jnp.where(chosen, many, 1)
    full_at = jax.random.randint(third_key, (), 0, N_SPACE)
    step_by = jax.random.randint(fourth_key, (), 1, N_SPACE)
    sparse_at = (full_at + step_by) % N_SPACE
    index = jnp.arange(N_SPACE)
    counts = jnp.where(index == full_at, VIS, counts)
    counts = jnp.where(index == sparse_at, 1, counts)
    return counts.astype(jnp.int32)


def bell_draw(stream_key, dims, deviation, bound, held_as=jnp.bfloat16):
    values = deviation * jax.random.normal(stream_key, dims, jnp.float32)
    return jnp.clip(values, min=-bound, max=bound).astype(held_as)


def setup_inputs(seed: int = 0) -> dict:
    splits = jax.random.split(jax.random.key(seed), 7)
    return {
        "tokens": draw_tokens(jax.random.fold_in(splits[6], 71), 0),
        "tube_count": draw_tube_count(jax.random.fold_in(splits[6], 71), 0),
        "ln_gain": jnp.clip(1.0 + 0.15 * jax.random.normal(splits[2], (D,), jnp.float32), 0.25, 1.75),
        "ln_bias": bell_draw(splits[3], (D,), 0.5, 3.0, jnp.float32),
        "w_qkv": draw_w_qkv(jax.random.fold_in(splits[6], 71), 0),
        "w_out": bell_draw(splits[5], (HEADS * HD, D), (HEADS * HD) ** -0.5, 0.25),
    }


EPSILON = 1e-06

def layer_norm(flat, ln_gain, ln_bias):
    values32 = flat.astype(jnp.float32)
    center = values32 - lax.optimization_barrier(jnp.mean(values32, axis=-1, keepdims=True))
    spread = lax.optimization_barrier(jnp.mean(center * center, axis=-1, keepdims=True))
    return (center * lax.rsqrt(spread + EPSILON) * ln_gain + ln_bias).astype(jnp.bfloat16)

def reference(tokens, tube_count, ln_gain, ln_bias, w_qkv, w_out):
    slot_total, time_total, width = tokens.shape
    inner = HEADS * HD
    flat = tokens.reshape(slot_total * time_total, width)
    normed = layer_norm(flat, ln_gain, ln_bias)
    projected = jnp.dot(normed, w_qkv, preferred_element_type=jnp.float32).astype(jnp.bfloat16)
    query_all = projected[:, :inner].astype(jnp.float32).reshape(slot_total, time_total, HEADS, HD)
    key_heads = projected[:, inner:2 * inner].astype(jnp.float32).reshape(-1, HEADS, HD)
    value_heads = projected[:, 2 * inner:].astype(jnp.float32).reshape(-1, HEADS, HD)
    slot_index = jnp.arange(slot_total)
    owner = jnp.arange(N_SPACE)
    slot_count = lax.optimization_barrier(jnp.sum(jnp.where(owner[None, :] == (slot_index // VIS)[:, None], tube_count[None, :], 0), axis=1))
    live_slot = (slot_index % VIS < slot_count).astype(jnp.int32)
    live_int = jnp.broadcast_to(live_slot[:, None], (slot_total, time_total)).reshape(-1)
    live_flat = live_int == 1
    scaling = HD ** (-0.5)

    def one_block(query_block):
        scores = jnp.einsum('qhd,khd->hqk', query_block, key_heads) * scaling
        scores = jnp.where(live_flat[None, None, :], scores, -1e+30)
        highest = lax.optimization_barrier(jnp.max(scores, axis=-1, keepdims=True))
        expw = jnp.exp(scores - highest)
        rounded = lax.optimization_barrier(expw.astype(jnp.bfloat16)).astype(jnp.float32)
        summed = jnp.einsum('hqk,khd->hqd', rounded, value_heads)
        result = summed / lax.optimization_barrier(jnp.sum(expw, axis=-1))[..., None]
        return jnp.transpose(result, (1, 0, 2)).reshape(time_total, inner).astype(jnp.bfloat16)
    attended = lax.map(one_block, query_all).reshape(-1, inner)
    mixed = flat.astype(jnp.float32) + jnp.dot(attended, w_out, preferred_element_type=jnp.float32)
    mixed = jnp.where(live_flat[:, None], mixed, 0.0)
    return mixed.astype(jnp.bfloat16).reshape(slot_total, time_total, width)
```

```python
import functools
import jax
import jax.numpy as jnp
from jax import lax
from jax.experimental import pallas as pl
from jax.experimental.pallas import tpu as pltpu
from jax.sharding import PartitionSpec as P

HEADS = 8


EPSILON = 1e-06
NEG_FILL = -1e30
LANES = 128
SUBLANES = 8
PACK = 16
QUERY_TILE = 128


def up_to(value, unit):
    return -(-value // unit) * unit


def live_rows(count, rows, slot_rows, time_dev, width):
    row = lax.broadcasted_iota(jnp.int32, (rows, width), 0)
    slot = row * 0
    for edge in range(slot_rows, rows, slot_rows):
        slot = slot + (row >= edge).astype(jnp.int32)
    return (slot < count) & (row - slot * slot_rows < time_dev)


def project_kernel(count_ref, x_ref, gain_ref, bias_ref, wq_ref, wk_ref, wv_ref, out_ref, normed_ref):
    slots, time_dev, width = x_ref.shape
    rows = normed_ref.shape[0]
    slot_rows = rows // slots
    half = rows // 2
    heads_step = out_ref.shape[0]
    head_size = LANES // 2
    scaling = head_size ** (-0.5)
    count = count_ref[0]

    @pl.when(pl.program_id(0) == 0)
    def _():
        for slot in range(slots):
            x = x_ref[slot].astype(jnp.float32)
            center = x - jnp.mean(x, axis=-1, keepdims=True)
            spread = jnp.mean(center * center, axis=-1, keepdims=True)
            normed = center * lax.rsqrt(spread + EPSILON) * gain_ref[...] + bias_ref[...]
            start = slot * slot_rows
            normed_ref[start : start + time_dev] = normed
            if slot_rows > time_dev:
                normed_ref[start + time_dev : start + slot_rows] = jnp.zeros(
                    (slot_rows - time_dev, width), jnp.float32
                )

    rows_in = normed_ref[...].astype(jnp.bfloat16)
    query = jnp.dot(rows_in, wq_ref[...], preferred_element_type=jnp.float32) * scaling
    key = jnp.dot(rows_in, wk_ref[...], preferred_element_type=jnp.float32)
    value = jnp.dot(rows_in, wv_ref[...], preferred_element_type=jnp.float32)
    live = live_rows(count, rows, slot_rows, time_dev, LANES)
    lane = lax.broadcasted_iota(jnp.int32, (rows, LANES), 1)
    left = lane < head_size
    left_half = left[:half]
    row_half = lax.broadcasted_iota(jnp.int32, (half, LANES), 0)
    mark = (row_half == half - 1) & jnp.logical_not(left_half)
    count_value = count.astype(jnp.float32)
    for pair in range(heads_step // 2):
        cols = slice(pair * LANES, (pair + 1) * LANES)
        key_pair = key[:, cols]
        key_pair = jnp.where(live, key_pair, key_pair[0:1])
        value_pair = jnp.where(live, value[:, cols], 0.0)
        even = jnp.where(left, key_pair, pltpu.roll(value_pair, head_size, 1))
        odd = jnp.where(left, pltpu.roll(key_pair, head_size, 1), value_pair)
        out_ref[2 * pair, 0:rows] = even.astype(jnp.bfloat16)
        out_ref[2 * pair + 1, 0:rows] = odd.astype(jnp.bfloat16)
        top = query[:half, cols]
        low = query[half:, cols]
        even = jnp.where(left_half, top, pltpu.roll(low, head_size, 1))
        odd = jnp.where(left_half, pltpu.roll(top, head_size, 1), low)
        even = jnp.where(mark, count_value, even)
        odd = jnp.where(mark, count_value, odd)
        out_ref[2 * pair, rows : rows + half] = even.astype(jnp.bfloat16)
        out_ref[2 * pair + 1, rows : rows + half] = odd.astype(jnp.bfloat16)


def project(count, tokens, ln_gain, ln_bias, w_qkv, rows):
    slots, time_dev, width = tokens.shape
    steps = 2
    heads_step = HEADS // steps
    cols = heads_step * LANES // 2
    whole = lambda step: (0, 0)
    return pl.pallas_call(
        project_kernel,
        grid=(steps,),
        out_shape=jax.ShapeDtypeStruct((HEADS, rows + rows // 2, LANES), jnp.bfloat16),
        in_specs=[
            pl.BlockSpec(memory_space=pltpu.SMEM),
            pl.BlockSpec(tokens.shape, lambda step: (0, 0, 0)),
            pl.BlockSpec((1, width), whole),
            pl.BlockSpec((1, width), whole),
            pl.BlockSpec((width, cols), lambda step: (0, step)),
            pl.BlockSpec((width, cols), lambda step: (0, steps + step)),
            pl.BlockSpec((width, cols), lambda step: (0, 2 * steps + step)),
        ],
        out_specs=pl.BlockSpec((heads_step, rows + rows // 2, LANES), lambda step: (step, 0, 0)),
        scratch_shapes=[pltpu.VMEM((rows, width), jnp.float32)],
        cost_estimate=pl.CostEstimate(
            flops=2 * rows * w_qkv.size, bytes_accessed=2 * w_qkv.size, transcendentals=0
        ),
        name="project",
    )(count, tokens, ln_gain.reshape(1, width), ln_bias.reshape(1, width), w_qkv, w_qkv, w_qkv)


def pack_kernel(slot_rows, time_dev, got_ref, kv_ref, query_ref, live_ref, start_ref):
    sources, message, lanes = got_ref.shape
    rows = message * 2 // 3
    half = rows // 2
    head_size = lanes // 2
    size = kv_ref.shape[0] - rows
    lane = lax.broadcasted_iota(jnp.int32, (PACK, lanes), 1)
    first = got_ref[0, 0:PACK].astype(jnp.float32)[0:1]
    fill = jnp.where(lane < head_size, jnp.broadcast_to(first, (PACK, lanes)), 0.0)
    fill = fill.astype(jnp.bfloat16)
    blank = jnp.zeros((PACK, lanes), jnp.bfloat16)
    for start in range(0, size + rows, PACK):
        kv_ref[start : start + PACK] = fill
        live_ref[start : start + PACK] = blank
        query_ref[start : start + PACK] = blank
    left = lax.broadcasted_iota(jnp.int32, (half, lanes), 1) < head_size
    start = jnp.int32(0)
    for source in range(sources):
        tail = got_ref[source, message - PACK : message].astype(jnp.float32)
        count = jnp.max(tail[PACK - 1 : PACK, head_size:]).astype(jnp.int32)
        start_ref[source] = start
        place = pl.multiple_of(start, PACK)
        kv_ref[pl.ds(place, rows)] = got_ref[source, 0:rows]
        live = live_rows(count, rows, slot_rows, time_dev, lanes)
        live_ref[pl.ds(place, rows)] = live.astype(jnp.float32).astype(jnp.bfloat16)
        pair = got_ref[source, rows:message].astype(jnp.float32)
        query_ref[pl.ds(place, half)] = jnp.where(left, pair, 0.0).astype(jnp.bfloat16)
        query_ref[pl.ds(pl.multiple_of(start + half, PACK), half)] = jnp.where(
            left, pltpu.roll(pair, head_size, 1), 0.0
        ).astype(jnp.bfloat16)
        used = count * slot_rows
        start = start + (used + PACK - 1) // PACK * PACK


def pack(got, size, slot_rows, time_dev):
    sources, message, lanes = got.shape
    rows = message * 2 // 3
    room = jax.ShapeDtypeStruct((size + rows, lanes), jnp.bfloat16)
    return pl.pallas_call(
        functools.partial(pack_kernel, slot_rows, time_dev),
        out_shape=(room, room, room, jax.ShapeDtypeStruct((sources,), jnp.int32)),
        in_specs=[pl.BlockSpec(memory_space=pltpu.VMEM)],
        out_specs=(
            pl.BlockSpec(memory_space=pltpu.VMEM),
            pl.BlockSpec(memory_space=pltpu.VMEM),
            pl.BlockSpec(memory_space=pltpu.VMEM),
            pl.BlockSpec(memory_space=pltpu.SMEM),
        ),
        name="pack",
    )(got)


def weigh(query, live, blocks, size, left):
    scores = [
        lax.dot_general(
            query, block[0:size], (((1,), (1,)), ((), ())), preferred_element_type=jnp.float32
        )
        for block in blocks
    ]
    best = functools.reduce(jnp.maximum, [jnp.max(s, axis=-1, keepdims=True) for s in scores])
    return scores, best


def own_kernel(size, query_ref, kv_ref, live_ref, best_ref, sum_ref):
    lanes = kv_ref.shape[1]
    left = lax.broadcasted_iota(jnp.int32, (size, lanes), 1) < lanes // 2

    def step(index, carry):
        place = pl.ds(pl.multiple_of(index * QUERY_TILE, QUERY_TILE), QUERY_TILE)
        scores = lax.dot_general(
            query_ref[place],
            kv_ref[0:size],
            (((1,), (1,)), ((), ())),
            preferred_element_type=jnp.float32,
        )
        best = jnp.max(scores, axis=-1, keepdims=True)
        weights = jnp.exp(scores - best).astype(jnp.bfloat16)
        side = jnp.where(left, live_ref[0:size], kv_ref[0:size])
        sum_ref[place] = jnp.dot(weights, side, preferred_element_type=jnp.float32)
        best_ref[place] = jnp.broadcast_to(best, (QUERY_TILE, lanes))
        return carry

    lax.fori_loop(0, size // QUERY_TILE, step, 0)


def rest_kernel(size, others, *refs):
    start_ref, query_ref, live_ref, best_ref, sum_ref = refs[:5]
    kv_refs = refs[5 : 5 + others]
    out_ref, held_ref = refs[5 + others :]
    sources, half, lanes = out_ref.shape
    head_size = lanes // 2
    left = lax.broadcasted_iota(jnp.int32, (size, lanes), 1) < head_size

    def step(index, carry):
        place = pl.ds(pl.multiple_of(index * QUERY_TILE, QUERY_TILE), QUERY_TILE)
        query = query_ref[place]
        before = best_ref[place][:, 0:1]
        scores = [
            lax.dot_general(
                query,
                kv_ref[0:size],
                (((1,), (1,)), ((), ())),
                preferred_element_type=jnp.float32,
            )
            for kv_ref in kv_refs
        ]
        best = before
        for part in scores:
            best = jnp.maximum(best, jnp.max(part, axis=-1, keepdims=True))
        total = sum_ref[place] * jnp.exp(before - best)
        for part, kv_ref in zip(scores, kv_refs):
            weights = jnp.exp(part - best).astype(jnp.bfloat16)
            side = jnp.where(left, live_ref[0:size], kv_ref[0:size])
            total = total + jnp.dot(weights, side, preferred_element_type=jnp.float32)
        held_ref[place] = total / pltpu.roll(total, head_size, 1)
        return carry

    lax.fori_loop(0, size // QUERY_TILE, step, 0)
    left_half = lax.broadcasted_iota(jnp.int32, (half, lanes), 1) < head_size
    for source in range(sources):
        start = start_ref[source]
        top = held_ref[pl.ds(pl.multiple_of(start, PACK), half)]
        low = held_ref[pl.ds(pl.multiple_of(start + half, PACK), half)]
        out_ref[source] = jnp.where(left_half, pltpu.roll(top, head_size, 1), low).astype(
            jnp.bfloat16
        )


def attend_size(size, slot_rows, time_dev, got):
    sources, message, lanes = got.shape
    rows = message * 2 // 3
    frames = lax.axis_size("frame")
    kv, query, live, starts = pack(got, size, slot_rows, time_dev)
    sent = kv[0:size]
    others = [
        lax.ppermute(sent, "frame", [(i, (i + hop) % frames) for i in range(frames)])
        for hop in range(1, frames)
    ]
    vmem = pl.BlockSpec(memory_space=pltpu.VMEM)
    state = jax.ShapeDtypeStruct((size, lanes), jnp.float32)
    cost = lambda n: pl.CostEstimate(
        flops=4 * n * size * size * lanes, bytes_accessed=size * lanes * 8, transcendentals=0
    )
    best, total = pl.pallas_call(
        functools.partial(own_kernel, size),
        out_shape=(state, state),
        in_specs=[vmem] * 3,
        out_specs=(vmem, vmem),
        cost_estimate=cost(1),
        name="attend_own",
    )(query, sent, live)
    return pl.pallas_call(
        functools.partial(rest_kernel, size, len(others)),
        out_shape=jax.ShapeDtypeStruct((sources, rows // 2, lanes), jnp.bfloat16),
        in_specs=[pl.BlockSpec(memory_space=pltpu.SMEM)] + [vmem] * (4 + len(others)),
        out_specs=vmem,
        scratch_shapes=[pltpu.VMEM((size + rows, lanes), jnp.float32)],
        cost_estimate=cost(len(others)),
        name="attend_rest",
    )(starts, query, live, best, total, *others)


def mix_kernel(count_ref, got_ref, x_ref, w_ref, out_ref):
    heads, half, lanes = got_ref.shape
    slots, time_dev, width = x_ref.shape
    slot_rows = 2 * half // slots
    head_size = lanes // 2
    left = lax.broadcasted_iota(jnp.int32, (half, lanes), 1) < head_size
    tops = []
    lows = []
    for pair in range(heads // 2):
        even = got_ref[2 * pair].astype(jnp.float32)
        odd = got_ref[2 * pair + 1].astype(jnp.float32)
        tops.append(jnp.where(left, even, pltpu.roll(odd, head_size, 1)))
        lows.append(jnp.where(left, pltpu.roll(even, head_size, 1), odd))
    top = jnp.concatenate(tops, axis=1)
    low = jnp.concatenate(lows, axis=1)
    attended = jnp.concatenate([top, low], axis=0).astype(jnp.bfloat16)
    mixed = jnp.dot(attended, w_ref[...], preferred_element_type=jnp.float32)
    for slot in range(slots):
        start = slot * slot_rows
        full = x_ref[slot].astype(jnp.float32) + mixed[start : start + time_dev]
        out_ref[slot] = jnp.where(slot < count_ref[0], full, 0.0).astype(jnp.bfloat16)


def mix(count, got, tokens, w_out):
    vmem = pl.BlockSpec(memory_space=pltpu.VMEM)
    return pl.pallas_call(
        mix_kernel,
        out_shape=jax.ShapeDtypeStruct(tokens.shape, jnp.bfloat16),
        in_specs=[pl.BlockSpec(memory_space=pltpu.SMEM), vmem, vmem, vmem],
        out_specs=vmem,
        cost_estimate=pl.CostEstimate(
            flops=4 * got.shape[1] * w_out.size, bytes_accessed=2 * w_out.size, transcendentals=0
        ),
        name="mix",
    )(count, got, tokens, w_out)


def head_per_device(tokens, tube_count, ln_gain, ln_bias, w_qkv, w_out):
    slots, time_dev, width = tokens.shape
    slot_rows = up_to(time_dev, SUBLANES)
    rows = slots * slot_rows
    messages = project(tube_count, tokens, ln_gain, ln_bias, w_qkv, rows)
    got = lax.all_to_all(messages, "space", 0, 0, tiled=True)
    most = up_to((HEADS - 1) * rows + up_to(slot_rows, PACK), QUERY_TILE)
    returned = attend_size(most, slot_rows, time_dev, got)
    back = lax.all_to_all(returned, "space", 0, 0, tiled=True)
    return mix(tube_count, back, tokens, w_out)


def layer_norm(flat, ln_gain, ln_bias):
    values32 = flat.astype(jnp.float32)
    center = values32 - jnp.mean(values32, axis=-1, keepdims=True)
    spread = jnp.mean(center * center, axis=-1, keepdims=True)
    return (center * lax.rsqrt(spread + EPSILON) * ln_gain + ln_bias).astype(jnp.bfloat16)


def live_mask(counts, slots_dev, time_dev):
    slot_ids = jnp.arange(slots_dev)[None, :, None]
    marks = jnp.broadcast_to(
        slot_ids < counts[:, None, None], (counts.shape[0], slots_dev, time_dev)
    )
    return marks.reshape(-1)


def attend(carry, query_heads, key_block, value_block, live_keys, scaling):
    best_now, total_now, accum = carry
    heads = query_heads.shape[1]
    key_heads = key_block.reshape(key_block.shape[0], heads, -1)
    value_heads = value_block.reshape(value_block.shape[0], heads, -1)
    scores = (
        jnp.einsum("qhd,khd->hqk", query_heads, key_heads, preferred_element_type=jnp.float32)
        * scaling
    )
    scores = jnp.where(live_keys[None, None, :], scores, NEG_FILL)
    best_next = jnp.maximum(best_now, jnp.max(scores, axis=-1))
    fading = jnp.exp(best_now - best_next)
    weights = jnp.exp(scores - best_next[..., None])
    total_next = total_now * fading + jnp.sum(weights, axis=-1)
    accum = accum * fading[..., None] + jnp.einsum(
        "hqk,khd->hqd",
        weights.astype(jnp.bfloat16),
        value_heads,
        preferred_element_type=jnp.float32,
    )
    return (best_next, total_next, accum)


def make_fold(query_heads, vis_dev, time_dev, scaling):
    rows_dev = vis_dev * time_dev

    def fold_masked(carry, piece, start):
        key_all, value_all, count_all = piece
        width_in = key_all.shape[1]
        shards = count_all.shape[0]
        group = 1
        for unused_bit in range(6):
            if shards % (group * 2) == 0 and group * rows_dev < 2048:
                group = group * 2
        blocks = shards // group
        key_groups = key_all.reshape(blocks, group * rows_dev, width_in)
        value_groups = value_all.reshape(blocks, group * rows_dev, width_in)
        count_groups = count_all.reshape(blocks, group)

        def step_group(state, item):
            key_group, value_group, count_group = item
            marks = live_mask(count_group, vis_dev, time_dev)
            return (attend(state, query_heads, key_group, value_group, marks, scaling), None)

        carry, unused = lax.scan(step_group, carry, (key_groups, value_groups, count_groups))
        return carry

    return fold_masked


def start_state(heads, rows, head_size):
    return (
        jnp.full((heads, rows), NEG_FILL, jnp.float32),
        jnp.zeros((heads, rows), jnp.float32),
        jnp.zeros((heads, rows, head_size), jnp.float32),
    )


def on_device(tokens, tube_count, ln_gain, ln_bias, w_qkv, w_out):
    vis_dev, time_dev, width = tokens.shape
    rows_dev = vis_dev * time_dev
    inner = w_out.shape[0]
    head_size = inner // HEADS
    flat = tokens.reshape(rows_dev, width)
    normed = layer_norm(flat, ln_gain, ln_bias)
    projected = jnp.dot(normed, w_qkv, preferred_element_type=jnp.float32).astype(jnp.bfloat16)
    scaling = head_size ** (-0.5)
    frames = lax.axis_size("frame")
    local_heads = HEADS // frames
    stacked = projected.reshape(rows_dev, 3, HEADS, head_size)
    regrouped = lax.all_to_all(stacked, "frame", split_axis=2, concat_axis=0, tiled=True)
    all_rows = regrouped.shape[0]
    query_local = regrouped[:, 0]
    key_local = regrouped[:, 1].reshape(all_rows, local_heads * head_size)
    value_local = regrouped[:, 2].reshape(all_rows, local_heads * head_size)
    counts_rep = jnp.tile(tube_count, frames)
    fold_fn = make_fold(query_local, vis_dev, time_dev, scaling)
    state = fold_fn(
        start_state(local_heads, all_rows, head_size),
        (
            lax.all_gather(key_local, "space", axis=0, tiled=True),
            lax.all_gather(value_local, "space", axis=0, tiled=True),
            lax.all_gather(counts_rep, "space", axis=0, tiled=True),
        ),
        jnp.int32(0),
    )
    best_final, total_final, accum_final = state
    attended = (accum_final / total_final[..., None]).astype(jnp.bfloat16)
    attended = jnp.transpose(attended, (1, 0, 2))
    returned = lax.all_to_all(attended, "frame", split_axis=0, concat_axis=1, tiled=True)
    attended = returned.reshape(rows_dev, inner)
    mixed = flat.astype(jnp.float32) + jnp.dot(attended, w_out, preferred_element_type=jnp.float32)
    own_live = live_mask(tube_count, vis_dev, time_dev)
    mixed = jnp.where(own_live[:, None], mixed, 0.0)
    return mixed.astype(jnp.bfloat16).reshape(vis_dev, time_dev, width)


def solution(mesh):
    in_specs = (P("space", "frame", None), P("space"), P(), P(), P(), P())
    out_specs = P("space", "frame", None)

    def layer(tokens, tube_count, ln_gain, ln_bias, w_qkv, w_out):
        slots = tokens.shape[0] // mesh.shape["space"]
        time_dev = tokens.shape[1] // mesh.shape["frame"]
        rows = slots * up_to(time_dev, SUBLANES)
        pairs = 2 * w_out.shape[0] == HEADS * LANES and rows % (2 * PACK) == 0
        padded = up_to(time_dev, SUBLANES) > time_dev
        fits = mesh.shape["space"] == HEADS and pairs and padded
        return jax.shard_map(
            head_per_device if fits else on_device,
            mesh=mesh,
            in_specs=in_specs,
            out_specs=out_specs,
            check_vma=False,
        )(tokens, tube_count, ln_gain, ln_bias, w_qkv, w_out)

    return layer
```

```python
import functools
import jax
import jax.numpy as jnp
from jax import lax
from jax.experimental import pallas as pl
from jax.experimental.pallas import tpu as pltpu
from jax.sharding import PartitionSpec as P

HEADS = 8


EPSILON = 1e-06
NEG_FILL = -1e30
LANES = 128
SUBLANES = 8
PACK = 16
QUERY_TILE = 128
SIZE_CASES = 5


def up_to(value, unit):
    return -(-value // unit) * unit


def packed_rows(count, slot_rows):
    return (count * slot_rows + PACK - 1) // PACK * PACK


def live_rows(count, rows, slot_rows, time_dev, width):
    row = lax.broadcasted_iota(jnp.int32, (rows, width), 0)
    slot = row * 0
    for edge in range(slot_rows, rows, slot_rows):
        slot = slot + (row >= edge).astype(jnp.int32)
    return (slot < count) & (row - slot * slot_rows < time_dev)


def project_kernel(count_ref, x_ref, gain_ref, bias_ref, wq_ref, wk_ref, wv_ref, out_ref, normed_ref):
    slots, time_dev, width = x_ref.shape
    rows = normed_ref.shape[0]
    slot_rows = rows // slots
    half = rows // 2
    heads_step = out_ref.shape[0]
    head_size = LANES // 2
    scaling = head_size ** (-0.5)
    count = count_ref[0]

    @pl.when(pl.program_id(0) == 0)
    def _():
        for slot in range(slots):
            x = x_ref[slot].astype(jnp.float32)
            center = x - jnp.mean(x, axis=-1, keepdims=True)
            spread = jnp.mean(center * center, axis=-1, keepdims=True)
            normed = center * lax.rsqrt(spread + EPSILON) * gain_ref[...] + bias_ref[...]
            start = slot * slot_rows
            normed_ref[start : start + time_dev] = normed
            if slot_rows > time_dev:
                normed_ref[start + time_dev : start + slot_rows] = jnp.zeros(
                    (slot_rows - time_dev, width), jnp.float32
                )

    rows_in = normed_ref[...].astype(jnp.bfloat16)
    query = jnp.dot(rows_in, wq_ref[...], preferred_element_type=jnp.float32) * scaling
    key = jnp.dot(rows_in, wk_ref[...], preferred_element_type=jnp.float32)
    value = jnp.dot(rows_in, wv_ref[...], preferred_element_type=jnp.float32)
    live = live_rows(count, rows, slot_rows, time_dev, LANES)
    lane = lax.broadcasted_iota(jnp.int32, (rows, LANES), 1)
    left = lane < head_size
    left_half = left[:half]
    row_half = lax.broadcasted_iota(jnp.int32, (half, LANES), 0)
    mark = (row_half == half - 1) & jnp.logical_not(left_half)
    count_value = count.astype(jnp.float32)
    for pair in range(heads_step // 2):
        cols = slice(pair * LANES, (pair + 1) * LANES)
        key_pair = key[:, cols]
        key_pair = jnp.where(live, key_pair, key_pair[0:1])
        value_pair = jnp.where(live, value[:, cols], 0.0)
        even = jnp.where(left, key_pair, pltpu.roll(value_pair, head_size, 1))
        odd = jnp.where(left, pltpu.roll(key_pair, head_size, 1), value_pair)
        out_ref[2 * pair, 0:rows] = even.astype(jnp.bfloat16)
        out_ref[2 * pair + 1, 0:rows] = odd.astype(jnp.bfloat16)
        top = query[:half, cols]
        low = query[half:, cols]
        even = jnp.where(left_half, top, pltpu.roll(low, head_size, 1))
        odd = jnp.where(left_half, pltpu.roll(top, head_size, 1), low)
        even = jnp.where(mark, count_value, even)
        odd = jnp.where(mark, count_value, odd)
        out_ref[2 * pair, rows : rows + half] = even.astype(jnp.bfloat16)
        out_ref[2 * pair + 1, rows : rows + half] = odd.astype(jnp.bfloat16)


def project(count, tokens, ln_gain, ln_bias, w_qkv, rows):
    slots, time_dev, width = tokens.shape
    steps = 2
    heads_step = HEADS // steps
    cols = heads_step * LANES // 2
    whole = lambda step: (0, 0)
    return pl.pallas_call(
        project_kernel,
        grid=(steps,),
        out_shape=jax.ShapeDtypeStruct((HEADS, rows + rows // 2, LANES), jnp.bfloat16),
        in_specs=[
            pl.BlockSpec(memory_space=pltpu.SMEM),
            pl.BlockSpec(tokens.shape, lambda step: (0, 0, 0)),
            pl.BlockSpec((1, width), whole),
            pl.BlockSpec((1, width), whole),
            pl.BlockSpec((width, cols), lambda step: (0, step)),
            pl.BlockSpec((width, cols), lambda step: (0, steps + step)),
            pl.BlockSpec((width, cols), lambda step: (0, 2 * steps + step)),
        ],
        out_specs=pl.BlockSpec((heads_step, rows + rows // 2, LANES), lambda step: (step, 0, 0)),
        scratch_shapes=[pltpu.VMEM((rows, width), jnp.float32)],
        cost_estimate=pl.CostEstimate(
            flops=2 * rows * w_qkv.size, bytes_accessed=2 * w_qkv.size, transcendentals=0
        ),
        name="project",
    )(count, tokens, ln_gain.reshape(1, width), ln_bias.reshape(1, width), w_qkv, w_qkv, w_qkv)


def pack_kernel(slot_rows, time_dev, got_ref, sent_ref, query_ref, live_ref, start_ref, kv_ref):
    sources, message, lanes = got_ref.shape
    rows = message * 2 // 3
    half = rows // 2
    head_size = lanes // 2
    size = sent_ref.shape[0]
    lane = lax.broadcasted_iota(jnp.int32, (PACK, lanes), 1)
    first = got_ref[0, 0:PACK].astype(jnp.float32)[0:1]
    fill = jnp.where(lane < head_size, jnp.broadcast_to(first, (PACK, lanes)), 0.0)
    fill = fill.astype(jnp.bfloat16)
    blank = jnp.zeros((PACK, lanes), jnp.bfloat16)
    for start in range(0, size + rows, PACK):
        kv_ref[start : start + PACK] = fill
        live_ref[start : start + PACK] = blank
        query_ref[start : start + PACK] = blank
    left = lax.broadcasted_iota(jnp.int32, (half, lanes), 1) < head_size
    start = jnp.int32(0)
    for source in range(sources):
        tail = got_ref[source, message - PACK : message].astype(jnp.float32)
        count = jnp.max(tail[PACK - 1 : PACK, head_size:]).astype(jnp.int32)
        start_ref[source] = start
        place = pl.multiple_of(start, PACK)
        kv_ref[pl.ds(place, rows)] = got_ref[source, 0:rows]
        live = live_rows(count, rows, slot_rows, time_dev, lanes)
        live_ref[pl.ds(place, rows)] = live.astype(jnp.float32).astype(jnp.bfloat16)
        pair = got_ref[source, rows:message].astype(jnp.float32)
        query_ref[pl.ds(place, half)] = jnp.where(left, pair, 0.0).astype(jnp.bfloat16)
        query_ref[pl.ds(pl.multiple_of(start + half, PACK), half)] = jnp.where(
            left, pltpu.roll(pair, head_size, 1), 0.0
        ).astype(jnp.bfloat16)
        start = start + packed_rows(count, slot_rows)
    sent_ref[...] = kv_ref[0:size]


def pack(got, size, slot_rows, time_dev):
    sources, message, lanes = got.shape
    rows = message * 2 // 3
    sent = jax.ShapeDtypeStruct((size, lanes), jnp.bfloat16)
    room = jax.ShapeDtypeStruct((size + rows, lanes), jnp.bfloat16)
    return pl.pallas_call(
        functools.partial(pack_kernel, slot_rows, time_dev),
        out_shape=(sent, room, room, jax.ShapeDtypeStruct((sources,), jnp.int32)),
        in_specs=[pl.BlockSpec(memory_space=pltpu.VMEM)],
        out_specs=(
            pl.BlockSpec(memory_space=pltpu.VMEM),
            pl.BlockSpec(memory_space=pltpu.VMEM),
            pl.BlockSpec(memory_space=pltpu.VMEM),
            pl.BlockSpec(memory_space=pltpu.SMEM),
        ),
        scratch_shapes=[pltpu.VMEM((size + rows, lanes), jnp.bfloat16)],
        name="pack",
    )(got)


def own_kernel(size, query_ref, kv_ref, live_ref, best_ref, sum_ref):
    lanes = kv_ref.shape[1]
    left = lax.broadcasted_iota(jnp.int32, (size, lanes), 1) < lanes // 2

    def step(index, carry):
        place = pl.ds(pl.multiple_of(index * QUERY_TILE, QUERY_TILE), QUERY_TILE)
        scores = lax.dot_general(
            query_ref[place],
            kv_ref[0:size],
            (((1,), (1,)), ((), ())),
            preferred_element_type=jnp.float32,
        )
        best = jnp.max(scores, axis=-1, keepdims=True)
        weights = jnp.exp(scores - best).astype(jnp.bfloat16)
        side = jnp.where(left, live_ref[0:size], kv_ref[0:size])
        sum_ref[place] = jnp.dot(weights, side, preferred_element_type=jnp.float32)
        best_ref[place] = jnp.broadcast_to(best, (QUERY_TILE, lanes))
        return carry

    lax.fori_loop(0, size // QUERY_TILE, step, 0)


def rest_kernel(size, others, *refs):
    start_ref, query_ref, live_ref, best_ref, sum_ref = refs[:5]
    kv_refs = refs[5 : 5 + others]
    out_ref, held_ref = refs[5 + others :]
    sources, half, lanes = out_ref.shape
    head_size = lanes // 2
    left = lax.broadcasted_iota(jnp.int32, (size, lanes), 1) < head_size

    def step(index, carry):
        place = pl.ds(pl.multiple_of(index * QUERY_TILE, QUERY_TILE), QUERY_TILE)
        query = query_ref[place]
        before = best_ref[place][:, 0:1]
        scores = [
            lax.dot_general(
                query,
                kv_ref[0:size],
                (((1,), (1,)), ((), ())),
                preferred_element_type=jnp.float32,
            )
            for kv_ref in kv_refs
        ]
        best = before
        for part in scores:
            best = jnp.maximum(best, jnp.max(part, axis=-1, keepdims=True))
        total = sum_ref[place] * jnp.exp(before - best)
        for part, kv_ref in zip(scores, kv_refs):
            weights = jnp.exp(part - best).astype(jnp.bfloat16)
            side = jnp.where(left, live_ref[0:size], kv_ref[0:size])
            total = total + jnp.dot(weights, side, preferred_element_type=jnp.float32)
        held_ref[place] = total / pltpu.roll(total, head_size, 1)
        return carry

    lax.fori_loop(0, size // QUERY_TILE, step, 0)
    left_half = lax.broadcasted_iota(jnp.int32, (half, lanes), 1) < head_size
    for source in range(sources):
        start = start_ref[source]
        top = held_ref[pl.ds(pl.multiple_of(start, PACK), half)]
        low = held_ref[pl.ds(pl.multiple_of(start + half, PACK), half)]
        out_ref[source] = jnp.where(left_half, pltpu.roll(top, head_size, 1), low).astype(
            jnp.bfloat16
        )


def attend_size(size, slot_rows, time_dev, got):
    sources, message, lanes = got.shape
    rows = message * 2 // 3
    frames = lax.axis_size("frame")
    sent, query, live, starts = pack(got, size, slot_rows, time_dev)
    others = [
        lax.ppermute(sent, "frame", [(i, (i + hop) % frames) for i in range(frames)])
        for hop in range(1, frames)
    ]
    vmem = pl.BlockSpec(memory_space=pltpu.VMEM)
    state = jax.ShapeDtypeStruct((size, lanes), jnp.float32)
    cost = lambda n: pl.CostEstimate(
        flops=4 * n * size * size * lanes, bytes_accessed=size * lanes * 8, transcendentals=0
    )
    best, total = pl.pallas_call(
        functools.partial(own_kernel, size),
        out_shape=(state, state),
        in_specs=[vmem] * 3,
        out_specs=(vmem, vmem),
        cost_estimate=cost(1),
        name="attend_own",
    )(query, sent, live)
    return pl.pallas_call(
        functools.partial(rest_kernel, size, len(others)),
        out_shape=jax.ShapeDtypeStruct((sources, rows // 2, lanes), jnp.bfloat16),
        in_specs=[pl.BlockSpec(memory_space=pltpu.SMEM)] + [vmem] * (4 + len(others)),
        out_specs=vmem,
        scratch_shapes=[pltpu.VMEM((size + rows, lanes), jnp.float32)],
        cost_estimate=cost(len(others)),
        name="attend_rest",
    )(starts, query, live, best, total, *others)


def mix_kernel(count_ref, got_ref, x_ref, w_ref, out_ref):
    heads, half, lanes = got_ref.shape
    slots, time_dev, width = x_ref.shape
    slot_rows = 2 * half // slots
    head_size = lanes // 2
    left = lax.broadcasted_iota(jnp.int32, (half, lanes), 1) < head_size
    tops = []
    lows = []
    for pair in range(heads // 2):
        even = got_ref[2 * pair].astype(jnp.float32)
        odd = got_ref[2 * pair + 1].astype(jnp.float32)
        tops.append(jnp.where(left, even, pltpu.roll(odd, head_size, 1)))
        lows.append(jnp.where(left, pltpu.roll(even, head_size, 1), odd))
    top = jnp.concatenate(tops, axis=1)
    low = jnp.concatenate(lows, axis=1)
    attended = jnp.concatenate([top, low], axis=0).astype(jnp.bfloat16)
    mixed = jnp.dot(attended, w_ref[...], preferred_element_type=jnp.float32)
    for slot in range(slots):
        start = slot * slot_rows
        full = x_ref[slot].astype(jnp.float32) + mixed[start : start + time_dev]
        out_ref[slot] = jnp.where(slot < count_ref[0], full, 0.0).astype(jnp.bfloat16)


def mix(count, got, tokens, w_out):
    vmem = pl.BlockSpec(memory_space=pltpu.VMEM)
    return pl.pallas_call(
        mix_kernel,
        out_shape=jax.ShapeDtypeStruct(tokens.shape, jnp.bfloat16),
        in_specs=[pl.BlockSpec(memory_space=pltpu.SMEM), vmem, vmem, vmem],
        out_specs=vmem,
        cost_estimate=pl.CostEstimate(
            flops=4 * got.shape[1] * w_out.size, bytes_accessed=2 * w_out.size, transcendentals=0
        ),
        name="mix",
    )(count, got, tokens, w_out)


def head_per_device(tokens, tube_count, ln_gain, ln_bias, w_qkv, w_out):
    slots, time_dev, width = tokens.shape
    slot_rows = up_to(time_dev, SUBLANES)
    rows = slots * slot_rows
    messages = project(tube_count, tokens, ln_gain, ln_bias, w_qkv, rows)
    got = lax.all_to_all(messages, "space", 0, 0, tiled=True)
    least = up_to((HEADS - 1) * up_to(slot_rows, PACK) + rows, QUERY_TILE)
    most = up_to((HEADS - 1) * rows + up_to(slot_rows, PACK), QUERY_TILE)
    sizes = list(range(least, most, QUERY_TILE))[:SIZE_CASES] + [most]
    counts = got[:, -1, -1].astype(jnp.int32)
    needed = jnp.sum(packed_rows(counts, slot_rows))
    case = jnp.clip((needed - least + QUERY_TILE - 1) // QUERY_TILE, 0, len(sizes) - 1)
    branches = [functools.partial(attend_size, size, slot_rows, time_dev) for size in sizes]
    returned = lax.switch(case, branches, got)
    back = lax.all_to_all(returned, "space", 0, 0, tiled=True)
    return mix(tube_count, back, tokens, w_out)


def layer_norm(flat, ln_gain, ln_bias):
    values32 = flat.astype(jnp.float32)
    center = values32 - jnp.mean(values32, axis=-1, keepdims=True)
    spread = jnp.mean(center * center, axis=-1, keepdims=True)
    return (center * lax.rsqrt(spread + EPSILON) * ln_gain + ln_bias).astype(jnp.bfloat16)


def live_mask(counts, slots_dev, time_dev):
    slot_ids = jnp.arange(slots_dev)[None, :, None]
    marks = jnp.broadcast_to(
        slot_ids < counts[:, None, None], (counts.shape[0], slots_dev, time_dev)
    )
    return marks.reshape(-1)


def attend(carry, query_heads, key_block, value_block, live_keys, scaling):
    best_now, total_now, accum = carry
    heads = query_heads.shape[1]
    key_heads = key_block.reshape(key_block.shape[0], heads, -1)
    value_heads = value_block.reshape(value_block.shape[0], heads, -1)
    scores = (
        jnp.einsum("qhd,khd->hqk", query_heads, key_heads, preferred_element_type=jnp.float32)
        * scaling
    )
    scores = jnp.where(live_keys[None, None, :], scores, NEG_FILL)
    best_next = jnp.maximum(best_now, jnp.max(scores, axis=-1))
    fading = jnp.exp(best_now - best_next)
    weights = jnp.exp(scores - best_next[..., None])
    total_next = total_now * fading + jnp.sum(weights, axis=-1)
    accum = accum * fading[..., None] + jnp.einsum(
        "hqk,khd->hqd",
        weights.astype(jnp.bfloat16),
        value_heads,
        preferred_element_type=jnp.float32,
    )
    return (best_next, total_next, accum)


def make_fold(query_heads, vis_dev, time_dev, scaling):
    rows_dev = vis_dev * time_dev

    def fold_masked(carry, piece, start):
        key_all, value_all, count_all = piece
        width_in = key_all.shape[1]
        shards = count_all.shape[0]
        group = 1
        for unused_bit in range(6):
            if shards % (group * 2) == 0 and group * rows_dev < 2048:
                group = group * 2
        blocks = shards // group
        key_groups = key_all.reshape(blocks, group * rows_dev, width_in)
        value_groups = value_all.reshape(blocks, group * rows_dev, width_in)
        count_groups = count_all.reshape(blocks, group)

        def step_group(state, item):
            key_group, value_group, count_group = item
            marks = live_mask(count_group, vis_dev, time_dev)
            return (attend(state, query_heads, key_group, value_group, marks, scaling), None)

        carry, unused = lax.scan(step_group, carry, (key_groups, value_groups, count_groups))
        return carry

    return fold_masked


def start_state(heads, rows, head_size):
    return (
        jnp.full((heads, rows), NEG_FILL, jnp.float32),
        jnp.zeros((heads, rows), jnp.float32),
        jnp.zeros((heads, rows, head_size), jnp.float32),
    )


def on_device(tokens, tube_count, ln_gain, ln_bias, w_qkv, w_out):
    vis_dev, time_dev, width = tokens.shape
    rows_dev = vis_dev * time_dev
    inner = w_out.shape[0]
    head_size = inner // HEADS
    flat = tokens.reshape(rows_dev, width)
    normed = layer_norm(flat, ln_gain, ln_bias)
    projected = jnp.dot(normed, w_qkv, preferred_element_type=jnp.float32).astype(jnp.bfloat16)
    scaling = head_size ** (-0.5)
    frames = lax.axis_size("frame")
    local_heads = HEADS // frames
    stacked = projected.reshape(rows_dev, 3, HEADS, head_size)
    regrouped = lax.all_to_all(stacked, "frame", split_axis=2, concat_axis=0, tiled=True)
    all_rows = regrouped.shape[0]
    query_local = regrouped[:, 0]
    key_local = regrouped[:, 1].reshape(all_rows, local_heads * head_size)
    value_local = regrouped[:, 2].reshape(all_rows, local_heads * head_size)
    counts_rep = jnp.tile(tube_count, frames)
    fold_fn = make_fold(query_local, vis_dev, time_dev, scaling)
    state = fold_fn(
        start_state(local_heads, all_rows, head_size),
        (
            lax.all_gather(key_local, "space", axis=0, tiled=True),
            lax.all_gather(value_local, "space", axis=0, tiled=True),
            lax.all_gather(counts_rep, "space", axis=0, tiled=True),
        ),
        jnp.int32(0),
    )
    best_final, total_final, accum_final = state
    attended = (accum_final / total_final[..., None]).astype(jnp.bfloat16)
    attended = jnp.transpose(attended, (1, 0, 2))
    returned = lax.all_to_all(attended, "frame", split_axis=0, concat_axis=1, tiled=True)
    attended = returned.reshape(rows_dev, inner)
    mixed = flat.astype(jnp.float32) + jnp.dot(attended, w_out, preferred_element_type=jnp.float32)
    own_live = live_mask(tube_count, vis_dev, time_dev)
    mixed = jnp.where(own_live[:, None], mixed, 0.0)
    return mixed.astype(jnp.bfloat16).reshape(vis_dev, time_dev, width)


def solution(mesh):
    in_specs = (P("space", "frame", None), P("space"), P(), P(), P(), P())
    out_specs = P("space", "frame", None)

    def layer(tokens, tube_count, ln_gain, ln_bias, w_qkv, w_out):
        slots = tokens.shape[0] // mesh.shape["space"]
        time_dev = tokens.shape[1] // mesh.shape["frame"]
        rows = slots * up_to(time_dev, SUBLANES)
        pairs = 2 * w_out.shape[0] == HEADS * LANES and rows % (2 * PACK) == 0
        padded = up_to(time_dev, SUBLANES) > time_dev
        fits = mesh.shape["space"] == HEADS and pairs and padded
        return jax.shard_map(
            head_per_device if fits else on_device,
            mesh=mesh,
            in_specs=in_specs,
            out_specs=out_specs,
            check_vma=False,
        )(tokens, tube_count, ln_gain, ln_bias, w_qkv, w_out)

    return layer
```

```python
import functools
import jax
import jax.numpy as jnp
from jax import lax
from jax.experimental import pallas as pl
from jax.experimental.pallas import tpu as pltpu
from jax.sharding import Mesh, PartitionSpec as P

HEADS = 8


EPSILON = 1e-06
NEG_FILL = -1e30
LANES = 128
SUBLANES = 8
PACK = 16
SIZE_STEP = 128
SIZE_CASES = 5
QUERY_TILE = 256
CHAINS = 2
VMEM_BYTES = 20 * 2**20

VMEM = pl.BlockSpec(memory_space=pltpu.VMEM)
SMEM = pl.BlockSpec(memory_space=pltpu.SMEM)
SWAP = [(0, 1), (1, 0)]


def up_to(value, unit):
    return -(-value // unit) * unit


def params():
    return pltpu.CompilerParams(vmem_limit_bytes=VMEM_BYTES)


def packed_rows(count, slot_rows):
    return (count * slot_rows + PACK - 1) // PACK * PACK


def slot_of(row, slots, slot_rows):
    slot = row * 0
    for edge in range(1, slots):
        slot = slot + (row >= edge * slot_rows).astype(jnp.int32)
    return slot


def live_rows(count, rows, slot_rows, time_dev, width):
    row = lax.broadcasted_iota(jnp.int32, (rows, width), 0)
    slot = slot_of(row, rows // slot_rows, slot_rows)
    return (slot < count) & (row - slot * slot_rows < time_dev)


def one_hot(shape, slots, slot_rows, padded_dim):
    padded = lax.broadcasted_iota(jnp.int32, shape, padded_dim)
    plain = lax.broadcasted_iota(jnp.int32, shape, 1 - padded_dim)
    slot = slot_of(padded, slots, slot_rows)
    hot = plain == (padded - slot * slot_rows) * slots + slot
    return hot.astype(jnp.float32).astype(jnp.bfloat16)


def project_kernel(count_ref, x_ref, gain_ref, bias_ref, wq_ref, wk_ref, wv_ref, out_ref, normed_ref):
    time_dev, slots, width = x_ref.shape
    rows = normed_ref.shape[0]
    slot_rows = rows // slots
    half = rows // 2
    heads_step = out_ref.shape[0]
    head_size = LANES // 2
    scaling = head_size ** (-0.5)
    count = count_ref[0]

    @pl.when(pl.program_id(0) == 0)
    def _():
        x = x_ref[...].astype(jnp.float32).reshape(time_dev * slots, width)
        center = x - jnp.mean(x, axis=-1, keepdims=True)
        spread = jnp.mean(center * center, axis=-1, keepdims=True)
        normed = center * lax.rsqrt(spread + EPSILON) * gain_ref[...] + bias_ref[...]
        hot = one_hot((rows, time_dev * slots), slots, slot_rows, 0)
        normed_ref[...] = jnp.dot(
            hot, normed.astype(jnp.bfloat16), preferred_element_type=jnp.float32
        ).astype(jnp.bfloat16)

    rows_in = normed_ref[...]
    query = jnp.dot(rows_in, wq_ref[...], preferred_element_type=jnp.float32) * scaling
    key = jnp.dot(rows_in, wk_ref[...], preferred_element_type=jnp.float32)
    value = jnp.dot(rows_in, wv_ref[...], preferred_element_type=jnp.float32)
    live = live_rows(count, rows, slot_rows, time_dev, LANES)
    left = lax.broadcasted_iota(jnp.int32, (rows, LANES), 1) < head_size
    left_half = left[:half]
    row_half = lax.broadcasted_iota(jnp.int32, (half, LANES), 0)
    mark = (row_half == half - 1) & jnp.logical_not(left_half)
    count_value = count.astype(jnp.float32)
    for pair in range(heads_step // 2):
        cols = slice(pair * LANES, (pair + 1) * LANES)
        key_pair = key[:, cols]
        key_pair = jnp.where(live, key_pair, key_pair[0:1])
        value_pair = jnp.where(live, value[:, cols], 0.0)
        even = jnp.where(left, key_pair, pltpu.roll(value_pair, head_size, 1))
        odd = jnp.where(left, pltpu.roll(key_pair, head_size, 1), value_pair)
        out_ref[2 * pair, 0:rows] = even.astype(jnp.bfloat16)
        out_ref[2 * pair + 1, 0:rows] = odd.astype(jnp.bfloat16)
        top = query[:half, cols]
        low = query[half:, cols]
        even = jnp.where(left_half, top, pltpu.roll(low, head_size, 1))
        odd = jnp.where(left_half, pltpu.roll(top, head_size, 1), low)
        even = jnp.where(mark, count_value, even)
        odd = jnp.where(mark, count_value, odd)
        out_ref[2 * pair, rows : rows + half] = even.astype(jnp.bfloat16)
        out_ref[2 * pair + 1, rows : rows + half] = odd.astype(jnp.bfloat16)


def project(count, tokens, ln_gain, ln_bias, w_qkv, rows):
    time_dev, slots, width = tokens.shape
    steps = 2
    heads_step = HEADS // steps
    cols = heads_step * LANES // 2
    whole = lambda step: (0, 0)
    return pl.pallas_call(
        project_kernel,
        grid=(steps,),
        out_shape=jax.ShapeDtypeStruct((HEADS, rows + rows // 2, LANES), jnp.bfloat16),
        in_specs=[
            SMEM,
            pl.BlockSpec(tokens.shape, lambda step: (0, 0, 0)),
            pl.BlockSpec((1, width), whole),
            pl.BlockSpec((1, width), whole),
            pl.BlockSpec((width, cols), lambda step: (0, step)),
            pl.BlockSpec((width, cols), lambda step: (0, steps + step)),
            pl.BlockSpec((width, cols), lambda step: (0, 2 * steps + step)),
        ],
        out_specs=pl.BlockSpec((heads_step, rows + rows // 2, LANES), lambda step: (step, 0, 0)),
        scratch_shapes=[pltpu.VMEM((rows, width), jnp.bfloat16)],
        compiler_params=params(),
        cost_estimate=pl.CostEstimate(
            flops=2 * rows * w_qkv.size, bytes_accessed=2 * w_qkv.size, transcendentals=0
        ),
        name="project",
    )(count, tokens, ln_gain.reshape(1, width), ln_bias.reshape(1, width), w_qkv, w_qkv, w_qkv)


def source_count(ref, source):
    message = ref.shape[1]
    tail = ref[source, message - PACK : message].astype(jnp.float32)
    return jnp.max(tail[PACK - 1 : PACK, LANES // 2 :]).astype(jnp.int32)


def case_kernel(slot_rows, least, cases, got_ref, other_ref, case_ref):
    total = jnp.int32(0)
    for ref in (got_ref, other_ref):
        for source in range(ref.shape[0]):
            total = total + packed_rows(source_count(ref, source), slot_rows)
    over = (total + 1) // 2 - least
    case_ref[0] = jnp.clip((over + SIZE_STEP - 1) // SIZE_STEP, 0, cases - 1)


def choose_case(got, other, slot_rows, least, cases):
    sources, message, lanes = got.shape
    tail = pl.BlockSpec((sources, PACK, lanes), lambda step: (0, message // PACK - 1, 0))
    return pl.pallas_call(
        functools.partial(case_kernel, slot_rows, least, cases),
        grid=(1,),
        out_shape=jax.ShapeDtypeStruct((1,), jnp.int32),
        in_specs=[tail, tail],
        out_specs=SMEM,
        compiler_params=params(),
        name="choose",
    )(got, other)[0]


def pack_kernel(
    slot_rows,
    time_dev,
    core_ref,
    got_ref,
    other_ref,
    sent_ref,
    kv_ref,
    live_ref,
    query_ref,
    start_ref,
    kv_room,
    live_room,
):
    sources, message, lanes = got_ref.shape
    rows = message * 2 // 3
    half = rows // 2
    head_size = lanes // 2
    size = sent_ref.shape[0]
    core = core_ref[0]
    lane = lax.broadcasted_iota(jnp.int32, (PACK, lanes), 1)
    first = got_ref[0, 0:PACK].astype(jnp.float32)[0:1]
    fill = jnp.where(lane < head_size, jnp.broadcast_to(first, (PACK, lanes)), 0.0)
    fill = fill.astype(jnp.bfloat16)
    blank = jnp.zeros((PACK, lanes), jnp.bfloat16)
    for start in range(0, 2 * size, PACK):
        kv_room[start : start + PACK] = fill
        live_room[start : start + PACK] = blank
    for start in range(0, query_ref.shape[0], PACK):
        query_ref[start : start + PACK] = blank

    def fill_in(refs):
        start = jnp.int32(0)
        for ref in refs:
            for source in range(sources):
                count = source_count(ref, source)
                place = pl.ds(pl.multiple_of(start, PACK), rows)
                kv_room[place] = ref[source, 0:rows]
                live = live_rows(count, rows, slot_rows, time_dev, lanes)
                live_room[place] = live.astype(jnp.float32).astype(jnp.bfloat16)
                start = start + packed_rows(count, slot_rows)

    @pl.when(core == 0)
    def _():
        fill_in((got_ref, other_ref))

    @pl.when(core != 0)
    def _():
        fill_in((other_ref, got_ref))

    sent_ref[...] = kv_room[pl.ds(pl.multiple_of(core * size, SIZE_STEP), size)]
    kv_ref[...] = kv_room[0 : 2 * size]
    live_ref[...] = live_room[0 : 2 * size]
    left = lax.broadcasted_iota(jnp.int32, (half, lanes), 1) < head_size
    start = jnp.int32(0)
    for source in range(sources):
        start_ref[source] = start
        pair = got_ref[source, rows:message].astype(jnp.float32)
        query_ref[pl.ds(pl.multiple_of(start, PACK), half)] = jnp.where(left, pair, 0.0).astype(
            jnp.bfloat16
        )
        query_ref[pl.ds(pl.multiple_of(start + half, PACK), half)] = jnp.where(
            left, pltpu.roll(pair, head_size, 1), 0.0
        ).astype(jnp.bfloat16)
        start = start + packed_rows(source_count(got_ref, source), slot_rows)
    start_ref[sources] = start


def pack(core, got, other, size, slot_rows, time_dev):
    sources, message, lanes = got.shape
    rows = message * 2 // 3
    array = lambda length: jax.ShapeDtypeStruct((length, lanes), jnp.bfloat16)
    room = pltpu.VMEM((2 * size + rows, lanes), jnp.bfloat16)
    queries = up_to(sources * rows, QUERY_TILE) + rows
    return pl.pallas_call(
        functools.partial(pack_kernel, slot_rows, time_dev),
        out_shape=(
            array(size),
            array(2 * size),
            array(2 * size),
            array(queries),
            jax.ShapeDtypeStruct((sources + 1,), jnp.int32),
        ),
        in_specs=[SMEM, VMEM, VMEM],
        out_specs=(VMEM, VMEM, VMEM, VMEM, SMEM),
        scratch_shapes=[room, room],
        compiler_params=params(),
        name="pack",
    )(core, got, other)


def attend_kernel(stage, half, *refs):
    core_ref, start_ref, query_ref, kv_ref, live_ref = refs[:5]
    side_ref = refs[-1]
    keys, lanes = kv_ref.shape
    head_size = lanes // 2
    left = lax.broadcasted_iota(jnp.int32, (keys, lanes), 1) < head_size
    if stage == 0:
        live = live_ref[...]
        best_in = sum_in = None
        best_out, sum_out = refs[5:7]
    else:
        part = core_ref[0] if stage == 1 else 1 - core_ref[0]
        live = live_ref[pl.ds(pl.multiple_of(part * keys, SIZE_STEP), keys)]
        best_in, sum_in = refs[5:7]
        if stage == 1:
            best_out, sum_out = refs[7:9]
        else:
            out_ref, sum_out = refs[7:9]
    side_ref[...] = jnp.where(left, live, kv_ref[...])
    total = start_ref[start_ref.shape[0] - 1]
    tile = QUERY_TILE // CHAINS

    def chain(place):
        scores = lax.dot_general(
            query_ref[place],
            kv_ref[...],
            (((1,), (1,)), ((), ())),
            preferred_element_type=jnp.float32,
        )
        best = jnp.max(scores, axis=-1, keepdims=True)
        if stage > 0:
            before = best_in[place][:, 0:1]
            best = jnp.maximum(best, before)
        weights = jnp.exp(scores - best).astype(jnp.bfloat16)
        sums = jnp.dot(weights, side_ref[...], preferred_element_type=jnp.float32)
        if stage > 0:
            sums = sums + sum_in[place] * jnp.exp(before - best)
        if stage == 2:
            sums = sums / pltpu.roll(sums, head_size, 1)
        else:
            best_out[place] = jnp.broadcast_to(best, (tile, lanes))
        sum_out[place] = sums

    def step(index, carry):
        for link in range(CHAINS):
            start = pl.multiple_of(index * QUERY_TILE + link * tile, tile)
            chain(pl.ds(start, tile))
        return carry

    lax.fori_loop(0, (total + QUERY_TILE - 1) // QUERY_TILE, step, 0)
    if stage == 2:
        left_half = lax.broadcasted_iota(jnp.int32, (half, lanes), 1) < head_size
        for source in range(out_ref.shape[0]):
            start = start_ref[source]
            top = sum_out[pl.ds(pl.multiple_of(start, PACK), half)]
            low = sum_out[pl.ds(pl.multiple_of(start + half, PACK), half)]
            out_ref[source] = jnp.where(left_half, pltpu.roll(top, head_size, 1), low).astype(
                jnp.bfloat16
            )


def run_stage(stage, half, core, starts, query, kv, live, *state):
    keys, lanes = kv.shape
    queries = query.shape[0]
    sources = starts.shape[0] - 1
    held = jax.ShapeDtypeStruct((queries, lanes), jnp.float32)
    scratch = [pltpu.VMEM((keys, lanes), jnp.bfloat16)]
    if stage == 2:
        out_shape = jax.ShapeDtypeStruct((sources, half, lanes), jnp.bfloat16)
        out_specs = VMEM
        scratch = [pltpu.VMEM((queries, lanes), jnp.float32)] + scratch
    else:
        out_shape = (held, held)
        out_specs = (VMEM, VMEM)
    return pl.pallas_call(
        functools.partial(attend_kernel, stage, half),
        out_shape=out_shape,
        in_specs=[SMEM, SMEM] + [VMEM] * (3 + len(state)),
        out_specs=out_specs,
        scratch_shapes=scratch,
        input_output_aliases={5: 0, 6: 1} if stage == 1 else {},
        compiler_params=params(),
        cost_estimate=pl.CostEstimate(
            flops=4 * keys * keys * lanes, bytes_accessed=keys * lanes * 8, transcendentals=0
        ),
        name="attend" + str(stage),
    )(core, starts, query, kv, live, *state)


def attend_size(size, slot_rows, time_dev, core, got, other):
    rows = got.shape[1] * 2 // 3
    half = rows // 2
    sent, kv, live, query, starts = pack(core, got, other, size, slot_rows, time_dev)
    far = lax.ppermute(sent, "far", SWAP)
    state = run_stage(0, half, core, starts, query, kv, live)
    far_other = lax.ppermute(far, "core", SWAP)
    state = run_stage(1, half, core, starts, query, far, live, *state)
    return run_stage(2, half, core, starts, query, far_other, live, *state)


def mix_kernel(count_ref, got_ref, x_ref, w_ref, out_ref):
    heads, half, lanes = got_ref.shape
    time_dev, slots, width = x_ref.shape
    slot_rows = 2 * half // slots
    head_size = lanes // 2
    left = lax.broadcasted_iota(jnp.int32, (half, lanes), 1) < head_size
    tops = []
    lows = []
    for pair in range(heads // 2):
        even = got_ref[2 * pair].astype(jnp.float32)
        odd = got_ref[2 * pair + 1].astype(jnp.float32)
        tops.append(jnp.where(left, even, pltpu.roll(odd, head_size, 1)))
        lows.append(jnp.where(left, pltpu.roll(even, head_size, 1), odd))
    top = jnp.concatenate(tops, axis=1)
    low = jnp.concatenate(lows, axis=1)
    attended = jnp.concatenate([top, low], axis=0)
    live = live_rows(count_ref[0], 2 * half, slot_rows, time_dev, attended.shape[1])
    attended = jnp.where(live, attended, 0.0).astype(jnp.bfloat16)
    hot = one_hot((time_dev * slots, 2 * half), slots, slot_rows, 1)
    attended = jnp.dot(hot, attended, preferred_element_type=jnp.float32).astype(jnp.bfloat16)
    mixed = jnp.dot(attended, w_ref[...], preferred_element_type=jnp.float32)
    full = x_ref[...].astype(jnp.float32) + mixed.reshape(time_dev, slots, width)
    slot = lax.broadcasted_iota(jnp.int32, full.shape, 1)
    out_ref[...] = jnp.where(slot < count_ref[0], full, 0.0).astype(jnp.bfloat16)


def mix(count, got, tokens, w_out):
    return pl.pallas_call(
        mix_kernel,
        out_shape=jax.ShapeDtypeStruct(tokens.shape, jnp.bfloat16),
        in_specs=[SMEM, VMEM, VMEM, VMEM],
        out_specs=VMEM,
        compiler_params=params(),
        cost_estimate=pl.CostEstimate(
            flops=4 * got.shape[1] * w_out.size, bytes_accessed=2 * w_out.size, transcendentals=0
        ),
        name="mix",
    )(count, got, tokens, w_out)


def head_per_device(tokens, tube_count, ln_gain, ln_bias, w_qkv, w_out):
    slots, time_dev, width = tokens.shape
    slot_rows = up_to(time_dev, SUBLANES)
    rows = slots * slot_rows
    by_time = jnp.transpose(tokens, (1, 0, 2))
    messages = project(tube_count, by_time, ln_gain, ln_bias, w_qkv, rows)
    got = lax.all_to_all(messages, ("near", "chip"), 0, 0, tiled=True)
    other = lax.ppermute(got, "core", SWAP)
    core = lax.axis_index("core").reshape(1)
    least = up_to((HEADS - 1) * up_to(slot_rows, PACK) + rows, SIZE_STEP)
    most = up_to((HEADS - 1) * rows + up_to(slot_rows, PACK), SIZE_STEP)
    sizes = list(range(least, most, SIZE_STEP))[:SIZE_CASES] + [most]
    case = choose_case(got, other, slot_rows, least, len(sizes))
    branches = [functools.partial(attend_size, size, slot_rows, time_dev) for size in sizes]
    returned = lax.switch(case, branches, core, got, other)
    back = lax.all_to_all(returned, ("near", "chip"), 0, 0, tiled=True)
    mixed = mix(tube_count, back, by_time, w_out)
    return jnp.transpose(mixed, (1, 0, 2))


def layer_norm(flat, ln_gain, ln_bias):
    values32 = flat.astype(jnp.float32)
    center = values32 - jnp.mean(values32, axis=-1, keepdims=True)
    spread = jnp.mean(center * center, axis=-1, keepdims=True)
    return (center * lax.rsqrt(spread + EPSILON) * ln_gain + ln_bias).astype(jnp.bfloat16)


def live_mask(counts, slots_dev, time_dev):
    slot_ids = jnp.arange(slots_dev)[None, :, None]
    marks = jnp.broadcast_to(
        slot_ids < counts[:, None, None], (counts.shape[0], slots_dev, time_dev)
    )
    return marks.reshape(-1)


def attend(carry, query_heads, key_block, value_block, live_keys, scaling):
    best_now, total_now, accum = carry
    heads = query_heads.shape[1]
    key_heads = key_block.reshape(key_block.shape[0], heads, -1)
    value_heads = value_block.reshape(value_block.shape[0], heads, -1)
    scores = (
        jnp.einsum("qhd,khd->hqk", query_heads, key_heads, preferred_element_type=jnp.float32)
        * scaling
    )
    scores = jnp.where(live_keys[None, None, :], scores, NEG_FILL)
    best_next = jnp.maximum(best_now, jnp.max(scores, axis=-1))
    fading = jnp.exp(best_now - best_next)
    weights = jnp.exp(scores - best_next[..., None])
    total_next = total_now * fading + jnp.sum(weights, axis=-1)
    accum = accum * fading[..., None] + jnp.einsum(
        "hqk,khd->hqd",
        weights.astype(jnp.bfloat16),
        value_heads,
        preferred_element_type=jnp.float32,
    )
    return (best_next, total_next, accum)


def make_fold(query_heads, vis_dev, time_dev, scaling):
    rows_dev = vis_dev * time_dev

    def fold_masked(carry, piece, start):
        key_all, value_all, count_all = piece
        width_in = key_all.shape[1]
        shards = count_all.shape[0]
        group = 1
        for unused_bit in range(6):
            if shards % (group * 2) == 0 and group * rows_dev < 2048:
                group = group * 2
        blocks = shards // group
        key_groups = key_all.reshape(blocks, group * rows_dev, width_in)
        value_groups = value_all.reshape(blocks, group * rows_dev, width_in)
        count_groups = count_all.reshape(blocks, group)

        def step_group(state, item):
            key_group, value_group, count_group = item
            marks = live_mask(count_group, vis_dev, time_dev)
            return (attend(state, query_heads, key_group, value_group, marks, scaling), None)

        carry, unused = lax.scan(step_group, carry, (key_groups, value_groups, count_groups))
        return carry

    return fold_masked


def start_state(heads, rows, head_size):
    return (
        jnp.full((heads, rows), NEG_FILL, jnp.float32),
        jnp.zeros((heads, rows), jnp.float32),
        jnp.zeros((heads, rows, head_size), jnp.float32),
    )


def on_device(tokens, tube_count, ln_gain, ln_bias, w_qkv, w_out):
    vis_dev, time_dev, width = tokens.shape
    rows_dev = vis_dev * time_dev
    inner = w_out.shape[0]
    head_size = inner // HEADS
    flat = tokens.reshape(rows_dev, width)
    normed = layer_norm(flat, ln_gain, ln_bias)
    projected = jnp.dot(normed, w_qkv, preferred_element_type=jnp.float32).astype(jnp.bfloat16)
    scaling = head_size ** (-0.5)
    frames = lax.axis_size("frame")
    local_heads = HEADS // frames
    stacked = projected.reshape(rows_dev, 3, HEADS, head_size)
    regrouped = lax.all_to_all(stacked, "frame", split_axis=2, concat_axis=0, tiled=True)
    all_rows = regrouped.shape[0]
    query_local = regrouped[:, 0]
    key_local = regrouped[:, 1].reshape(all_rows, local_heads * head_size)
    value_local = regrouped[:, 2].reshape(all_rows, local_heads * head_size)
    counts_rep = jnp.tile(tube_count, frames)
    fold_fn = make_fold(query_local, vis_dev, time_dev, scaling)
    state = fold_fn(
        start_state(local_heads, all_rows, head_size),
        (
            lax.all_gather(key_local, "space", axis=0, tiled=True),
            lax.all_gather(value_local, "space", axis=0, tiled=True),
            lax.all_gather(counts_rep, "space", axis=0, tiled=True),
        ),
        jnp.int32(0),
    )
    best_final, total_final, accum_final = state
    attended = (accum_final / total_final[..., None]).astype(jnp.bfloat16)
    attended = jnp.transpose(attended, (1, 0, 2))
    returned = lax.all_to_all(attended, "frame", split_axis=0, concat_axis=1, tiled=True)
    attended = returned.reshape(rows_dev, inner)
    mixed = flat.astype(jnp.float32) + jnp.dot(attended, w_out, preferred_element_type=jnp.float32)
    own_live = live_mask(tube_count, vis_dev, time_dev)
    mixed = jnp.where(own_live[:, None], mixed, 0.0)
    return mixed.astype(jnp.bfloat16).reshape(vis_dev, time_dev, width)


def solution(mesh):
    frames, spaces = mesh.shape["frame"], mesh.shape["space"]
    near = max(1, 2 * HEADS // spaces)
    parts = (frames // near, near, spaces // 2, 2)

    def layer(tokens, tube_count, ln_gain, ln_bias, w_qkv, w_out):
        slots = tokens.shape[0] // spaces
        time_dev = tokens.shape[1] // frames
        rows = slots * up_to(time_dev, SUBLANES)
        pairs = 2 * w_out.shape[0] == HEADS * LANES and rows % (2 * PACK) == 0
        padded = up_to(time_dev, SUBLANES) > time_dev
        split = parts[0] == 2 and parts[1] * parts[2] == HEADS and parts[0] * near == frames
        if split and pairs and padded:
            run, over = head_per_device, Mesh(
                mesh.devices.reshape(parts), ("far", "near", "chip", "core")
            )
            frame, space = ("far", "near"), ("chip", "core")
        else:
            run, over, frame, space = on_device, mesh, "frame", "space"
        return jax.shard_map(
            run,
            mesh=over,
            in_specs=(P(space, frame, None), P(space), P(), P(), P(), P()),
            out_specs=P(space, frame, None),
            check_vma=False,
        )(tokens, tube_count, ln_gain, ln_bias, w_qkv, w_out)

    return layer
```

```python
import functools
import jax
import jax.numpy as jnp
from jax import lax
from jax.experimental import pallas as pl
from jax.experimental.pallas import tpu as pltpu
from jax.sharding import Mesh, PartitionSpec as P

HEADS = 8


EPSILON = 1e-06
NEG_FILL = -1e30
LANES = 128
SUBLANES = 8
PACK = 16
SIZE_STEP = 128
SIZE_CASES = 3
QUERY_TILE = 256
QUERY_BIG = 512
PROJECT_STEPS = 2
VMEM_BYTES = 20 * 2**20
VMEM_WHOLE = 67043328

VMEM = pl.BlockSpec(memory_space=pltpu.VMEM)
SMEM = pl.BlockSpec(memory_space=pltpu.SMEM)
SWAP = [(0, 1), (1, 0)]


def up_to(value, unit):
    return -(-value // unit) * unit


def params():
    return pltpu.CompilerParams(vmem_limit_bytes=VMEM_BYTES)


def packed_rows(count, slot_rows):
    return (count * slot_rows + PACK - 1) // PACK * PACK


def slot_of(row, slots, slot_rows):
    slot = row * 0
    for edge in range(1, slots):
        slot = slot + (row >= edge * slot_rows).astype(jnp.int32)
    return slot


def live_rows(count, rows, slot_rows, time_dev, width):
    row = lax.broadcasted_iota(jnp.int32, (rows, width), 0)
    slot = slot_of(row, rows // slot_rows, slot_rows)
    return (slot < count) & (row - slot * slot_rows < time_dev)


def one_hot(shape, slots, slot_rows, padded_dim):
    padded = lax.broadcasted_iota(jnp.int32, shape, padded_dim)
    plain = lax.broadcasted_iota(jnp.int32, shape, 1 - padded_dim)
    slot = slot_of(padded, slots, slot_rows)
    hot = plain == (padded - slot * slot_rows) * slots + slot
    return hot.astype(jnp.float32).astype(jnp.bfloat16)


def project_kernel(
    count_ref,
    x_hbm,
    gain_hbm,
    bias_hbm,
    w_hbm,
    out_ref,
    x_ref,
    gain_ref,
    bias_ref,
    w_ref,
    input_sems,
    w_sems,
):
    time_dev, slots, width = x_ref.shape
    heads, message, lanes = out_ref.shape
    rows = message * 2 // 3
    slot_rows = rows // slots
    half = rows // 2
    head_size = lanes // 2
    scaling = head_size ** (-0.5)
    count = count_ref[0]
    inputs = [
        pltpu.make_async_copy(source, target, input_sems.at[place])
        for place, (source, target) in enumerate(
            ((x_hbm, x_ref), (gain_hbm, gain_ref), (bias_hbm, bias_ref))
        )
    ]
    for copy in inputs:
        copy.start()
    kinds = 3
    wide = w_ref.shape[1] // (kinds * PROJECT_STEPS)
    weights = []
    for step in range(PROJECT_STEPS):
        for kind in range(kinds):
            cols = pl.ds((kind * PROJECT_STEPS + step) * wide, wide)
            copy = pltpu.make_async_copy(
                w_hbm.at[:, cols], w_ref.at[:, cols], w_sems.at[step, kind]
            )
            copy.start()
            weights.append((copy, cols))
    for copy in inputs:
        copy.wait()
    x = x_ref[...].astype(jnp.float32).reshape(time_dev * slots, width)
    center = x - jnp.mean(x, axis=-1, keepdims=True)
    spread = jnp.mean(center * center, axis=-1, keepdims=True)
    normed = center * lax.rsqrt(spread + EPSILON) * gain_ref[...] + bias_ref[...]
    hot = one_hot((rows, time_dev * slots), slots, slot_rows, 0)
    rows_in = jnp.dot(
        hot, normed.astype(jnp.bfloat16), preferred_element_type=jnp.float32
    ).astype(jnp.bfloat16)
    live = live_rows(count, rows, slot_rows, time_dev, lanes)
    left = lax.broadcasted_iota(jnp.int32, (rows, lanes), 1) < head_size
    left_half = left[:half]
    row_half = lax.broadcasted_iota(jnp.int32, (half, lanes), 0)
    mark = (row_half == half - 1) & jnp.logical_not(left_half)
    count_value = count.astype(jnp.float32)
    pairs = heads // 2 // PROJECT_STEPS
    for step in range(PROJECT_STEPS):
        found = []
        for copy, cols in weights[step * kinds : (step + 1) * kinds]:
            copy.wait()
            found.append(jnp.dot(rows_in, w_ref[:, cols], preferred_element_type=jnp.float32))
        query, key, value = found
        query = query * scaling
        for pair in range(pairs):
            head = 2 * (step * pairs + pair)
            cols = slice(pair * lanes, (pair + 1) * lanes)
            key_pair = key[:, cols]
            key_pair = jnp.where(live, key_pair, key_pair[0:1])
            value_pair = jnp.where(live, value[:, cols], 0.0)
            even = jnp.where(left, key_pair, pltpu.roll(value_pair, head_size, 1))
            odd = jnp.where(left, pltpu.roll(key_pair, head_size, 1), value_pair)
            out_ref[head, 0:rows] = even.astype(jnp.bfloat16)
            out_ref[head + 1, 0:rows] = odd.astype(jnp.bfloat16)
            top = query[:half, cols]
            low = query[half:, cols]
            even = jnp.where(left_half, top, pltpu.roll(low, head_size, 1))
            odd = jnp.where(left_half, pltpu.roll(top, head_size, 1), low)
            even = jnp.where(mark, count_value, even)
            odd = jnp.where(mark, count_value, odd)
            out_ref[head, rows:message] = even.astype(jnp.bfloat16)
            out_ref[head + 1, rows:message] = odd.astype(jnp.bfloat16)


def project(count, tokens, ln_gain, ln_bias, w_qkv, rows):
    width = tokens.shape[-1]
    gain = ln_gain.reshape(1, width)
    bias = ln_bias.reshape(1, width)
    hbm = pl.BlockSpec(memory_space=pltpu.HBM)
    return pl.pallas_call(
        project_kernel,
        out_shape=jax.ShapeDtypeStruct((HEADS, rows + rows // 2, LANES), jnp.bfloat16),
        in_specs=[SMEM, hbm, hbm, hbm, hbm],
        out_specs=VMEM,
        scratch_shapes=[
            pltpu.VMEM(tokens.shape, tokens.dtype),
            pltpu.VMEM(gain.shape, gain.dtype),
            pltpu.VMEM(bias.shape, bias.dtype),
            pltpu.VMEM(w_qkv.shape, w_qkv.dtype),
            pltpu.SemaphoreType.DMA((3,)),
            pltpu.SemaphoreType.DMA((PROJECT_STEPS, 3)),
        ],
        compiler_params=pltpu.CompilerParams(vmem_limit_bytes=VMEM_WHOLE),
        cost_estimate=pl.CostEstimate(
            flops=2 * rows * w_qkv.size, bytes_accessed=2 * w_qkv.size, transcendentals=0
        ),
        name="project",
    )(count, tokens, gain, bias, w_qkv)


def source_count(ref, source):
    message = ref.shape[1]
    tail = ref[source, message - PACK : message].astype(jnp.float32)
    return jnp.max(tail[PACK - 1 : PACK, LANES // 2 :]).astype(jnp.int32)


def case_kernel(slot_rows, least, cases, got_ref, other_ref, case_ref):
    total = jnp.int32(0)
    for ref in (got_ref, other_ref):
        for source in range(ref.shape[0]):
            total = total + packed_rows(source_count(ref, source), slot_rows)
    over = (total + 1) // 2 - least
    case_ref[0] = jnp.clip((over + SIZE_STEP - 1) // SIZE_STEP, 0, cases - 1)


def choose_case(got, other, slot_rows, least, cases):
    sources, message, lanes = got.shape
    tail = pl.BlockSpec((sources, PACK, lanes), lambda step: (0, message // PACK - 1, 0))
    return pl.pallas_call(
        functools.partial(case_kernel, slot_rows, least, cases),
        grid=(1,),
        out_shape=jax.ShapeDtypeStruct((1,), jnp.int32),
        in_specs=[tail, tail],
        out_specs=SMEM,
        compiler_params=params(),
        name="choose",
    )(got, other)[0]


def pack_kernel(
    slot_rows,
    time_dev,
    core_ref,
    got_ref,
    other_ref,
    sent_ref,
    kv_ref,
    live_ref,
    query_ref,
    start_ref,
    kv_room,
    live_room,
):
    sources, message, lanes = got_ref.shape
    rows = message * 2 // 3
    half = rows // 2
    head_size = lanes // 2
    size = sent_ref.shape[0]
    core = core_ref[0]
    lane = lax.broadcasted_iota(jnp.int32, (PACK, lanes), 1)
    first = got_ref[0, 0:PACK].astype(jnp.float32)[0:1]
    fill = jnp.where(lane < head_size, jnp.broadcast_to(first, (PACK, lanes)), 0.0)
    fill = fill.astype(jnp.bfloat16)
    blank = jnp.zeros((PACK, lanes), jnp.bfloat16)
    for start in range(0, 2 * size, PACK):
        kv_room[start : start + PACK] = fill
        live_room[start : start + PACK] = blank
    for start in range(0, query_ref.shape[0], PACK):
        query_ref[start : start + PACK] = blank

    def fill_in(refs):
        start = jnp.int32(0)
        for ref in refs:
            for source in range(sources):
                count = source_count(ref, source)
                place = pl.ds(pl.multiple_of(start, PACK), rows)
                kv_room[place] = ref[source, 0:rows]
                live = live_rows(count, rows, slot_rows, time_dev, lanes)
                live_room[place] = live.astype(jnp.float32).astype(jnp.bfloat16)
                start = start + packed_rows(count, slot_rows)

    @pl.when(core == 0)
    def _():
        fill_in((got_ref, other_ref))

    @pl.when(core != 0)
    def _():
        fill_in((other_ref, got_ref))

    sent_ref[...] = kv_room[pl.ds(pl.multiple_of(core * size, SIZE_STEP), size)]
    kv_ref[...] = kv_room[0 : 2 * size]
    live_ref[...] = live_room[0 : 2 * size]
    left = lax.broadcasted_iota(jnp.int32, (half, lanes), 1) < head_size
    start = jnp.int32(0)
    for source in range(sources):
        start_ref[source] = start
        pair = got_ref[source, rows:message].astype(jnp.float32)
        query_ref[pl.ds(pl.multiple_of(start, PACK), half)] = jnp.where(left, pair, 0.0).astype(
            jnp.bfloat16
        )
        query_ref[pl.ds(pl.multiple_of(start + half, PACK), half)] = jnp.where(
            left, pltpu.roll(pair, head_size, 1), 0.0
        ).astype(jnp.bfloat16)
        start = start + packed_rows(source_count(got_ref, source), slot_rows)
    start_ref[sources] = start


def pack(core, got, other, size, slot_rows, time_dev):
    sources, message, lanes = got.shape
    rows = message * 2 // 3
    array = lambda length: jax.ShapeDtypeStruct((length, lanes), jnp.bfloat16)
    room = pltpu.VMEM((2 * size + rows, lanes), jnp.bfloat16)
    queries = up_to(sources * rows, QUERY_TILE) + rows
    return pl.pallas_call(
        functools.partial(pack_kernel, slot_rows, time_dev),
        out_shape=(
            array(size),
            array(2 * size),
            array(2 * size),
            array(queries),
            jax.ShapeDtypeStruct((sources + 1,), jnp.int32),
        ),
        in_specs=[SMEM, VMEM, VMEM],
        out_specs=(VMEM, VMEM, VMEM, VMEM, SMEM),
        scratch_shapes=[room, room],
        compiler_params=params(),
        name="pack",
    )(core, got, other)


def attend_kernel(stage, half, *refs):
    core_ref, start_ref, query_ref, kv_ref, live_ref = refs[:5]
    side_ref = refs[-1]
    keys, lanes = kv_ref.shape
    head_size = lanes // 2
    left = lax.broadcasted_iota(jnp.int32, (keys, lanes), 1) < head_size
    if stage == 0:
        live = live_ref[...]
        best_in = sum_in = None
        best_out, sum_out = refs[5:7]
    else:
        part = core_ref[0] if stage == 1 else 1 - core_ref[0]
        live = live_ref[pl.ds(pl.multiple_of(part * keys, SIZE_STEP), keys)]
        best_in, sum_in = refs[5:7]
        if stage == 1:
            best_out, sum_out = refs[7:9]
        else:
            out_ref, sum_out = refs[7:9]
    side_ref[...] = jnp.where(left, live, kv_ref[...])
    total = start_ref[start_ref.shape[0] - 1]

    def chain(start, tile):
        place = pl.ds(pl.multiple_of(start, QUERY_TILE), tile)
        scores = lax.dot_general(
            query_ref[place],
            kv_ref[...],
            (((1,), (1,)), ((), ())),
            preferred_element_type=jnp.float32,
        )
        best = jnp.max(scores, axis=-1, keepdims=True)
        if stage > 0:
            before = best_in[place][:, 0:1]
            best = jnp.maximum(best, before)
        weights = jnp.exp(scores - best).astype(jnp.bfloat16)
        sums = jnp.dot(weights, side_ref[...], preferred_element_type=jnp.float32)
        if stage > 0:
            sums = sums + sum_in[place] * jnp.exp(before - best)
        if stage == 2:
            sums = sums / pltpu.roll(sums, head_size, 1)
        else:
            best_out[place] = jnp.broadcast_to(best, (tile, lanes))
        sum_out[place] = sums

    def step(index, carry):
        chain(index * QUERY_BIG, QUERY_BIG)
        return carry

    bigs = (total + QUERY_BIG - QUERY_TILE - 1) // QUERY_BIG
    lax.fori_loop(0, bigs, step, 0)

    @pl.when(total > bigs * QUERY_BIG)
    def _():
        chain(bigs * QUERY_BIG, QUERY_TILE)

    if stage == 2:
        left_half = lax.broadcasted_iota(jnp.int32, (half, lanes), 1) < head_size
        for source in range(out_ref.shape[0]):
            start = start_ref[source]
            top = sum_out[pl.ds(pl.multiple_of(start, PACK), half)]
            low = sum_out[pl.ds(pl.multiple_of(start + half, PACK), half)]
            out_ref[source] = jnp.where(left_half, pltpu.roll(top, head_size, 1), low).astype(
                jnp.bfloat16
            )


def run_stage(stage, half, core, starts, query, kv, live, *state):
    keys, lanes = kv.shape
    queries = query.shape[0]
    sources = starts.shape[0] - 1
    held = jax.ShapeDtypeStruct((queries, lanes), jnp.float32)
    scratch = [pltpu.VMEM((keys, lanes), jnp.bfloat16)]
    if stage == 2:
        out_shape = jax.ShapeDtypeStruct((sources, half, lanes), jnp.bfloat16)
        out_specs = VMEM
        scratch = [pltpu.VMEM((queries, lanes), jnp.float32)] + scratch
    else:
        out_shape = (held, held)
        out_specs = (VMEM, VMEM)
    return pl.pallas_call(
        functools.partial(attend_kernel, stage, half),
        out_shape=out_shape,
        in_specs=[SMEM, SMEM] + [VMEM] * (3 + len(state)),
        out_specs=out_specs,
        scratch_shapes=scratch,
        input_output_aliases={5: 0, 6: 1} if stage == 1 else {},
        compiler_params=params(),
        cost_estimate=pl.CostEstimate(
            flops=4 * keys * keys * lanes, bytes_accessed=keys * lanes * 8, transcendentals=0
        ),
        name="attend" + str(stage),
    )(core, starts, query, kv, live, *state)


def attend_size(size, slot_rows, time_dev, core, got, other):
    rows = got.shape[1] * 2 // 3
    half = rows // 2
    sent, kv, live, query, starts = pack(core, got, other, size, slot_rows, time_dev)
    far = lax.ppermute(sent, "far", SWAP)
    state = run_stage(0, half, core, starts, query, kv, live)
    far, *state = lax.optimization_barrier((far, *state))
    far_other = lax.ppermute(far, "core", SWAP)
    state = run_stage(1, half, core, starts, query, far, live, *state)
    return run_stage(2, half, core, starts, query, far_other, live, *state)


def mix_kernel(count_ref, got_ref, x_ref, w_ref, out_ref):
    heads, half, lanes = got_ref.shape
    time_dev, slots, width = x_ref.shape
    slot_rows = 2 * half // slots
    head_size = lanes // 2
    left = lax.broadcasted_iota(jnp.int32, (half, lanes), 1) < head_size
    tops = []
    lows = []
    for pair in range(heads // 2):
        even = got_ref[2 * pair].astype(jnp.float32)
        odd = got_ref[2 * pair + 1].astype(jnp.float32)
        tops.append(jnp.where(left, even, pltpu.roll(odd, head_size, 1)))
        lows.append(jnp.where(left, pltpu.roll(even, head_size, 1), odd))
    top = jnp.concatenate(tops, axis=1)
    low = jnp.concatenate(lows, axis=1)
    attended = jnp.concatenate([top, low], axis=0)
    live = live_rows(count_ref[0], 2 * half, slot_rows, time_dev, attended.shape[1])
    attended = jnp.where(live, attended, 0.0).astype(jnp.bfloat16)
    hot = one_hot((time_dev * slots, 2 * half), slots, slot_rows, 1)
    attended = jnp.dot(hot, attended, preferred_element_type=jnp.float32).astype(jnp.bfloat16)
    mixed = jnp.dot(attended, w_ref[...], preferred_element_type=jnp.float32)
    full = x_ref[...].astype(jnp.float32) + mixed.reshape(time_dev, slots, width)
    slot = lax.broadcasted_iota(jnp.int32, full.shape, 1)
    out_ref[...] = jnp.where(slot < count_ref[0], full, 0.0).astype(jnp.bfloat16)


def mix(count, got, tokens, w_out):
    return pl.pallas_call(
        mix_kernel,
        out_shape=jax.ShapeDtypeStruct(tokens.shape, jnp.bfloat16),
        in_specs=[SMEM, VMEM, VMEM, VMEM],
        out_specs=VMEM,
        compiler_params=params(),
        cost_estimate=pl.CostEstimate(
            flops=4 * got.shape[1] * w_out.size, bytes_accessed=2 * w_out.size, transcendentals=0
        ),
        name="mix",
    )(count, got, tokens, w_out)


def head_per_device(tokens, tube_count, ln_gain, ln_bias, w_qkv, w_out):
    slots, time_dev, width = tokens.shape
    slot_rows = up_to(time_dev, SUBLANES)
    rows = slots * slot_rows
    by_time = jnp.transpose(tokens, (1, 0, 2))
    messages = project(tube_count, by_time, ln_gain, ln_bias, w_qkv, rows)
    got = lax.all_to_all(messages, ("near", "chip"), 0, 0, tiled=True)
    other = lax.ppermute(got, "core", SWAP)
    core = lax.axis_index("core").reshape(1)
    least = up_to((HEADS - 1) * up_to(slot_rows, PACK) + rows, SIZE_STEP) + SIZE_STEP
    most = up_to((HEADS - 1) * rows + up_to(slot_rows, PACK), SIZE_STEP)
    sizes = list(range(least, most, SIZE_STEP))[:SIZE_CASES] + [most]
    case = choose_case(got, other, slot_rows, least, len(sizes))
    branches = [functools.partial(attend_size, size, slot_rows, time_dev) for size in sizes]
    returned = lax.switch(case, branches, core, got, other)
    back = lax.all_to_all(returned, ("near", "chip"), 0, 0, tiled=True)
    mixed = mix(tube_count, back, by_time, w_out)
    return jnp.transpose(mixed, (1, 0, 2))


def layer_norm(flat, ln_gain, ln_bias):
    values32 = flat.astype(jnp.float32)
    center = values32 - jnp.mean(values32, axis=-1, keepdims=True)
    spread = jnp.mean(center * center, axis=-1, keepdims=True)
    return (center * lax.rsqrt(spread + EPSILON) * ln_gain + ln_bias).astype(jnp.bfloat16)


def live_mask(counts, slots_dev, time_dev):
    slot_ids = jnp.arange(slots_dev)[None, :, None]
    marks = jnp.broadcast_to(
        slot_ids < counts[:, None, None], (counts.shape[0], slots_dev, time_dev)
    )
    return marks.reshape(-1)


def attend(carry, query_heads, key_block, value_block, live_keys, scaling):
    best_now, total_now, accum = carry
    heads = query_heads.shape[1]
    key_heads = key_block.reshape(key_block.shape[0], heads, -1)
    value_heads = value_block.reshape(value_block.shape[0], heads, -1)
    scores = (
        jnp.einsum("qhd,khd->hqk", query_heads, key_heads, preferred_element_type=jnp.float32)
        * scaling
    )
    scores = jnp.where(live_keys[None, None, :], scores, NEG_FILL)
    best_next = jnp.maximum(best_now, jnp.max(scores, axis=-1))
    fading = jnp.exp(best_now - best_next)
    weights = jnp.exp(scores - best_next[..., None])
    total_next = total_now * fading + jnp.sum(weights, axis=-1)
    accum = accum * fading[..., None] + jnp.einsum(
        "hqk,khd->hqd",
        weights.astype(jnp.bfloat16),
        value_heads,
        preferred_element_type=jnp.float32,
    )
    return (best_next, total_next, accum)


def make_fold(query_heads, vis_dev, time_dev, scaling):
    rows_dev = vis_dev * time_dev

    def fold_masked(carry, piece, start):
        key_all, value_all, count_all = piece
        width_in = key_all.shape[1]
        shards = count_all.shape[0]
        group = 1
        for unused_bit in range(6):
            if shards % (group * 2) == 0 and group * rows_dev < 2048:
                group = group * 2
        blocks = shards // group
        key_groups = key_all.reshape(blocks, group * rows_dev, width_in)
        value_groups = value_all.reshape(blocks, group * rows_dev, width_in)
        count_groups = count_all.reshape(blocks, group)

        def step_group(state, item):
            key_group, value_group, count_group = item
            marks = live_mask(count_group, vis_dev, time_dev)
            return (attend(state, query_heads, key_group, value_group, marks, scaling), None)

        carry, unused = lax.scan(step_group, carry, (key_groups, value_groups, count_groups))
        return carry

    return fold_masked


def start_state(heads, rows, head_size):
    return (
        jnp.full((heads, rows), NEG_FILL, jnp.float32),
        jnp.zeros((heads, rows), jnp.float32),
        jnp.zeros((heads, rows, head_size), jnp.float32),
    )


def on_device(tokens, tube_count, ln_gain, ln_bias, w_qkv, w_out):
    vis_dev, time_dev, width = tokens.shape
    rows_dev = vis_dev * time_dev
    inner = w_out.shape[0]
    head_size = inner // HEADS
    flat = tokens.reshape(rows_dev, width)
    normed = layer_norm(flat, ln_gain, ln_bias)
    projected = jnp.dot(normed, w_qkv, preferred_element_type=jnp.float32).astype(jnp.bfloat16)
    scaling = head_size ** (-0.5)
    frames = lax.axis_size("frame")
    local_heads = HEADS // frames
    stacked = projected.reshape(rows_dev, 3, HEADS, head_size)
    regrouped = lax.all_to_all(stacked, "frame", split_axis=2, concat_axis=0, tiled=True)
    all_rows = regrouped.shape[0]
    query_local = regrouped[:, 0]
    key_local = regrouped[:, 1].reshape(all_rows, local_heads * head_size)
    value_local = regrouped[:, 2].reshape(all_rows, local_heads * head_size)
    counts_rep = jnp.tile(tube_count, frames)
    fold_fn = make_fold(query_local, vis_dev, time_dev, scaling)
    state = fold_fn(
        start_state(local_heads, all_rows, head_size),
        (
            lax.all_gather(key_local, "space", axis=0, tiled=True),
            lax.all_gather(value_local, "space", axis=0, tiled=True),
            lax.all_gather(counts_rep, "space", axis=0, tiled=True),
        ),
        jnp.int32(0),
    )
    best_final, total_final, accum_final = state
    attended = (accum_final / total_final[..., None]).astype(jnp.bfloat16)
    attended = jnp.transpose(attended, (1, 0, 2))
    returned = lax.all_to_all(attended, "frame", split_axis=0, concat_axis=1, tiled=True)
    attended = returned.reshape(rows_dev, inner)
    mixed = flat.astype(jnp.float32) + jnp.dot(attended, w_out, preferred_element_type=jnp.float32)
    own_live = live_mask(tube_count, vis_dev, time_dev)
    mixed = jnp.where(own_live[:, None], mixed, 0.0)
    return mixed.astype(jnp.bfloat16).reshape(vis_dev, time_dev, width)


def solution(mesh):
    frames, spaces = mesh.shape["frame"], mesh.shape["space"]
    near = max(1, 2 * HEADS // spaces)
    parts = (frames // near, near, spaces // 2, 2)

    def layer(tokens, tube_count, ln_gain, ln_bias, w_qkv, w_out):
        slots = tokens.shape[0] // spaces
        time_dev = tokens.shape[1] // frames
        rows = slots * up_to(time_dev, SUBLANES)
        pairs = 2 * w_out.shape[0] == HEADS * LANES and rows % (2 * PACK) == 0
        padded = up_to(time_dev, SUBLANES) > time_dev
        split = parts[0] == 2 and parts[1] * parts[2] == HEADS and parts[0] * near == frames
        if split and pairs and padded:
            run, over = head_per_device, Mesh(
                mesh.devices.reshape(parts), ("far", "near", "chip", "core")
            )
            frame, space = ("far", "near"), ("chip", "core")
        else:
            run, over, frame, space = on_device, mesh, "frame", "space"
        return jax.shard_map(
            run,
            mesh=over,
            in_specs=(P(space, frame, None), P(space), P(), P(), P(), P()),
            out_specs=P(space, frame, None),
            check_vma=False,
        )(tokens, tube_count, ln_gain, ln_bias, w_qkv, w_out)

    return layer
```

```python
import functools
import jax
import jax.numpy as jnp
from jax import lax
from jax.experimental import pallas as pl
from jax.experimental.pallas import tpu as pltpu
from jax.sharding import Mesh, PartitionSpec as P

HEADS = 8


EPSILON = 1e-06
NEG_FILL = -1e30
LANES = 128
SUBLANES = 8
PACK = 16
SIZE_STEP = 128
SIZE_CASES = 3
MARKS = 2
QUERY_TILE = 256
QUERY_BIG = 512
VMEM_BYTES = 20 * 2**20
VMEM_MOST = 64600000

VMEM = pl.BlockSpec(memory_space=pltpu.VMEM)
SMEM = pl.BlockSpec(memory_space=pltpu.SMEM)
SWAP = [(0, 1), (1, 0)]


def up_to(value, unit):
    return -(-value // unit) * unit


def params():
    return pltpu.CompilerParams(vmem_limit_bytes=VMEM_BYTES)


def packed_rows(count, slot_rows):
    return (count * slot_rows + PACK - 1) // PACK * PACK


def slot_of(row, slots, slot_rows):
    slot = row * 0
    for edge in range(1, slots):
        slot = slot + (row >= edge * slot_rows).astype(jnp.int32)
    return slot


def live_rows(count, rows, slot_rows, time_dev, width):
    row = lax.broadcasted_iota(jnp.int32, (rows, width), 0)
    slot = slot_of(row, rows // slot_rows, slot_rows)
    return (slot < count) & (row - slot * slot_rows < time_dev)


def one_hot(shape, slots, slot_rows, padded_dim):
    padded = lax.broadcasted_iota(jnp.int32, shape, padded_dim)
    plain = lax.broadcasted_iota(jnp.int32, shape, 1 - padded_dim)
    slot = slot_of(padded, slots, slot_rows)
    hot = plain == (padded - slot * slot_rows) * slots + slot
    return hot.astype(jnp.float32).astype(jnp.bfloat16)


def project_kernel(
    where_ref,
    count_ref,
    other_count_ref,
    x_ref,
    other_ref,
    gain_ref,
    bias_ref,
    w_hbm,
    *refs,
):
    chips = len(refs) - 5
    outs = refs[:chips]
    w_ref, query_ref, key_ref, value_ref, sems = refs[chips:]
    time_dev, slots, width = x_ref.shape
    message, lanes = outs[0].shape
    rows = message // 3
    slot_rows = rows // slots
    half = rows // 2
    head_size = lanes // 2
    scaling = head_size ** (-0.5)
    wide = w_ref.shape[2]
    core = where_ref[0]
    chip = where_ref[1]
    copies = []
    for kind in range(3):
        start = pl.multiple_of(2 * wide * kind + wide * core, wide)
        copy = pltpu.make_async_copy(
            w_hbm.at[:, pl.ds(start, wide)], w_ref.at[kind], sems.at[kind]
        )
        copy.start()
        copies.append(copy)
    hot = one_hot((rows, time_dev * slots), slots, slot_rows, 0)
    stacked = []
    for ref in (x_ref, other_ref):
        x = ref[...].astype(jnp.float32).reshape(time_dev * slots, width)
        center = x - jnp.mean(x, axis=-1, keepdims=True)
        spread = jnp.mean(center * center, axis=-1, keepdims=True)
        normed = center * lax.rsqrt(spread + EPSILON) * gain_ref[...] + bias_ref[...]
        stacked.append(
            jnp.dot(hot, normed.astype(jnp.bfloat16), preferred_element_type=jnp.float32)
        )
    rows_in = jnp.concatenate(stacked, axis=0).astype(jnp.bfloat16)
    for copy, kind, target in zip(copies, range(3), (query_ref, key_ref, value_ref)):
        copy.wait()
        target[...] = jnp.dot(rows_in, w_ref[kind], preferred_element_type=jnp.float32)
    left = lax.broadcasted_iota(jnp.int32, (rows, lanes), 1) < head_size
    left_half = left[:half]
    row_half = lax.broadcasted_iota(jnp.int32, (half, lanes), 0)
    counts = (count_ref[0], other_count_ref[0])
    flipped = lax.rem(chip, 2) == 1
    for slot in range(chips // 2):
        block = (slot + chip // 2) % (chips // 2) if chips == 4 else slot
        cols = pl.ds(pl.multiple_of(block * lanes, lanes), lanes)
        for group, count in enumerate(counts):
            base = group * rows
            key_pair = key_ref[base : base + rows, cols]
            value_pair = value_ref[base : base + rows, cols]
            live = live_rows(count, rows, slot_rows, time_dev, lanes)
            key_pair = jnp.where(live, key_pair, key_pair[0:1])
            value_pair = jnp.where(live, value_pair, 0.0)
            even = jnp.where(left, key_pair, pltpu.roll(value_pair, head_size, 1))
            odd = jnp.where(left, pltpu.roll(key_pair, head_size, 1), value_pair)
            first = jnp.where(flipped, odd, even).astype(jnp.bfloat16)
            second = jnp.where(flipped, even, odd).astype(jnp.bfloat16)
            outs[2 * slot][base : base + rows] = first
            outs[2 * slot + 1][base : base + rows] = second
            top = query_ref[base : base + half, cols] * scaling
            low = query_ref[base + half : base + rows, cols] * scaling
            even = jnp.where(left_half, top, pltpu.roll(low, head_size, 1))
            odd = jnp.where(left_half, pltpu.roll(top, head_size, 1), low)
            first = jnp.where(flipped, odd, even)
            second = jnp.where(flipped, even, odd)
            if group == 1:
                for index, mark in enumerate(counts):
                    here = (row_half == half - MARKS + index) & jnp.logical_not(left_half)
                    first = jnp.where(here, mark.astype(jnp.float32), first)
                    second = jnp.where(here, mark.astype(jnp.float32), second)
            place = 2 * rows + group * half
            outs[2 * slot][place : place + half] = first.astype(jnp.bfloat16)
            outs[2 * slot + 1][place : place + half] = second.astype(jnp.bfloat16)


def project(where, count, other_count, tokens, other_tokens, ln_gain, ln_bias, w_qkv, rows):
    width = tokens.shape[-1]
    chips = HEADS // 2
    wide = w_qkv.shape[1] // 6
    held = pltpu.VMEM((2 * rows, wide), jnp.float32)
    message = jax.ShapeDtypeStruct((3 * rows, LANES), jnp.bfloat16)
    return pl.pallas_call(
        project_kernel,
        out_shape=(message,) * chips,
        in_specs=[SMEM, SMEM, SMEM, VMEM, VMEM, VMEM, VMEM, pl.BlockSpec(memory_space=pltpu.HBM)],
        out_specs=(VMEM,) * chips,
        scratch_shapes=[
            pltpu.VMEM((3, width, wide), w_qkv.dtype),
            held,
            held,
            held,
            pltpu.SemaphoreType.DMA((3,)),
        ],
        compiler_params=pltpu.CompilerParams(vmem_limit_bytes=VMEM_MOST),
        cost_estimate=pl.CostEstimate(
            flops=2 * rows * w_qkv.size, bytes_accessed=w_qkv.size, transcendentals=0
        ),
        name="project",
    )(
        where,
        count,
        other_count,
        tokens,
        other_tokens,
        ln_gain.reshape(1, width),
        ln_bias.reshape(1, width),
        w_qkv,
    )


def source_counts(ref):
    message = ref.shape[0]
    tail = ref[message - PACK : message].astype(jnp.float32)
    return [
        jnp.max(tail[PACK - MARKS + index : PACK - MARKS + index + 1, LANES // 2 :]).astype(jnp.int32)
        for index in range(MARKS)
    ]


def case_kernel(slot_rows, least, cases, *refs):
    case_ref = refs[-1]
    total = jnp.int32(0)
    for ref in refs[:-1]:
        for count in source_counts(ref):
            total = total + packed_rows(count, slot_rows)
    case_ref[0] = jnp.clip((total - least + SIZE_STEP - 1) // SIZE_STEP, 0, cases - 1)


def choose_case(got, slot_rows, least, cases):
    message, lanes = got[0].shape
    tail = pl.BlockSpec((PACK, lanes), lambda step: (message // PACK - 1, 0))
    return pl.pallas_call(
        functools.partial(case_kernel, slot_rows, least, cases),
        grid=(1,),
        out_shape=jax.ShapeDtypeStruct((1,), jnp.int32),
        in_specs=[tail] * len(got),
        out_specs=SMEM,
        compiler_params=params(),
        name="choose",
    )(*got)[0]


def pack_kernel(slot_rows, time_dev, *refs):
    got_refs = refs[:-7]
    early_ref, late_ref, live_ref, query_ref, start_ref, kv_room, live_room = refs[-7:]
    message, lanes = got_refs[0].shape
    rows = message // 3
    half = rows // 2
    head_size = lanes // 2
    size = live_ref.shape[0]
    lane = lax.broadcasted_iota(jnp.int32, (PACK, lanes), 1)
    first = got_refs[0][0:PACK].astype(jnp.float32)[0:1]
    fill = jnp.where(lane < head_size, jnp.broadcast_to(first, (PACK, lanes)), 0.0)
    fill = fill.astype(jnp.bfloat16)
    blank = jnp.zeros((PACK, lanes), jnp.bfloat16)
    for start in range(0, size, PACK):
        kv_room[start : start + PACK] = fill
        live_room[start : start + PACK] = blank
    for start in range(0, query_ref.shape[0], PACK):
        query_ref[start : start + PACK] = blank
    left = lax.broadcasted_iota(jnp.int32, (half, lanes), 1) < head_size
    start = jnp.int32(0)
    for index, ref in enumerate(got_refs):
        for group, count in enumerate(source_counts(ref)):
            start_ref[MARKS * index + group] = start
            place = pl.ds(pl.multiple_of(start, PACK), rows)
            kv_room[place] = ref[group * rows : (group + 1) * rows]
            live = live_rows(count, rows, slot_rows, time_dev, lanes)
            live_room[place] = live.astype(jnp.float32).astype(jnp.bfloat16)
            base = 2 * rows + group * half
            pair = ref[base : base + half].astype(jnp.float32)
            query_ref[pl.ds(pl.multiple_of(start, PACK), half)] = jnp.where(left, pair, 0.0).astype(
                jnp.bfloat16
            )
            query_ref[pl.ds(pl.multiple_of(start + half, PACK), half)] = jnp.where(
                left, pltpu.roll(pair, head_size, 1), 0.0
            ).astype(jnp.bfloat16)
            start = start + packed_rows(count, slot_rows)
    start_ref[MARKS * len(got_refs)] = start
    early_ref[...] = kv_room[0 : size // 2]
    late_ref[...] = kv_room[size // 2 : size]
    live_ref[...] = live_room[0:size]


def pack(got, size, slot_rows, time_dev):
    message, lanes = got[0].shape
    rows = message // 3
    sources = MARKS * len(got)
    array = lambda length: jax.ShapeDtypeStruct((length, lanes), jnp.bfloat16)
    room = pltpu.VMEM((size + rows, lanes), jnp.bfloat16)
    return pl.pallas_call(
        functools.partial(pack_kernel, slot_rows, time_dev),
        out_shape=(
            array(size // 2),
            array(size // 2),
            array(size),
            array(up_to(sources * rows, QUERY_TILE) + rows),
            jax.ShapeDtypeStruct((sources + 1,), jnp.int32),
        ),
        in_specs=[VMEM] * len(got),
        out_specs=(VMEM, VMEM, VMEM, VMEM, SMEM),
        scratch_shapes=[room, room],
        compiler_params=params(),
        name="pack",
    )(*got)


def attend_kernel(first, last, outs, *refs):
    start_ref, query_ref, live_ref, early_ref, late_ref = refs[:5]
    rest = list(refs[5:])
    side_ref = rest.pop()
    if not first:
        best_in, sum_in = rest[:2]
        rest = rest[2:]
    if last:
        sum_out = rest.pop()
        out_refs = rest
    else:
        best_out, sum_out = rest
    part, lanes = early_ref.shape
    head_size = lanes // 2
    left = lax.broadcasted_iota(jnp.int32, (part, lanes), 1) < head_size
    for index, ref in enumerate((early_ref, late_ref)):
        rows = slice(index * part, (index + 1) * part)
        side_ref[rows] = jnp.where(left, live_ref[rows], ref[...])
    total = start_ref[start_ref.shape[0] - 1]

    def chain(start, tile):
        place = pl.ds(pl.multiple_of(start, QUERY_TILE), tile)
        query = query_ref[place]
        scores = [
            lax.dot_general(
                query, ref[...], (((1,), (1,)), ((), ())), preferred_element_type=jnp.float32
            )
            for ref in (early_ref, late_ref)
        ]
        best = jnp.maximum(*[jnp.max(score, axis=-1, keepdims=True) for score in scores])
        if not first:
            before = best_in[place][:, 0:1]
            best = jnp.maximum(best, before)
        weights = [jnp.exp(score - best).astype(jnp.bfloat16) for score in scores]
        sums = sum(
            jnp.dot(
                weight,
                side_ref[index * part : (index + 1) * part],
                preferred_element_type=jnp.float32,
            )
            for index, weight in enumerate(weights)
        )
        if not first:
            sums = sums + sum_in[place] * jnp.exp(before - best)
        if last:
            sums = sums / pltpu.roll(sums, head_size, 1)
        else:
            best_out[place] = jnp.broadcast_to(best, (tile, lanes))
        sum_out[place] = sums

    def step(index, carry):
        chain(index * QUERY_BIG, QUERY_BIG)
        return carry

    bigs = (total + QUERY_BIG - QUERY_TILE - 1) // QUERY_BIG
    lax.fori_loop(0, bigs, step, 0)

    @pl.when(total > bigs * QUERY_BIG)
    def _():
        chain(bigs * QUERY_BIG, QUERY_TILE)

    if last:
        half = out_refs[0].shape[0] // MARKS
        left_half = lax.broadcasted_iota(jnp.int32, (half, lanes), 1) < head_size
        for index, ref in enumerate(out_refs):
            for group in range(MARKS):
                start = start_ref[MARKS * index + group]
                top = sum_out[pl.ds(pl.multiple_of(start, PACK), half)]
                low = sum_out[pl.ds(pl.multiple_of(start + half, PACK), half)]
                ref[group * half : (group + 1) * half] = jnp.where(
                    left_half, pltpu.roll(top, head_size, 1), low
                ).astype(jnp.bfloat16)


def run_stage(stage, stages, starts, query, live, blocks, state, half):
    part, lanes = blocks[0].shape
    queries = query.shape[0]
    outs = (starts.shape[0] - 1) // MARKS
    first, last = stage == 0, stage == stages - 1
    held = jax.ShapeDtypeStruct((queries, lanes), jnp.float32)
    scratch = [pltpu.VMEM((2 * part, lanes), jnp.bfloat16)]
    if last:
        out_shape = (jax.ShapeDtypeStruct((MARKS * half, lanes), jnp.bfloat16),) * outs
        scratch = [pltpu.VMEM((queries, lanes), jnp.float32)] + scratch
    else:
        out_shape = (held, held)
    return pl.pallas_call(
        functools.partial(attend_kernel, first, last, outs),
        out_shape=out_shape,
        in_specs=[SMEM] + [VMEM] * (4 + len(state)),
        out_specs=(VMEM,) * len(out_shape),
        scratch_shapes=scratch,
        input_output_aliases={} if first or last else {5: 0, 6: 1},
        compiler_params=params(),
        cost_estimate=pl.CostEstimate(
            flops=16 * part * part * lanes, bytes_accessed=part * lanes * 16, transcendentals=0
        ),
        name="attend" + str(stage),
    )(starts, query, live, *blocks, *state)


def tie(value, *after):
    return lax.optimization_barrier((value, *after))


def attend_size(size, slot_rows, time_dev, *got):
    half = got[0].shape[0] // 6
    early, late, live, query, starts = pack(got, size, slot_rows, time_dev)
    far_early = lax.ppermute(early, "far", SWAP)
    far_late = lax.ppermute(late, "far", SWAP)
    near_early = lax.ppermute(early, "near", SWAP)
    near_late = lax.ppermute(late, "near", SWAP)
    run = lambda stage, blocks, state: run_stage(
        stage, 4, starts, query, live, blocks, state, half
    )
    state = run(0, (early, late), ())
    near_early, near_late, *state = tie(near_early, near_late, *state)
    state = run(1, (near_early, near_late), state)
    far_early, *state = tie(far_early, *state)
    both_early = lax.ppermute(far_early, "near", SWAP)
    both_late = lax.ppermute(far_late, "near", SWAP)
    state = run(2, (far_early, far_late), state)
    both_early, both_late, *state = tie(both_early, both_late, *state)
    return run(3, (both_early, both_late), state)


def mix_kernel(where_ref, count_ref, other_ref, x_ref, w_ref, *refs):
    got_refs = refs[:-2]
    out_ref, held_ref = refs[-2:]
    chips = len(got_refs)
    half, lanes = other_ref.shape[0] // chips, other_ref.shape[1]
    time_dev, slots, width = x_ref.shape
    slot_rows = 2 * half // slots
    head_size = lanes // 2
    core = where_ref[0]
    chip = where_ref[1]
    flipped = lax.rem(chip, 2) == 1
    left = lax.broadcasted_iota(jnp.int32, (half, lanes), 1) < head_size
    live = live_rows(count_ref[0], 2 * half, slot_rows, time_dev, lanes)
    for slot in range(chips // 2):
        block = (slot + chip // 2) % (chips // 2) if chips == 4 else slot
        for side in range(2):
            if side == 0:
                owner = core
                first = got_refs[2 * slot][0:half]
                second = got_refs[2 * slot + 1][0:half]
            else:
                owner = 1 - core
                first = other_ref[2 * slot * half : (2 * slot + 1) * half]
                second = other_ref[(2 * slot + 1) * half : (2 * slot + 2) * half]
            first = first.astype(jnp.float32)
            second = second.astype(jnp.float32)
            even = jnp.where(flipped, second, first)
            odd = jnp.where(flipped, first, second)
            top = jnp.where(left, even, pltpu.roll(odd, head_size, 1))
            low = jnp.where(left, pltpu.roll(even, head_size, 1), odd)
            pair = jnp.where(live, jnp.concatenate([top, low], axis=0), 0.0)
            place = pl.multiple_of((owner * (chips // 2) + block) * lanes, lanes)
            held_ref[:, pl.ds(place, lanes)] = pair.astype(jnp.bfloat16)
    hot = one_hot((time_dev * slots, 2 * half), slots, slot_rows, 1)
    attended = jnp.dot(hot, held_ref[...], preferred_element_type=jnp.float32).astype(jnp.bfloat16)
    mixed = jnp.dot(attended, w_ref[...], preferred_element_type=jnp.float32)
    full = x_ref[...].astype(jnp.float32) + mixed.reshape(time_dev, slots, width)
    slot = lax.broadcasted_iota(jnp.int32, full.shape, 1)
    out_ref[...] = jnp.where(slot < count_ref[0], full, 0.0).astype(jnp.bfloat16)


def mix(where, count, got, other, tokens, w_out):
    half, lanes = got[0].shape[0] // MARKS, got[0].shape[1]
    return pl.pallas_call(
        mix_kernel,
        out_shape=jax.ShapeDtypeStruct(tokens.shape, jnp.bfloat16),
        in_specs=[SMEM, SMEM] + [VMEM] * (3 + len(got)),
        out_specs=VMEM,
        scratch_shapes=[pltpu.VMEM((2 * half, w_out.shape[0]), jnp.bfloat16)],
        compiler_params=params(),
        cost_estimate=pl.CostEstimate(
            flops=4 * half * w_out.size, bytes_accessed=2 * w_out.size, transcendentals=0
        ),
        name="mix",
    )(where, count, other, tokens, w_out, *got)


def spread(arrays, chips):
    return [arrays[0]] + [
        lax.ppermute(arrays[hop], "chip", [(i, i ^ hop) for i in range(chips)])
        for hop in range(1, chips)
    ]


def head_per_device(tokens, tube_count, ln_gain, ln_bias, w_qkv, w_out):
    slots, time_dev, width = tokens.shape
    slot_rows = up_to(time_dev, SUBLANES)
    rows = slots * slot_rows
    half = rows // 2
    chips = lax.axis_size("chip")
    where = jnp.stack([lax.axis_index("core"), lax.axis_index("chip")]).astype(jnp.int32)
    by_time = jnp.transpose(tokens, (1, 0, 2))
    other_tokens = lax.ppermute(by_time, "core", SWAP)
    other_count = lax.ppermute(tube_count, "core", SWAP)
    messages = project(
        where, tube_count, other_count, by_time, other_tokens, ln_gain, ln_bias, w_qkv, rows
    )
    got = spread(messages, chips)
    least = up_to((HEADS - 1) * up_to(slot_rows, PACK) + rows, SIZE_STEP) + SIZE_STEP
    most = up_to((HEADS - 1) * rows + up_to(slot_rows, PACK), SIZE_STEP)
    sizes = list(range(least, most, SIZE_STEP))[:SIZE_CASES] + [most]
    case = choose_case(got, slot_rows, least, len(sizes))
    branches = [functools.partial(attend_size, size, slot_rows, time_dev) for size in sizes]
    returned = lax.switch(case, branches, *got)
    back = spread(returned, chips)
    other = lax.ppermute(jnp.concatenate([b[half:] for b in back], axis=0), "core", SWAP)
    mixed = mix(where, tube_count, back, other, by_time, w_out)
    return jnp.transpose(mixed, (1, 0, 2))


def layer_norm(flat, ln_gain, ln_bias):
    values32 = flat.astype(jnp.float32)
    center = values32 - jnp.mean(values32, axis=-1, keepdims=True)
    spread = jnp.mean(center * center, axis=-1, keepdims=True)
    return (center * lax.rsqrt(spread + EPSILON) * ln_gain + ln_bias).astype(jnp.bfloat16)


def live_mask(counts, slots_dev, time_dev):
    slot_ids = jnp.arange(slots_dev)[None, :, None]
    marks = jnp.broadcast_to(
        slot_ids < counts[:, None, None], (counts.shape[0], slots_dev, time_dev)
    )
    return marks.reshape(-1)


def attend(carry, query_heads, key_block, value_block, live_keys, scaling):
    best_now, total_now, accum = carry
    heads = query_heads.shape[1]
    key_heads = key_block.reshape(key_block.shape[0], heads, -1)
    value_heads = value_block.reshape(value_block.shape[0], heads, -1)
    scores = (
        jnp.einsum("qhd,khd->hqk", query_heads, key_heads, preferred_element_type=jnp.float32)
        * scaling
    )
    scores = jnp.where(live_keys[None, None, :], scores, NEG_FILL)
    best_next = jnp.maximum(best_now, jnp.max(scores, axis=-1))
    fading = jnp.exp(best_now - best_next)
    weights = jnp.exp(scores - best_next[..., None])
    total_next = total_now * fading + jnp.sum(weights, axis=-1)
    accum = accum * fading[..., None] + jnp.einsum(
        "hqk,khd->hqd",
        weights.astype(jnp.bfloat16),
        value_heads,
        preferred_element_type=jnp.float32,
    )
    return (best_next, total_next, accum)


def make_fold(query_heads, vis_dev, time_dev, scaling):
    rows_dev = vis_dev * time_dev

    def fold_masked(carry, piece, start):
        key_all, value_all, count_all = piece
        width_in = key_all.shape[1]
        shards = count_all.shape[0]
        group = 1
        for unused_bit in range(6):
            if shards % (group * 2) == 0 and group * rows_dev < 2048:
                group = group * 2
        blocks = shards // group
        key_groups = key_all.reshape(blocks, group * rows_dev, width_in)
        value_groups = value_all.reshape(blocks, group * rows_dev, width_in)
        count_groups = count_all.reshape(blocks, group)

        def step_group(state, item):
            key_group, value_group, count_group = item
            marks = live_mask(count_group, vis_dev, time_dev)
            return (attend(state, query_heads, key_group, value_group, marks, scaling), None)

        carry, unused = lax.scan(step_group, carry, (key_groups, value_groups, count_groups))
        return carry

    return fold_masked


def start_state(heads, rows, head_size):
    return (
        jnp.full((heads, rows), NEG_FILL, jnp.float32),
        jnp.zeros((heads, rows), jnp.float32),
        jnp.zeros((heads, rows, head_size), jnp.float32),
    )


def on_device(tokens, tube_count, ln_gain, ln_bias, w_qkv, w_out):
    vis_dev, time_dev, width = tokens.shape
    rows_dev = vis_dev * time_dev
    inner = w_out.shape[0]
    head_size = inner // HEADS
    flat = tokens.reshape(rows_dev, width)
    normed = layer_norm(flat, ln_gain, ln_bias)
    projected = jnp.dot(normed, w_qkv, preferred_element_type=jnp.float32).astype(jnp.bfloat16)
    scaling = head_size ** (-0.5)
    frames = lax.axis_size("frame")
    local_heads = HEADS // frames
    stacked = projected.reshape(rows_dev, 3, HEADS, head_size)
    regrouped = lax.all_to_all(stacked, "frame", split_axis=2, concat_axis=0, tiled=True)
    all_rows = regrouped.shape[0]
    query_local = regrouped[:, 0]
    key_local = regrouped[:, 1].reshape(all_rows, local_heads * head_size)
    value_local = regrouped[:, 2].reshape(all_rows, local_heads * head_size)
    counts_rep = jnp.tile(tube_count, frames)
    fold_fn = make_fold(query_local, vis_dev, time_dev, scaling)
    state = fold_fn(
        start_state(local_heads, all_rows, head_size),
        (
            lax.all_gather(key_local, "space", axis=0, tiled=True),
            lax.all_gather(value_local, "space", axis=0, tiled=True),
            lax.all_gather(counts_rep, "space", axis=0, tiled=True),
        ),
        jnp.int32(0),
    )
    best_final, total_final, accum_final = state
    attended = (accum_final / total_final[..., None]).astype(jnp.bfloat16)
    attended = jnp.transpose(attended, (1, 0, 2))
    returned = lax.all_to_all(attended, "frame", split_axis=0, concat_axis=1, tiled=True)
    attended = returned.reshape(rows_dev, inner)
    mixed = flat.astype(jnp.float32) + jnp.dot(attended, w_out, preferred_element_type=jnp.float32)
    own_live = live_mask(tube_count, vis_dev, time_dev)
    mixed = jnp.where(own_live[:, None], mixed, 0.0)
    return mixed.astype(jnp.bfloat16).reshape(vis_dev, time_dev, width)


def solution(mesh):
    frames, spaces = mesh.shape["frame"], mesh.shape["space"]
    parts = (2, frames // 2, spaces // 2, 2)

    def layer(tokens, tube_count, ln_gain, ln_bias, w_qkv, w_out):
        slots = tokens.shape[0] // spaces
        time_dev = tokens.shape[1] // frames
        rows = slots * up_to(time_dev, SUBLANES)
        pairs = 2 * w_out.shape[0] == HEADS * LANES and rows % (2 * PACK) == 0
        padded = up_to(time_dev, SUBLANES) >= time_dev + MARKS
        split = parts[1] == 2 and parts[2] == 4 and spaces == HEADS
        if split and pairs and padded:
            run, over = head_per_device, Mesh(
                mesh.devices.reshape(parts), ("far", "near", "chip", "core")
            )
            frame, space = ("far", "near"), ("chip", "core")
        else:
            run, over, frame, space = on_device, mesh, "frame", "space"
        return jax.shard_map(
            run,
            mesh=over,
            in_specs=(P(space, frame, None), P(space), P(), P(), P(), P()),
            out_specs=P(space, frame, None),
            check_vma=False,
        )(tokens, tube_count, ln_gain, ln_bias, w_qkv, w_out)

    return layer
```

```python
import functools
import jax
import jax.numpy as jnp
from jax import lax
from jax.experimental import pallas as pl
from jax.experimental.pallas import tpu as pltpu
from jax.sharding import Mesh, PartitionSpec as P

HEADS = 8


EPSILON = 1e-06
NEG_FILL = -1e30
LANES = 128
SUBLANES = 8
PACK = 16
SIZE_STEP = 128
SIZE_CASES = 3
MARKS = 2
QUERY_TILE = 256
QUERY_BIG = 512
VMEM_BYTES = 20 * 2**20
VMEM_MOST = 64600000

VMEM = pl.BlockSpec(memory_space=pltpu.VMEM)
SMEM = pl.BlockSpec(memory_space=pltpu.SMEM)
SWAP = [(0, 1), (1, 0)]


def up_to(value, unit):
    return -(-value // unit) * unit


def params():
    return pltpu.CompilerParams(vmem_limit_bytes=VMEM_BYTES)


def packed_rows(count, slot_rows):
    return (count * slot_rows + PACK - 1) // PACK * PACK


def slot_of(row, slots, slot_rows):
    slot = row * 0
    for edge in range(1, slots):
        slot = slot + (row >= edge * slot_rows).astype(jnp.int32)
    return slot


def live_rows(count, rows, slot_rows, time_dev, width):
    row = lax.broadcasted_iota(jnp.int32, (rows, width), 0)
    slot = slot_of(row, rows // slot_rows, slot_rows)
    return (slot < count) & (row - slot * slot_rows < time_dev)


def one_hot(shape, slots, slot_rows, padded_dim):
    padded = lax.broadcasted_iota(jnp.int32, shape, padded_dim)
    plain = lax.broadcasted_iota(jnp.int32, shape, 1 - padded_dim)
    slot = slot_of(padded, slots, slot_rows)
    hot = plain == (padded - slot * slot_rows) * slots + slot
    return hot.astype(jnp.float32).astype(jnp.bfloat16)


def normalise(x_ref, gain_ref, bias_ref, rows):
    time_dev, slots, width = x_ref.shape
    x = x_ref[...].astype(jnp.float32).reshape(time_dev * slots, width)
    center = x - jnp.mean(x, axis=-1, keepdims=True)
    spread = jnp.mean(center * center, axis=-1, keepdims=True)
    normed = center * lax.rsqrt(spread + EPSILON) * gain_ref[...] + bias_ref[...]
    hot = one_hot((rows, time_dev * slots), slots, rows // slots, 0)
    return jnp.dot(
        hot, normed.astype(jnp.bfloat16), preferred_element_type=jnp.float32
    ).astype(jnp.bfloat16)


def fetch_kernel(
    core_ref,
    x_hbm,
    gain_hbm,
    bias_hbm,
    w_hbm,
    rows_ref,
    gain_ref,
    bias_ref,
    w_ref,
    x_ref,
    sems,
):
    kinds, width, wide = w_ref.shape
    pairs = [(x_hbm, x_ref), (gain_hbm, gain_ref), (bias_hbm, bias_ref)]
    for kind in range(kinds):
        start = pl.multiple_of(2 * wide * kind + wide * core_ref[0], wide)
        pairs.append((w_hbm.at[:, pl.ds(start, wide)], w_ref.at[kind]))
    copies = [
        pltpu.make_async_copy(source, target, sems.at[place])
        for place, (source, target) in enumerate(pairs)
    ]
    for copy in copies:
        copy.start()
    for copy in copies[:-kinds]:
        copy.wait()
    rows_ref[...] = normalise(x_ref, gain_ref, bias_ref, rows_ref.shape[0])
    for copy in copies[-kinds:]:
        copy.wait()


def fetch(core, tokens, ln_gain, ln_bias, w_qkv, rows):
    width = tokens.shape[-1]
    wide = w_qkv.shape[1] // 6
    gain = ln_gain.reshape(1, width)
    bias = ln_bias.reshape(1, width)
    inputs = [pltpu.with_memory_space_constraint(a, pltpu.HBM) for a in (tokens, gain, bias, w_qkv)]
    hbm = pl.BlockSpec(memory_space=pltpu.HBM)
    return pl.pallas_call(
        fetch_kernel,
        out_shape=(
            jax.ShapeDtypeStruct((rows, width), jnp.bfloat16),
            jax.ShapeDtypeStruct(gain.shape, gain.dtype),
            jax.ShapeDtypeStruct(bias.shape, bias.dtype),
            jax.ShapeDtypeStruct((3, width, wide), w_qkv.dtype),
        ),
        in_specs=[SMEM] + [hbm] * 4,
        out_specs=(VMEM,) * 4,
        scratch_shapes=[
            pltpu.VMEM(tokens.shape, tokens.dtype),
            pltpu.SemaphoreType.DMA((6,)),
        ],
        compiler_params=params(),
        cost_estimate=pl.CostEstimate(
            flops=2 * rows * w_qkv.size, bytes_accessed=w_qkv.size, transcendentals=0
        ),
        name="fetch",
    )(core, *inputs)


def project_kernel(
    chip_ref,
    count_ref,
    other_count_ref,
    rows_ref,
    other_ref,
    gain_ref,
    bias_ref,
    w_ref,
    *refs,
):
    chips = len(refs) - 3
    outs = refs[:chips]
    query_ref, key_ref, value_ref = refs[chips:]
    time_dev, slots, width = other_ref.shape
    message, lanes = outs[0].shape
    rows = message // 3
    slot_rows = rows // slots
    half = rows // 2
    head_size = lanes // 2
    scaling = head_size ** (-0.5)
    chip = chip_ref[0]
    rows_in = jnp.concatenate(
        [rows_ref[...], normalise(other_ref, gain_ref, bias_ref, rows)], axis=0
    )
    for kind, target in enumerate((query_ref, key_ref, value_ref)):
        target[...] = jnp.dot(rows_in, w_ref[kind], preferred_element_type=jnp.float32)
    left = lax.broadcasted_iota(jnp.int32, (rows, lanes), 1) < head_size
    left_half = left[:half]
    row_half = lax.broadcasted_iota(jnp.int32, (half, lanes), 0)
    counts = (count_ref[0], other_count_ref[0])
    flipped = lax.rem(chip, 2) == 1
    for slot in range(chips // 2):
        block = (slot + chip // 2) % (chips // 2) if chips == 4 else slot
        cols = pl.ds(pl.multiple_of(block * lanes, lanes), lanes)
        for group, count in enumerate(counts):
            base = group * rows
            key_pair = key_ref[base : base + rows, cols]
            value_pair = value_ref[base : base + rows, cols]
            live = live_rows(count, rows, slot_rows, time_dev, lanes)
            key_pair = jnp.where(live, key_pair, key_pair[0:1])
            value_pair = jnp.where(live, value_pair, 0.0)
            even = jnp.where(left, key_pair, pltpu.roll(value_pair, head_size, 1))
            odd = jnp.where(left, pltpu.roll(key_pair, head_size, 1), value_pair)
            first = jnp.where(flipped, odd, even).astype(jnp.bfloat16)
            second = jnp.where(flipped, even, odd).astype(jnp.bfloat16)
            outs[2 * slot][base : base + rows] = first
            outs[2 * slot + 1][base : base + rows] = second
            top = query_ref[base : base + half, cols] * scaling
            low = query_ref[base + half : base + rows, cols] * scaling
            even = jnp.where(left_half, top, pltpu.roll(low, head_size, 1))
            odd = jnp.where(left_half, pltpu.roll(top, head_size, 1), low)
            first = jnp.where(flipped, odd, even)
            second = jnp.where(flipped, even, odd)
            if group == 1:
                for index, mark in enumerate(counts):
                    here = (row_half == half - MARKS + index) & jnp.logical_not(left_half)
                    first = jnp.where(here, mark.astype(jnp.float32), first)
                    second = jnp.where(here, mark.astype(jnp.float32), second)
            place = 2 * rows + group * half
            outs[2 * slot][place : place + half] = first.astype(jnp.bfloat16)
            outs[2 * slot + 1][place : place + half] = second.astype(jnp.bfloat16)


def project(chip, count, other_count, rows_in, other_tokens, gain, bias, weights):
    chips = HEADS // 2
    rows = rows_in.shape[0]
    wide = weights.shape[-1]
    held = pltpu.VMEM((2 * rows, wide), jnp.float32)
    message = jax.ShapeDtypeStruct((3 * rows, LANES), jnp.bfloat16)
    return pl.pallas_call(
        project_kernel,
        out_shape=(message,) * chips,
        in_specs=[SMEM] * 3 + [VMEM] * 5,
        out_specs=(VMEM,) * chips,
        scratch_shapes=[held] * 3,
        compiler_params=params(),
        cost_estimate=pl.CostEstimate(
            flops=4 * rows * weights.size, bytes_accessed=2 * weights.size, transcendentals=0
        ),
        name="project",
    )(chip, count, other_count, rows_in, other_tokens, gain, bias, weights)


def source_counts(ref):
    message = ref.shape[0]
    tail = ref[message - PACK : message].astype(jnp.float32)
    return [
        jnp.max(tail[PACK - MARKS + index : PACK - MARKS + index + 1, LANES // 2 :]).astype(jnp.int32)
        for index in range(MARKS)
    ]


def case_kernel(slot_rows, least, cases, *refs):
    case_ref = refs[-1]
    total = jnp.int32(0)
    for ref in refs[:-1]:
        for count in source_counts(ref):
            total = total + packed_rows(count, slot_rows)
    case_ref[0] = jnp.clip((total - least + SIZE_STEP - 1) // SIZE_STEP, 0, cases - 1)


def choose_case(got, slot_rows, least, cases):
    message, lanes = got[0].shape
    tail = pl.BlockSpec((PACK, lanes), lambda step: (message // PACK - 1, 0))
    return pl.pallas_call(
        functools.partial(case_kernel, slot_rows, least, cases),
        grid=(1,),
        out_shape=jax.ShapeDtypeStruct((1,), jnp.int32),
        in_specs=[tail] * len(got),
        out_specs=SMEM,
        compiler_params=params(),
        name="choose",
    )(*got)[0]


def pack_kernel(slot_rows, time_dev, *refs):
    got_refs = refs[:-7]
    early_ref, late_ref, live_ref, query_ref, start_ref, kv_room, live_room = refs[-7:]
    message, lanes = got_refs[0].shape
    rows = message // 3
    half = rows // 2
    head_size = lanes // 2
    size = live_ref.shape[0]
    lane = lax.broadcasted_iota(jnp.int32, (PACK, lanes), 1)
    first = got_refs[0][0:PACK].astype(jnp.float32)[0:1]
    fill = jnp.where(lane < head_size, jnp.broadcast_to(first, (PACK, lanes)), 0.0)
    fill = fill.astype(jnp.bfloat16)
    blank = jnp.zeros((PACK, lanes), jnp.bfloat16)
    for start in range(0, size, PACK):
        kv_room[start : start + PACK] = fill
        live_room[start : start + PACK] = blank
    for start in range(0, query_ref.shape[0], PACK):
        query_ref[start : start + PACK] = blank
    left = lax.broadcasted_iota(jnp.int32, (half, lanes), 1) < head_size
    start = jnp.int32(0)
    for index, ref in enumerate(got_refs):
        for group, count in enumerate(source_counts(ref)):
            start_ref[MARKS * index + group] = start
            place = pl.ds(pl.multiple_of(start, PACK), rows)
            kv_room[place] = ref[group * rows : (group + 1) * rows]
            live = live_rows(count, rows, slot_rows, time_dev, lanes)
            live_room[place] = live.astype(jnp.float32).astype(jnp.bfloat16)
            base = 2 * rows + group * half
            pair = ref[base : base + half].astype(jnp.float32)
            query_ref[pl.ds(pl.multiple_of(start, PACK), half)] = jnp.where(left, pair, 0.0).astype(
                jnp.bfloat16
            )
            query_ref[pl.ds(pl.multiple_of(start + half, PACK), half)] = jnp.where(
                left, pltpu.roll(pair, head_size, 1), 0.0
            ).astype(jnp.bfloat16)
            start = start + packed_rows(count, slot_rows)
    start_ref[MARKS * len(got_refs)] = start
    early_ref[...] = kv_room[0 : size // 2]
    late_ref[...] = kv_room[size // 2 : size]
    live_ref[...] = live_room[0:size]


def pack(got, size, slot_rows, time_dev):
    message, lanes = got[0].shape
    rows = message // 3
    sources = MARKS * len(got)
    array = lambda length: jax.ShapeDtypeStruct((length, lanes), jnp.bfloat16)
    room = pltpu.VMEM((size + rows, lanes), jnp.bfloat16)
    return pl.pallas_call(
        functools.partial(pack_kernel, slot_rows, time_dev),
        out_shape=(
            array(size // 2),
            array(size // 2),
            array(size),
            array(up_to(sources * rows, QUERY_TILE) + rows),
            jax.ShapeDtypeStruct((sources + 1,), jnp.int32),
        ),
        in_specs=[VMEM] * len(got),
        out_specs=(VMEM, VMEM, VMEM, VMEM, SMEM),
        scratch_shapes=[room, room],
        compiler_params=params(),
        name="pack",
    )(*got)


def attend_kernel(first, last, outs, *refs):
    start_ref, query_ref, live_ref, early_ref, late_ref = refs[:5]
    rest = list(refs[5:])
    side_ref = rest.pop()
    if not first:
        best_in, sum_in = rest[:2]
        rest = rest[2:]
    if last:
        sum_out = rest.pop()
        out_ref = rest[0]
    else:
        best_out, sum_out = rest
    part, lanes = early_ref.shape
    head_size = lanes // 2
    left = lax.broadcasted_iota(jnp.int32, (part, lanes), 1) < head_size
    for index, ref in enumerate((early_ref, late_ref)):
        rows = slice(index * part, (index + 1) * part)
        side_ref[rows] = jnp.where(left, live_ref[rows], ref[...])
    total = start_ref[start_ref.shape[0] - 1]

    def chain(start, tile):
        place = pl.ds(pl.multiple_of(start, QUERY_TILE), tile)
        query = query_ref[place]
        scores = [
            lax.dot_general(
                query, ref[...], (((1,), (1,)), ((), ())), preferred_element_type=jnp.float32
            )
            for ref in (early_ref, late_ref)
        ]
        best = jnp.maximum(*[jnp.max(score, axis=-1, keepdims=True) for score in scores])
        if not first:
            before = best_in[place][:, 0:1]
            best = jnp.maximum(best, before)
        weights = [jnp.exp(score - best).astype(jnp.bfloat16) for score in scores]
        sums = sum(
            jnp.dot(
                weight,
                side_ref[index * part : (index + 1) * part],
                preferred_element_type=jnp.float32,
            )
            for index, weight in enumerate(weights)
        )
        if not first:
            sums = sums + sum_in[place] * jnp.exp(before - best)
        if last:
            sums = sums / pltpu.roll(sums, head_size, 1)
        else:
            best_out[place] = jnp.broadcast_to(best, (tile, lanes))
        sum_out[place] = sums

    def step(index, carry):
        chain(index * QUERY_BIG, QUERY_BIG)
        return carry

    bigs = (total + QUERY_BIG - QUERY_TILE - 1) // QUERY_BIG
    lax.fori_loop(0, bigs, step, 0)

    @pl.when(total > bigs * QUERY_BIG)
    def _():
        chain(bigs * QUERY_BIG, QUERY_TILE)

    if last:
        half = out_ref.shape[1] // MARKS
        left_half = lax.broadcasted_iota(jnp.int32, (half, lanes), 1) < head_size
        for source in range(MARKS * out_ref.shape[0]):
            start = start_ref[source]
            top = sum_out[pl.ds(pl.multiple_of(start, PACK), half)]
            low = sum_out[pl.ds(pl.multiple_of(start + half, PACK), half)]
            base = source % MARKS * half
            out_ref[source // MARKS, base : base + half] = jnp.where(
                left_half, pltpu.roll(top, head_size, 1), low
            ).astype(jnp.bfloat16)


def run_stage(stage, stages, starts, query, live, blocks, state, half):
    part, lanes = blocks[0].shape
    queries = query.shape[0]
    outs = (starts.shape[0] - 1) // MARKS
    first, last = stage == 0, stage == stages - 1
    held = jax.ShapeDtypeStruct((queries, lanes), jnp.float32)
    scratch = [pltpu.VMEM((2 * part, lanes), jnp.bfloat16)]
    if last:
        out_shape = (jax.ShapeDtypeStruct((outs, MARKS * half, lanes), jnp.bfloat16),)
        scratch = [pltpu.VMEM((queries, lanes), jnp.float32)] + scratch
    else:
        out_shape = (held, held)
    return pl.pallas_call(
        functools.partial(attend_kernel, first, last, outs),
        out_shape=out_shape,
        in_specs=[SMEM] + [VMEM] * (4 + len(state)),
        out_specs=(VMEM,) * len(out_shape),
        scratch_shapes=scratch,
        input_output_aliases={} if first or last else {5: 0, 6: 1},
        compiler_params=params(),
        cost_estimate=pl.CostEstimate(
            flops=16 * part * part * lanes, bytes_accessed=part * lanes * 16, transcendentals=0
        ),
        name="attend" + str(stage),
    )(starts, query, live, *blocks, *state)


def tie(value, *after):
    return lax.optimization_barrier((value, *after))


def attend_size(size, slot_rows, time_dev, *got):
    half = got[0].shape[0] // 6
    early, late, live, query, starts = pack(got, size, slot_rows, time_dev)
    far_early = lax.ppermute(early, "far", SWAP)
    far_late = lax.ppermute(late, "far", SWAP)
    near_early = lax.ppermute(early, "near", SWAP)
    near_late = lax.ppermute(late, "near", SWAP)
    run = lambda stage, blocks, state: run_stage(
        stage, 4, starts, query, live, blocks, state, half
    )
    state = run(0, (early, late), ())
    near_early, near_late, *state = tie(near_early, near_late, *state)
    state = run(1, (near_early, near_late), state)
    far_early, *state = tie(far_early, *state)
    both_early = lax.ppermute(far_early, "near", SWAP)
    both_late = lax.ppermute(far_late, "near", SWAP)
    state = run(2, (far_early, far_late), state)
    both_early, both_late, *state = tie(both_early, both_late, *state)
    return run(3, (both_early, both_late), state)[0]


def mix_kernel(core_ref, chip_ref, count_ref, got_ref, other_ref, x_ref, w_ref, out_ref, held_ref):
    chips, half, lanes = got_ref.shape
    time_dev, slots, width = x_ref.shape
    slot_rows = 2 * half // slots
    head_size = lanes // 2
    core = core_ref[0]
    chip = chip_ref[0]
    flipped = lax.rem(chip, 2) == 1
    left = lax.broadcasted_iota(jnp.int32, (half, lanes), 1) < head_size
    live = live_rows(count_ref[0], 2 * half, slot_rows, time_dev, lanes)
    for slot in range(chips // 2):
        block = (slot + chip // 2) % (chips // 2) if chips == 4 else slot
        for side in range(2):
            if side == 0:
                owner = core
                first = got_ref[2 * slot]
                second = got_ref[2 * slot + 1]
            else:
                owner = 1 - core
                first = other_ref[2 * slot]
                second = other_ref[2 * slot + 1]
            first = first.astype(jnp.float32)
            second = second.astype(jnp.float32)
            even = jnp.where(flipped, second, first)
            odd = jnp.where(flipped, first, second)
            top = jnp.where(left, even, pltpu.roll(odd, head_size, 1))
            low = jnp.where(left, pltpu.roll(even, head_size, 1), odd)
            pair = jnp.where(live, jnp.concatenate([top, low], axis=0), 0.0)
            place = pl.multiple_of((owner * (chips // 2) + block) * lanes, lanes)
            held_ref[:, pl.ds(place, lanes)] = pair.astype(jnp.bfloat16)
    hot = one_hot((time_dev * slots, 2 * half), slots, slot_rows, 1)
    attended = jnp.dot(hot, held_ref[...], preferred_element_type=jnp.float32).astype(jnp.bfloat16)
    mixed = jnp.dot(attended, w_ref[...], preferred_element_type=jnp.float32)
    full = x_ref[...].astype(jnp.float32) + mixed.reshape(time_dev, slots, width)
    slot = lax.broadcasted_iota(jnp.int32, full.shape, 1)
    out_ref[...] = jnp.where(slot < count_ref[0], full, 0.0).astype(jnp.bfloat16)


def mix(core, chip, count, got, other, tokens, w_out):
    half, lanes = got.shape[1:]
    return pl.pallas_call(
        mix_kernel,
        out_shape=jax.ShapeDtypeStruct(tokens.shape, jnp.bfloat16),
        in_specs=[SMEM] * 3 + [VMEM] * 4,
        out_specs=VMEM,
        scratch_shapes=[pltpu.VMEM((2 * half, w_out.shape[0]), jnp.bfloat16)],
        compiler_params=params(),
        cost_estimate=pl.CostEstimate(
            flops=4 * half * w_out.size, bytes_accessed=2 * w_out.size, transcendentals=0
        ),
        name="mix",
    )(core, chip, count, got, other, tokens, w_out)


def spread(arrays, chips):
    return [arrays[0]] + [
        lax.ppermute(arrays[hop], "chip", [(i, i ^ hop) for i in range(chips)])
        for hop in range(1, chips)
    ]


def head_per_device(tokens, tube_count, ln_gain, ln_bias, w_qkv, w_out):
    slots, time_dev, width = tokens.shape
    slot_rows = up_to(time_dev, SUBLANES)
    rows = slots * slot_rows
    half = rows // 2
    chips = lax.axis_size("chip")
    core = lax.axis_index("core").reshape(1)
    chip = lax.axis_index("chip").reshape(1)
    by_time = jnp.transpose(tokens, (1, 0, 2))
    other_tokens = lax.ppermute(by_time, "core", SWAP)
    other_count = lax.ppermute(tube_count, "core", SWAP)
    fetched = fetch(core, by_time, ln_gain, ln_bias, w_qkv, rows)
    rows_in, gain, bias, weights = fetched
    messages = project(
        chip, tube_count, other_count, rows_in, other_tokens, gain, bias, weights
    )
    got = spread(messages, chips)
    least = up_to((HEADS - 1) * up_to(slot_rows, PACK) + rows, SIZE_STEP) + SIZE_STEP
    most = up_to((HEADS - 1) * rows + up_to(slot_rows, PACK), SIZE_STEP)
    sizes = list(range(least, most, SIZE_STEP))[:SIZE_CASES] + [most]
    case = choose_case(got, slot_rows, least, len(sizes))
    branches = [functools.partial(attend_size, size, slot_rows, time_dev) for size in sizes]
    returned = lax.switch(case, branches, *got)
    back = jnp.stack(spread(returned, chips))
    other = lax.ppermute(back[:, half:], "core", SWAP)
    mixed = mix(core, chip, tube_count, back[:, :half], other, by_time, w_out)
    return jnp.transpose(mixed, (1, 0, 2))


def layer_norm(flat, ln_gain, ln_bias):
    values32 = flat.astype(jnp.float32)
    center = values32 - jnp.mean(values32, axis=-1, keepdims=True)
    spread = jnp.mean(center * center, axis=-1, keepdims=True)
    return (center * lax.rsqrt(spread + EPSILON) * ln_gain + ln_bias).astype(jnp.bfloat16)


def live_mask(counts, slots_dev, time_dev):
    slot_ids = jnp.arange(slots_dev)[None, :, None]
    marks = jnp.broadcast_to(
        slot_ids < counts[:, None, None], (counts.shape[0], slots_dev, time_dev)
    )
    return marks.reshape(-1)


def attend(carry, query_heads, key_block, value_block, live_keys, scaling):
    best_now, total_now, accum = carry
    heads = query_heads.shape[1]
    key_heads = key_block.reshape(key_block.shape[0], heads, -1)
    value_heads = value_block.reshape(value_block.shape[0], heads, -1)
    scores = (
        jnp.einsum("qhd,khd->hqk", query_heads, key_heads, preferred_element_type=jnp.float32)
        * scaling
    )
    scores = jnp.where(live_keys[None, None, :], scores, NEG_FILL)
    best_next = jnp.maximum(best_now, jnp.max(scores, axis=-1))
    fading = jnp.exp(best_now - best_next)
    weights = jnp.exp(scores - best_next[..., None])
    total_next = total_now * fading + jnp.sum(weights, axis=-1)
    accum = accum * fading[..., None] + jnp.einsum(
        "hqk,khd->hqd",
        weights.astype(jnp.bfloat16),
        value_heads,
        preferred_element_type=jnp.float32,
    )
    return (best_next, total_next, accum)


def make_fold(query_heads, vis_dev, time_dev, scaling):
    rows_dev = vis_dev * time_dev

    def fold_masked(carry, piece, start):
        key_all, value_all, count_all = piece
        width_in = key_all.shape[1]
        shards = count_all.shape[0]
        group = 1
        for unused_bit in range(6):
            if shards % (group * 2) == 0 and group * rows_dev < 2048:
                group = group * 2
        blocks = shards // group
        key_groups = key_all.reshape(blocks, group * rows_dev, width_in)
        value_groups = value_all.reshape(blocks, group * rows_dev, width_in)
        count_groups = count_all.reshape(blocks, group)

        def step_group(state, item):
            key_group, value_group, count_group = item
            marks = live_mask(count_group, vis_dev, time_dev)
            return (attend(state, query_heads, key_group, value_group, marks, scaling), None)

        carry, unused = lax.scan(step_group, carry, (key_groups, value_groups, count_groups))
        return carry

    return fold_masked


def start_state(heads, rows, head_size):
    return (
        jnp.full((heads, rows), NEG_FILL, jnp.float32),
        jnp.zeros((heads, rows), jnp.float32),
        jnp.zeros((heads, rows, head_size), jnp.float32),
    )


def on_device(tokens, tube_count, ln_gain, ln_bias, w_qkv, w_out):
    vis_dev, time_dev, width = tokens.shape
    rows_dev = vis_dev * time_dev
    inner = w_out.shape[0]
    head_size = inner // HEADS
    flat = tokens.reshape(rows_dev, width)
    normed = layer_norm(flat, ln_gain, ln_bias)
    projected = jnp.dot(normed, w_qkv, preferred_element_type=jnp.float32).astype(jnp.bfloat16)
    scaling = head_size ** (-0.5)
    frames = lax.axis_size("frame")
    local_heads = HEADS // frames
    stacked = projected.reshape(rows_dev, 3, HEADS, head_size)
    regrouped = lax.all_to_all(stacked, "frame", split_axis=2, concat_axis=0, tiled=True)
    all_rows = regrouped.shape[0]
    query_local = regrouped[:, 0]
    key_local = regrouped[:, 1].reshape(all_rows, local_heads * head_size)
    value_local = regrouped[:, 2].reshape(all_rows, local_heads * head_size)
    counts_rep = jnp.tile(tube_count, frames)
    fold_fn = make_fold(query_local, vis_dev, time_dev, scaling)
    state = fold_fn(
        start_state(local_heads, all_rows, head_size),
        (
            lax.all_gather(key_local, "space", axis=0, tiled=True),
            lax.all_gather(value_local, "space", axis=0, tiled=True),
            lax.all_gather(counts_rep, "space", axis=0, tiled=True),
        ),
        jnp.int32(0),
    )
    best_final, total_final, accum_final = state
    attended = (accum_final / total_final[..., None]).astype(jnp.bfloat16)
    attended = jnp.transpose(attended, (1, 0, 2))
    returned = lax.all_to_all(attended, "frame", split_axis=0, concat_axis=1, tiled=True)
    attended = returned.reshape(rows_dev, inner)
    mixed = flat.astype(jnp.float32) + jnp.dot(attended, w_out, preferred_element_type=jnp.float32)
    own_live = live_mask(tube_count, vis_dev, time_dev)
    mixed = jnp.where(own_live[:, None], mixed, 0.0)
    return mixed.astype(jnp.bfloat16).reshape(vis_dev, time_dev, width)


def solution(mesh):
    frames, spaces = mesh.shape["frame"], mesh.shape["space"]
    parts = (2, frames // 2, spaces // 2, 2)

    def layer(tokens, tube_count, ln_gain, ln_bias, w_qkv, w_out):
        slots = tokens.shape[0] // spaces
        time_dev = tokens.shape[1] // frames
        rows = slots * up_to(time_dev, SUBLANES)
        pairs = 2 * w_out.shape[0] == HEADS * LANES and rows % (2 * PACK) == 0
        padded = up_to(time_dev, SUBLANES) >= time_dev + MARKS
        split = parts[1] == 2 and parts[2] == 4 and spaces == HEADS
        if split and pairs and padded:
            run, over = head_per_device, Mesh(
                mesh.devices.reshape(parts), ("far", "near", "chip", "core")
            )
            frame, space = ("far", "near"), ("chip", "core")
        else:
            run, over, frame, space = on_device, mesh, "frame", "space"
        return jax.shard_map(
            run,
            mesh=over,
            in_specs=(P(space, frame, None), P(space), P(), P(), P(), P()),
            out_specs=P(space, frame, None),
            check_vma=False,
        )(tokens, tube_count, ln_gain, ln_bias, w_qkv, w_out)

    return layer
```

```python
import functools
import jax
import jax.numpy as jnp
from jax import lax
from jax.experimental import pallas as pl
from jax.experimental.pallas import tpu as pltpu
from jax.sharding import Mesh, PartitionSpec as P

HEADS = 8


EPSILON = 1e-06
NEG_FILL = -1e30
LANES = 128
SUBLANES = 8
PACK = 16
SIZE_STEP = 128
SIZE_CASES = 3
MARKS = 2
QUERY_TILE = 256
QUERY_BIG = 512
VMEM_BYTES = 20 * 2**20

VMEM = pl.BlockSpec(memory_space=pltpu.VMEM)
SMEM = pl.BlockSpec(memory_space=pltpu.SMEM)
SWAP = [(0, 1), (1, 0)]


def up_to(value, unit):
    return -(-value // unit) * unit


def params():
    return pltpu.CompilerParams(vmem_limit_bytes=VMEM_BYTES)


def packed_rows(count, slot_rows):
    return (count * slot_rows + PACK - 1) // PACK * PACK


def slot_of(row, slots, slot_rows):
    slot = row * 0
    for edge in range(1, slots):
        slot = slot + (row >= edge * slot_rows).astype(jnp.int32)
    return slot


def live_rows(count, rows, slot_rows, time_dev, width):
    row = lax.broadcasted_iota(jnp.int32, (rows, width), 0)
    slot = slot_of(row, rows // slot_rows, slot_rows)
    return (slot < count) & (row - slot * slot_rows < time_dev)


def one_hot(shape, slots, slot_rows, padded_dim):
    padded = lax.broadcasted_iota(jnp.int32, shape, padded_dim)
    plain = lax.broadcasted_iota(jnp.int32, shape, 1 - padded_dim)
    slot = slot_of(padded, slots, slot_rows)
    hot = plain == (padded - slot * slot_rows) * slots + slot
    return hot.astype(jnp.float32).astype(jnp.bfloat16)


def normalise(x_ref, gain_ref, bias_ref, rows):
    time_dev, slots, width = x_ref.shape
    x = x_ref[...].astype(jnp.float32).reshape(time_dev * slots, width)
    center = x - jnp.mean(x, axis=-1, keepdims=True)
    spread = jnp.mean(center * center, axis=-1, keepdims=True)
    normed = center * lax.rsqrt(spread + EPSILON) * gain_ref[...] + bias_ref[...]
    hot = one_hot((rows, time_dev * slots), slots, rows // slots, 0)
    return jnp.dot(
        hot, normed.astype(jnp.bfloat16), preferred_element_type=jnp.float32
    ).astype(jnp.bfloat16)


def fetch_kernel(
    core_ref,
    x_hbm,
    gain_hbm,
    bias_hbm,
    w_hbm,
    rows_ref,
    gain_ref,
    bias_ref,
    w_ref,
    x_ref,
    sems,
):
    kinds, _, wide = w_ref.shape
    pairs = [(x_hbm, x_ref), (gain_hbm, gain_ref), (bias_hbm, bias_ref)]
    for kind in range(kinds):
        start = pl.multiple_of(2 * wide * kind + wide * core_ref[0], wide)
        pairs.append((w_hbm.at[:, pl.ds(start, wide)], w_ref.at[kind]))
    copies = [
        pltpu.make_async_copy(source, target, sems.at[place])
        for place, (source, target) in enumerate(pairs)
    ]
    for copy in copies:
        copy.start()
    for copy in copies[:-kinds]:
        copy.wait()
    rows_ref[...] = normalise(x_ref, gain_ref, bias_ref, rows_ref.shape[0])
    for copy in copies[-kinds:]:
        copy.wait()


def fetch(core, tokens, ln_gain, ln_bias, w_qkv, rows):
    width = tokens.shape[-1]
    wide = w_qkv.shape[1] // 6
    gain = ln_gain.reshape(1, width)
    bias = ln_bias.reshape(1, width)
    inputs = [pltpu.with_memory_space_constraint(a, pltpu.HBM) for a in (tokens, gain, bias, w_qkv)]
    hbm = pl.BlockSpec(memory_space=pltpu.HBM)
    return pl.pallas_call(
        fetch_kernel,
        out_shape=(
            jax.ShapeDtypeStruct((rows, width), jnp.bfloat16),
            jax.ShapeDtypeStruct(gain.shape, gain.dtype),
            jax.ShapeDtypeStruct(bias.shape, bias.dtype),
            jax.ShapeDtypeStruct((3, width, wide), w_qkv.dtype),
        ),
        in_specs=[SMEM] + [hbm] * 4,
        out_specs=(VMEM,) * 4,
        scratch_shapes=[
            pltpu.VMEM(tokens.shape, tokens.dtype),
            pltpu.SemaphoreType.DMA((6,)),
        ],
        compiler_params=params(),
        cost_estimate=pl.CostEstimate(
            flops=2 * rows * w_qkv.size, bytes_accessed=w_qkv.size, transcendentals=0
        ),
        name="fetch",
    )(core, *inputs)


def project_kernel(
    chip_ref,
    count_ref,
    other_count_ref,
    rows_ref,
    other_ref,
    gain_ref,
    bias_ref,
    w_ref,
    *refs,
):
    chips = len(refs) - 3
    outs = refs[:chips]
    query_ref, key_ref, value_ref = refs[chips:]
    time_dev, slots, _ = other_ref.shape
    message, lanes = outs[0].shape
    rows = message // 3
    slot_rows = rows // slots
    half = rows // 2
    head_size = lanes // 2
    scaling = head_size ** (-0.5)
    chip = chip_ref[0]
    rows_in = jnp.concatenate(
        [rows_ref[...], normalise(other_ref, gain_ref, bias_ref, rows)], axis=0
    )
    for kind, target in enumerate((query_ref, key_ref, value_ref)):
        target[...] = jnp.dot(rows_in, w_ref[kind], preferred_element_type=jnp.float32)
    left = lax.broadcasted_iota(jnp.int32, (rows, lanes), 1) < head_size
    left_half = left[:half]
    row_half = lax.broadcasted_iota(jnp.int32, (half, lanes), 0)
    counts = (count_ref[0], other_count_ref[0])
    flipped = lax.rem(chip, 2) == 1
    for slot in range(chips // 2):
        block = (slot + chip // 2) % (chips // 2) if chips == 4 else slot
        cols = pl.ds(pl.multiple_of(block * lanes, lanes), lanes)
        for group, count in enumerate(counts):
            base = group * rows
            key_pair = key_ref[base : base + rows, cols]
            value_pair = value_ref[base : base + rows, cols]
            live = live_rows(count, rows, slot_rows, time_dev, lanes)
            key_pair = jnp.where(live, key_pair, key_pair[0:1])
            value_pair = jnp.where(live, value_pair, 0.0)
            even = jnp.where(left, key_pair, pltpu.roll(value_pair, head_size, 1))
            odd = jnp.where(left, pltpu.roll(key_pair, head_size, 1), value_pair)
            first = jnp.where(flipped, odd, even).astype(jnp.bfloat16)
            second = jnp.where(flipped, even, odd).astype(jnp.bfloat16)
            outs[2 * slot][base : base + rows] = first
            outs[2 * slot + 1][base : base + rows] = second
            top = query_ref[base : base + half, cols] * scaling
            low = query_ref[base + half : base + rows, cols] * scaling
            even = jnp.where(left_half, top, pltpu.roll(low, head_size, 1))
            odd = jnp.where(left_half, pltpu.roll(top, head_size, 1), low)
            first = jnp.where(flipped, odd, even)
            second = jnp.where(flipped, even, odd)
            if group == 1:
                for index, mark in enumerate(counts):
                    here = (row_half == half - MARKS + index) & jnp.logical_not(left_half)
                    first = jnp.where(here, mark.astype(jnp.float32), first)
                    second = jnp.where(here, mark.astype(jnp.float32), second)
            place = 2 * rows + group * half
            outs[2 * slot][place : place + half] = first.astype(jnp.bfloat16)
            outs[2 * slot + 1][place : place + half] = second.astype(jnp.bfloat16)


def project(chip, count, other_count, rows_in, other_tokens, gain, bias, weights):
    chips = HEADS // 2
    rows = rows_in.shape[0]
    wide = weights.shape[-1]
    held = pltpu.VMEM((2 * rows, wide), jnp.float32)
    message = jax.ShapeDtypeStruct((3 * rows, LANES), jnp.bfloat16)
    return pl.pallas_call(
        project_kernel,
        out_shape=(message,) * chips,
        in_specs=[SMEM] * 3 + [VMEM] * 5,
        out_specs=(VMEM,) * chips,
        scratch_shapes=[held] * 3,
        compiler_params=params(),
        cost_estimate=pl.CostEstimate(
            flops=4 * rows * weights.size, bytes_accessed=2 * weights.size, transcendentals=0
        ),
        name="project",
    )(chip, count, other_count, rows_in, other_tokens, gain, bias, weights)


def source_counts(ref):
    message = ref.shape[0]
    tail = ref[message - PACK : message].astype(jnp.float32)
    return [
        jnp.max(tail[PACK - MARKS + index : PACK - MARKS + index + 1, LANES // 2 :]).astype(jnp.int32)
        for index in range(MARKS)
    ]


def pack_kernel(slot_rows, time_dev, least, cases, *refs):
    got_refs = refs[:-5]
    kv_room, live_room, query_ref, start_ref, case_ref = refs[-5:]
    message, lanes = got_refs[0].shape
    rows = message // 3
    half = rows // 2
    head_size = lanes // 2
    size = live_room.shape[0] - rows
    lane = lax.broadcasted_iota(jnp.int32, (PACK, lanes), 1)
    first = got_refs[0][0:PACK].astype(jnp.float32)[0:1]
    fill = jnp.where(lane < head_size, jnp.broadcast_to(first, (PACK, lanes)), 0.0)
    fill = fill.astype(jnp.bfloat16)
    blank = jnp.zeros((PACK, lanes), jnp.bfloat16)
    for start in range(0, size, PACK):
        kv_room[start : start + PACK] = fill
        live_room[start : start + PACK] = blank
    for start in range(0, query_ref.shape[0], PACK):
        query_ref[start : start + PACK] = blank
    left = lax.broadcasted_iota(jnp.int32, (half, lanes), 1) < head_size
    start = jnp.int32(0)
    for index, ref in enumerate(got_refs):
        for group, count in enumerate(source_counts(ref)):
            start_ref[MARKS * index + group] = start
            place = pl.ds(pl.multiple_of(start, PACK), rows)
            kv_room[place] = ref[group * rows : (group + 1) * rows]
            live = live_rows(count, rows, slot_rows, time_dev, lanes)
            live_room[place] = live.astype(jnp.float32).astype(jnp.bfloat16)
            base = 2 * rows + group * half
            pair = ref[base : base + half].astype(jnp.float32)
            query_ref[pl.ds(pl.multiple_of(start, PACK), half)] = jnp.where(left, pair, 0.0).astype(
                jnp.bfloat16
            )
            query_ref[pl.ds(pl.multiple_of(start + half, PACK), half)] = jnp.where(
                left, pltpu.roll(pair, head_size, 1), 0.0
            ).astype(jnp.bfloat16)
            start = start + packed_rows(count, slot_rows)
    start_ref[MARKS * len(got_refs)] = start
    case_ref[0] = jnp.clip((start - least + SIZE_STEP - 1) // SIZE_STEP, 0, cases - 1)


def pack(got, sizes, slot_rows, time_dev):
    message, lanes = got[0].shape
    rows = message // 3
    sources = MARKS * len(got)
    room = jax.ShapeDtypeStruct((sizes[-1] + rows, lanes), jnp.bfloat16)
    queries = up_to(sources * rows, QUERY_TILE) + rows
    return pl.pallas_call(
        functools.partial(pack_kernel, slot_rows, time_dev, sizes[0], len(sizes)),
        out_shape=(
            room,
            room,
            jax.ShapeDtypeStruct((queries, lanes), jnp.bfloat16),
            jax.ShapeDtypeStruct((sources + 1,), jnp.int32),
            jax.ShapeDtypeStruct((1,), jnp.int32),
        ),
        in_specs=[VMEM] * len(got),
        out_specs=(VMEM, VMEM, VMEM, SMEM, SMEM),
        compiler_params=params(),
        name="pack",
    )(*got)


def attend_kernel(first, last, lengths, *refs):
    start_ref, query_ref, live_ref = refs[:3]
    block_refs = refs[3 : 3 + len(lengths)]
    rest = list(refs[3 + len(lengths) :])
    side_ref = rest.pop()
    if not first:
        best_in, sum_in = rest[:2]
        rest = rest[2:]
    if last:
        sum_out = rest.pop()
        out_ref = rest[0]
    else:
        best_out, sum_out = rest
    lanes = live_ref.shape[1]
    head_size = lanes // 2
    blocks = []
    begin = 0
    for length, ref in zip(lengths, block_refs):
        left = lax.broadcasted_iota(jnp.int32, (length, lanes), 1) < head_size
        rows = slice(begin, begin + length)
        side_ref[rows] = jnp.where(left, live_ref[rows], ref[0:length])
        blocks.append((ref, length, rows))
        begin = begin + length
    total = start_ref[start_ref.shape[0] - 1]

    def chain(start, tile):
        place = pl.ds(pl.multiple_of(start, QUERY_TILE), tile)
        query = query_ref[place]
        scores = [
            lax.dot_general(
                query,
                ref[0:length],
                (((1,), (1,)), ((), ())),
                preferred_element_type=jnp.float32,
            )
            for ref, length, rows in blocks
        ]
        best = functools.reduce(
            jnp.maximum, [jnp.max(score, axis=-1, keepdims=True) for score in scores]
        )
        if not first:
            before = best_in[place][:, 0:1]
            best = jnp.maximum(best, before)
        sums = sum(
            jnp.dot(
                jnp.exp(score - best).astype(jnp.bfloat16),
                side_ref[rows],
                preferred_element_type=jnp.float32,
            )
            for score, (ref, length, rows) in zip(scores, blocks)
        )
        if not first:
            sums = sums + sum_in[place] * jnp.exp(before - best)
        if last:
            sums = sums / pltpu.roll(sums, head_size, 1)
        else:
            best_out[place] = jnp.broadcast_to(best, (tile, lanes))
        sum_out[place] = sums

    def step(index, carry):
        chain(index * QUERY_BIG, QUERY_BIG)
        return carry

    bigs = (total + QUERY_BIG - QUERY_TILE - 1) // QUERY_BIG
    lax.fori_loop(0, bigs, step, 0)

    @pl.when(total > bigs * QUERY_BIG)
    def _():
        chain(bigs * QUERY_BIG, QUERY_TILE)

    if last:
        half = out_ref.shape[1] // MARKS
        left_half = lax.broadcasted_iota(jnp.int32, (half, lanes), 1) < head_size
        for source in range(MARKS * out_ref.shape[0]):
            start = start_ref[source]
            top = sum_out[pl.ds(pl.multiple_of(start, PACK), half)]
            low = sum_out[pl.ds(pl.multiple_of(start + half, PACK), half)]
            base = source % MARKS * half
            out_ref[source // MARKS, base : base + half] = jnp.where(
                left_half, pltpu.roll(top, head_size, 1), low
            ).astype(jnp.bfloat16)


def run_stage(stage, stages, starts, query, live, blocks, lengths, state, half):
    lanes = query.shape[1]
    queries = query.shape[0]
    outs = (starts.shape[0] - 1) // MARKS
    first, last = stage == 0, stage == stages - 1
    held = jax.ShapeDtypeStruct((queries, lanes), jnp.float32)
    keys = sum(lengths)
    scratch = [pltpu.VMEM((keys, lanes), jnp.bfloat16)]
    if last:
        out_shape = (jax.ShapeDtypeStruct((outs, MARKS * half, lanes), jnp.bfloat16),)
        scratch = [pltpu.VMEM((queries, lanes), jnp.float32)] + scratch
    else:
        out_shape = (held, held)
    places = 3 + len(blocks)
    return pl.pallas_call(
        functools.partial(attend_kernel, first, last, lengths),
        out_shape=out_shape,
        in_specs=[SMEM] + [VMEM] * (2 + len(blocks) + len(state)),
        out_specs=(VMEM,) * len(out_shape),
        scratch_shapes=scratch,
        input_output_aliases={} if first or last else {places: 0, places + 1: 1},
        compiler_params=params(),
        cost_estimate=pl.CostEstimate(
            flops=4 * keys * keys * lanes, bytes_accessed=keys * lanes * 8, transcendentals=0
        ),
    )(starts, query, live, *blocks, *state)


def tie(value, *after):
    return lax.optimization_barrier((value, *after))


def attend_size(size, half, *packed):
    return exchange_and_attend(size, half, *packed)


def exchange_and_attend(size, half, kv, live, query, starts):
    late = up_to(size // 4, SIZE_STEP // 2)
    early = size - late
    first, second, both = tie(kv[:early], kv[early:size], kv[:size])
    far_early = lax.ppermute(first, "far", SWAP)
    far_late = lax.ppermute(second, "far", SWAP)
    near = lax.ppermute(both, "near", SWAP)
    run = lambda stage, blocks, lengths, state: run_stage(
        stage, 4, starts, query, live, blocks, lengths, state, half
    )
    state = run(0, (both,), (size,), ())
    near, *state = tie(near, *state)
    state = run(1, (near,), (size,), state)
    far_early, *state = tie(far_early, *state)
    both_early = lax.ppermute(far_early, "near", SWAP)
    both_late = lax.ppermute(far_late, "near", SWAP)
    state = run(2, (far_early, far_late), (early, late), state)
    both_early, both_late, *state = tie(both_early, both_late, *state)
    return run(3, (both_early, both_late), (early, late), state)[0]


def mix_kernel(core_ref, chip_ref, count_ref, got_ref, other_ref, x_ref, w_ref, out_ref, held_ref):
    chips, half, lanes = got_ref.shape
    time_dev, slots, width = x_ref.shape
    slot_rows = 2 * half // slots
    head_size = lanes // 2
    core = core_ref[0]
    chip = chip_ref[0]
    flipped = lax.rem(chip, 2) == 1
    left = lax.broadcasted_iota(jnp.int32, (half, lanes), 1) < head_size
    live = live_rows(count_ref[0], 2 * half, slot_rows, time_dev, lanes)
    for slot in range(chips // 2):
        block = (slot + chip // 2) % (chips // 2) if chips == 4 else slot
        for side in range(2):
            if side == 0:
                owner = core
                first = got_ref[2 * slot]
                second = got_ref[2 * slot + 1]
            else:
                owner = 1 - core
                first = other_ref[2 * slot]
                second = other_ref[2 * slot + 1]
            first = first.astype(jnp.float32)
            second = second.astype(jnp.float32)
            even = jnp.where(flipped, second, first)
            odd = jnp.where(flipped, first, second)
            top = jnp.where(left, even, pltpu.roll(odd, head_size, 1))
            low = jnp.where(left, pltpu.roll(even, head_size, 1), odd)
            pair = jnp.where(live, jnp.concatenate([top, low], axis=0), 0.0)
            place = pl.multiple_of((owner * (chips // 2) + block) * lanes, lanes)
            held_ref[:, pl.ds(place, lanes)] = pair.astype(jnp.bfloat16)
    hot = one_hot((time_dev * slots, 2 * half), slots, slot_rows, 1)
    attended = jnp.dot(hot, held_ref[...], preferred_element_type=jnp.float32).astype(jnp.bfloat16)
    mixed = jnp.dot(attended, w_ref[...], preferred_element_type=jnp.float32)
    full = x_ref[...].astype(jnp.float32) + mixed.reshape(time_dev, slots, width)
    slot = lax.broadcasted_iota(jnp.int32, full.shape, 1)
    out_ref[...] = jnp.where(slot < count_ref[0], full, 0.0).astype(jnp.bfloat16)


def mix(core, chip, count, got, other, tokens, w_out):
    half, _ = got.shape[1:]
    return pl.pallas_call(
        mix_kernel,
        out_shape=jax.ShapeDtypeStruct(tokens.shape, jnp.bfloat16),
        in_specs=[SMEM] * 3 + [VMEM] * 4,
        out_specs=VMEM,
        scratch_shapes=[pltpu.VMEM((2 * half, w_out.shape[0]), jnp.bfloat16)],
        compiler_params=params(),
        cost_estimate=pl.CostEstimate(
            flops=4 * half * w_out.size, bytes_accessed=2 * w_out.size, transcendentals=0
        ),
        name="mix",
    )(core, chip, count, got, other, tokens, w_out)


def spread(arrays, chips):
    return [arrays[0]] + [
        lax.ppermute(arrays[hop], "chip", [(i, i ^ hop) for i in range(chips)])
        for hop in range(1, chips)
    ]


def head_per_device(tokens, tube_count, ln_gain, ln_bias, w_qkv, w_out):
    slots, time_dev, _ = tokens.shape
    slot_rows = up_to(time_dev, SUBLANES)
    rows = slots * slot_rows
    half = rows // 2
    chips = lax.axis_size("chip")
    core = lax.axis_index("core").reshape(1)
    chip = lax.axis_index("chip").reshape(1)
    by_time = jnp.transpose(tokens, (1, 0, 2))
    other_tokens = lax.ppermute(by_time, "core", SWAP)
    other_count = lax.ppermute(tube_count, "core", SWAP)
    fetched = fetch(core, by_time, ln_gain, ln_bias, w_qkv, rows)
    rows_in, gain, bias, weights = fetched
    messages = project(
        chip, tube_count, other_count, rows_in, other_tokens, gain, bias, weights
    )
    got = spread(messages, chips)
    least = up_to((HEADS - 1) * up_to(slot_rows, PACK) + rows, SIZE_STEP) + SIZE_STEP
    most = up_to((HEADS - 1) * rows + up_to(slot_rows, PACK), SIZE_STEP)
    sizes = list(range(least, most, SIZE_STEP))[:SIZE_CASES] + [most]
    kv, live, query, starts, case = pack(got, sizes, slot_rows, time_dev)
    branches = [functools.partial(attend_size, size, half) for size in sizes]
    returned = lax.switch(case[0], branches, kv, live, query, starts)
    back = jnp.stack(spread(returned, chips))
    other = lax.ppermute(back[:, half:], "core", SWAP)
    mixed = mix(core, chip, tube_count, back[:, :half], other, by_time, w_out)
    return jnp.transpose(mixed, (1, 0, 2))


def layer_norm(flat, ln_gain, ln_bias):
    values32 = flat.astype(jnp.float32)
    center = values32 - jnp.mean(values32, axis=-1, keepdims=True)
    spread = jnp.mean(center * center, axis=-1, keepdims=True)
    return (center * lax.rsqrt(spread + EPSILON) * ln_gain + ln_bias).astype(jnp.bfloat16)


def live_mask(counts, slots_dev, time_dev):
    slot_ids = jnp.arange(slots_dev)[None, :, None]
    marks = jnp.broadcast_to(
        slot_ids < counts[:, None, None], (counts.shape[0], slots_dev, time_dev)
    )
    return marks.reshape(-1)


def attend(carry, query_heads, key_block, value_block, live_keys, scaling):
    best_now, total_now, accum = carry
    heads = query_heads.shape[1]
    key_heads = key_block.reshape(key_block.shape[0], heads, -1)
    value_heads = value_block.reshape(value_block.shape[0], heads, -1)
    scores = (
        jnp.einsum("qhd,khd->hqk", query_heads, key_heads, preferred_element_type=jnp.float32)
        * scaling
    )
    scores = jnp.where(live_keys[None, None, :], scores, NEG_FILL)
    best_next = jnp.maximum(best_now, jnp.max(scores, axis=-1))
    fading = jnp.exp(best_now - best_next)
    weights = jnp.exp(scores - best_next[..., None])
    total_next = total_now * fading + jnp.sum(weights, axis=-1)
    accum = accum * fading[..., None] + jnp.einsum(
        "hqk,khd->hqd",
        weights.astype(jnp.bfloat16),
        value_heads,
        preferred_element_type=jnp.float32,
    )
    return (best_next, total_next, accum)


def make_fold(query_heads, vis_dev, time_dev, scaling):
    rows_dev = vis_dev * time_dev

    def fold_masked(carry, piece, start):
        key_all, value_all, count_all = piece
        width_in = key_all.shape[1]
        shards = count_all.shape[0]
        group = 1
        for _ in range(6):
            if shards % (group * 2) == 0 and group * rows_dev < 2048:
                group = group * 2
        blocks = shards // group
        key_groups = key_all.reshape(blocks, group * rows_dev, width_in)
        value_groups = value_all.reshape(blocks, group * rows_dev, width_in)
        count_groups = count_all.reshape(blocks, group)

        def step_group(state, item):
            key_group, value_group, count_group = item
            marks = live_mask(count_group, vis_dev, time_dev)
            return (attend(state, query_heads, key_group, value_group, marks, scaling), None)

        carry, _ = lax.scan(step_group, carry, (key_groups, value_groups, count_groups))
        return carry

    return fold_masked


def start_state(heads, rows, head_size):
    return (
        jnp.full((heads, rows), NEG_FILL, jnp.float32),
        jnp.zeros((heads, rows), jnp.float32),
        jnp.zeros((heads, rows, head_size), jnp.float32),
    )


def on_device(tokens, tube_count, ln_gain, ln_bias, w_qkv, w_out):
    vis_dev, time_dev, width = tokens.shape
    rows_dev = vis_dev * time_dev
    inner = w_out.shape[0]
    head_size = inner // HEADS
    flat = tokens.reshape(rows_dev, width)
    normed = layer_norm(flat, ln_gain, ln_bias)
    projected = jnp.dot(normed, w_qkv, preferred_element_type=jnp.float32).astype(jnp.bfloat16)
    scaling = head_size ** (-0.5)
    frames = lax.axis_size("frame")
    local_heads = HEADS // frames
    stacked = projected.reshape(rows_dev, 3, HEADS, head_size)
    regrouped = lax.all_to_all(stacked, "frame", split_axis=2, concat_axis=0, tiled=True)
    all_rows = regrouped.shape[0]
    query_local = regrouped[:, 0]
    key_local = regrouped[:, 1].reshape(all_rows, local_heads * head_size)
    value_local = regrouped[:, 2].reshape(all_rows, local_heads * head_size)
    counts_rep = jnp.tile(tube_count, frames)
    fold_fn = make_fold(query_local, vis_dev, time_dev, scaling)
    state = fold_fn(
        start_state(local_heads, all_rows, head_size),
        (
            lax.all_gather(key_local, "space", axis=0, tiled=True),
            lax.all_gather(value_local, "space", axis=0, tiled=True),
            lax.all_gather(counts_rep, "space", axis=0, tiled=True),
        ),
        jnp.int32(0),
    )
    _, total_final, accum_final = state
    attended = (accum_final / total_final[..., None]).astype(jnp.bfloat16)
    attended = jnp.transpose(attended, (1, 0, 2))
    returned = lax.all_to_all(attended, "frame", split_axis=0, concat_axis=1, tiled=True)
    attended = returned.reshape(rows_dev, inner)
    mixed = flat.astype(jnp.float32) + jnp.dot(attended, w_out, preferred_element_type=jnp.float32)
    own_live = live_mask(tube_count, vis_dev, time_dev)
    mixed = jnp.where(own_live[:, None], mixed, 0.0)
    return mixed.astype(jnp.bfloat16).reshape(vis_dev, time_dev, width)


def solution(mesh):
    frames, spaces = mesh.shape["frame"], mesh.shape["space"]
    parts = (2, frames // 2, spaces // 2, 2)

    def layer(tokens, tube_count, ln_gain, ln_bias, w_qkv, w_out):
        slots = tokens.shape[0] // spaces
        time_dev = tokens.shape[1] // frames
        rows = slots * up_to(time_dev, SUBLANES)
        pairs = 2 * w_out.shape[0] == HEADS * LANES and rows % (2 * PACK) == 0
        padded = up_to(time_dev, SUBLANES) >= time_dev + MARKS
        split = parts[1] == 2 and parts[2] == 4 and spaces == HEADS
        if split and pairs and padded:
            run, over = head_per_device, Mesh(
                mesh.devices.reshape(parts), ("far", "near", "chip", "core")
            )
            frame, space = ("far", "near"), ("chip", "core")
        else:
            run, over, frame, space = on_device, mesh, "frame", "space"
        mapped = jax.shard_map(
            run,
            mesh=over,
            in_specs=(P(space, frame, None), P(space), P(), P(), P(), P()),
            out_specs=P(space, frame, None),
            check_vma=False,
        )
        return mapped(tokens, tube_count, ln_gain, ln_bias, w_qkv, w_out)

    return layer
```

```python
import functools
import jax
import jax.numpy as jnp
from jax import lax
from jax.experimental import pallas as pl
from jax.experimental.pallas import tpu as pltpu
from jax.sharding import Mesh, PartitionSpec as P

HEADS = 8


EPSILON = 1e-06
NEG_FILL = -1e30
LANES = 128
SUBLANES = 8
PACK = 16
SIZE_STEP = 128
MARKS = 2
SIZES_ABOVE = (128, 192, 320, 448)
SCORE_BOUND = 60.0
QUERY_SMALL = 128
QUERY_TILE = 256
QUERY_BIG = 512
VMEM_BYTES = 20 * 2**20

VMEM = pl.BlockSpec(memory_space=pltpu.VMEM)
SMEM = pl.BlockSpec(memory_space=pltpu.SMEM)
SWAP = [(0, 1), (1, 0)]


def up_to(value, unit):
    return -(-value // unit) * unit


def params():
    return pltpu.CompilerParams(vmem_limit_bytes=VMEM_BYTES)


def packed_rows(count, slot_rows):
    return count * slot_rows


def slot_of(row, slots, slot_rows):
    slot = row * 0
    for edge in range(1, slots):
        slot = slot + (row >= edge * slot_rows).astype(jnp.int32)
    return slot


def live_rows(count, rows, slot_rows, time_dev, width):
    row = lax.broadcasted_iota(jnp.int32, (rows, width), 0)
    slot = slot_of(row, rows // slot_rows, slot_rows)
    return (slot < count) & (row - slot * slot_rows < time_dev)


def one_hot(shape, slots, slot_rows, padded_dim):
    padded = lax.broadcasted_iota(jnp.int32, shape, padded_dim)
    plain = lax.broadcasted_iota(jnp.int32, shape, 1 - padded_dim)
    slot = slot_of(padded, slots, slot_rows)
    hot = plain == (padded - slot * slot_rows) * slots + slot
    return hot.astype(jnp.float32).astype(jnp.bfloat16)


def scalar(ref):
    return jnp.max(ref[...].astype(jnp.float32)).astype(jnp.int32)


def normalise(x_ref, gain_ref, bias_ref, rows):
    time_dev, slots, width = x_ref.shape
    x = x_ref[...].astype(jnp.float32).reshape(time_dev * slots, width)
    center = x - jnp.mean(x, axis=-1, keepdims=True)
    spread = jnp.mean(center * center, axis=-1, keepdims=True)
    normed = center * lax.rsqrt(spread + EPSILON) * gain_ref[...] + bias_ref[...]
    hot = one_hot((rows, time_dev * slots), slots, rows // slots, 0)
    return jnp.dot(
        hot, normed.astype(jnp.bfloat16), preferred_element_type=jnp.float32
    ).astype(jnp.bfloat16)


def fetch_kernel(
    core_ref,
    x_hbm,
    gain_hbm,
    bias_hbm,
    w_hbm,
    rows_ref,
    gain_ref,
    bias_ref,
    w_ref,
    x_ref,
    sems,
):
    kinds, _, wide = w_ref.shape
    pairs = [(x_hbm, x_ref), (gain_hbm, gain_ref), (bias_hbm, bias_ref)]
    for kind in range(kinds):
        start = pl.multiple_of(2 * wide * kind + wide * core_ref[0], wide)
        pairs.append((w_hbm.at[:, pl.ds(start, wide)], w_ref.at[kind]))
    copies = [
        pltpu.make_async_copy(source, target, sems.at[place])
        for place, (source, target) in enumerate(pairs)
    ]
    for copy in copies:
        copy.start()
    for copy in copies[:-kinds]:
        copy.wait()
    rows_ref[...] = normalise(x_ref, gain_ref, bias_ref, rows_ref.shape[0])
    for copy in copies[-kinds:]:
        copy.wait()


def fetch(core, tokens, ln_gain, ln_bias, w_qkv, rows):
    width = tokens.shape[-1]
    wide = w_qkv.shape[1] // 6
    gain = ln_gain.reshape(1, width)
    bias = ln_bias.reshape(1, width)
    inputs = [pltpu.with_memory_space_constraint(a, pltpu.HBM) for a in (tokens, gain, bias, w_qkv)]
    hbm = pl.BlockSpec(memory_space=pltpu.HBM)
    return pl.pallas_call(
        fetch_kernel,
        out_shape=(
            jax.ShapeDtypeStruct((rows, width), jnp.bfloat16),
            jax.ShapeDtypeStruct(gain.shape, gain.dtype),
            jax.ShapeDtypeStruct(bias.shape, bias.dtype),
            jax.ShapeDtypeStruct((3, width, wide), w_qkv.dtype),
        ),
        in_specs=[SMEM] + [hbm] * 4,
        out_specs=(VMEM,) * 4,
        scratch_shapes=[
            pltpu.VMEM(tokens.shape, tokens.dtype),
            pltpu.SemaphoreType.DMA((6,)),
        ],
        compiler_params=params(),
        cost_estimate=pl.CostEstimate(
            flops=2 * rows * w_qkv.size, bytes_accessed=w_qkv.size, transcendentals=0
        ),
        name="fetch",
    )(core, *inputs)


def project_kernel(
    chip_ref,
    count_ref,
    other_count_ref,
    rows_ref,
    other_ref,
    gain_ref,
    bias_ref,
    w_ref,
    *refs,
):
    chips = len(refs) - 3
    outs = refs[:chips]
    query_ref, key_ref, value_ref = refs[chips:]
    time_dev, slots, _ = other_ref.shape
    message, lanes = outs[0].shape
    rows = message // 3
    slot_rows = rows // slots
    half = rows // 2
    head_size = lanes // 2
    scaling = head_size ** (-0.5)
    chip = chip_ref[0]
    rows_in = jnp.concatenate(
        [rows_ref[...], normalise(other_ref, gain_ref, bias_ref, rows)], axis=0
    )
    for kind, target in enumerate((query_ref, key_ref, value_ref)):
        target[...] = jnp.dot(rows_in, w_ref[kind], preferred_element_type=jnp.float32)
    left = lax.broadcasted_iota(jnp.int32, (rows, lanes), 1) < head_size
    left_half = left[:half]
    row_half = lax.broadcasted_iota(jnp.int32, (half, lanes), 0)
    counts = (scalar(count_ref), scalar(other_count_ref))
    flipped = lax.rem(chip, 2) == 1
    for slot in range(chips // 2):
        block = (slot + chip // 2) % (chips // 2) if chips == 4 else slot
        cols = pl.ds(pl.multiple_of(block * lanes, lanes), lanes)
        for group, count in enumerate(counts):
            base = group * rows
            key_pair = key_ref[base : base + rows, cols]
            value_pair = value_ref[base : base + rows, cols]
            live = live_rows(count, rows, slot_rows, time_dev, lanes)
            key_pair = jnp.where(live, key_pair, key_pair[0:1])
            value_pair = jnp.where(live, value_pair, 0.0)
            even = jnp.where(left, key_pair, pltpu.roll(value_pair, head_size, 1))
            odd = jnp.where(left, pltpu.roll(key_pair, head_size, 1), value_pair)
            first = jnp.where(flipped, odd, even).astype(jnp.bfloat16)
            second = jnp.where(flipped, even, odd).astype(jnp.bfloat16)
            outs[2 * slot][base : base + rows] = first
            outs[2 * slot + 1][base : base + rows] = second
            top = query_ref[base : base + half, cols] * scaling
            low = query_ref[base + half : base + rows, cols] * scaling
            even = jnp.where(left_half, top, pltpu.roll(low, head_size, 1))
            odd = jnp.where(left_half, pltpu.roll(top, head_size, 1), low)
            first = jnp.where(flipped, odd, even)
            second = jnp.where(flipped, even, odd)
            if group == 1:
                for index, mark in enumerate(counts):
                    here = (row_half == half - MARKS + index) & jnp.logical_not(left_half)
                    first = jnp.where(here, mark.astype(jnp.float32), first)
                    second = jnp.where(here, mark.astype(jnp.float32), second)
            place = 2 * rows + group * half
            outs[2 * slot][place : place + half] = first.astype(jnp.bfloat16)
            outs[2 * slot + 1][place : place + half] = second.astype(jnp.bfloat16)


def project(chip, count, other_count, rows_in, other_tokens, gain, bias, weights):
    chips = HEADS // 2
    rows = rows_in.shape[0]
    wide = weights.shape[-1]
    held = pltpu.VMEM((2 * rows, wide), jnp.float32)
    message = jax.ShapeDtypeStruct((3 * rows, LANES), jnp.bfloat16)
    return pl.pallas_call(
        project_kernel,
        out_shape=(message,) * chips,
        in_specs=[SMEM] + [VMEM] * 7,
        out_specs=(VMEM,) * chips,
        scratch_shapes=[held] * 3,
        compiler_params=params(),
        cost_estimate=pl.CostEstimate(
            flops=4 * rows * weights.size, bytes_accessed=2 * weights.size, transcendentals=0
        ),
        name="project",
    )(chip, count, other_count, rows_in, other_tokens, gain, bias, weights)


def source_counts(ref):
    message = ref.shape[0]
    tail = ref[message - PACK : message].astype(jnp.float32)
    return [
        jnp.max(tail[PACK - MARKS + index : PACK - MARKS + index + 1, LANES // 2 :]).astype(jnp.int32)
        for index in range(MARKS)
    ]


def pack_kernel(slot_rows, time_dev, sizes, *refs):
    got_refs = refs[:-5]
    kv_room, live_room, query_ref, start_ref, case_ref = refs[-5:]
    message, lanes = got_refs[0].shape
    rows = message // 3
    half = rows // 2
    head_size = lanes // 2
    size = live_room.shape[0] - rows
    lane = lax.broadcasted_iota(jnp.int32, (PACK, lanes), 1)
    first = got_refs[0][0:PACK].astype(jnp.float32)[0:1]
    fill = jnp.where(lane < head_size, jnp.broadcast_to(first, (PACK, lanes)), 0.0)
    fill = fill.astype(jnp.bfloat16)
    blank = jnp.zeros((PACK, lanes), jnp.bfloat16)
    for start in range(0, size, PACK):
        kv_room[start : start + PACK] = fill
        live_room[start : start + PACK] = blank
    for start in range(0, query_ref.shape[0], PACK):
        query_ref[start : start + PACK] = blank
    left = lax.broadcasted_iota(jnp.int32, (half, lanes), 1) < head_size
    plain = left & (lax.broadcasted_iota(jnp.int32, (half, lanes), 0) < half - MARKS)
    start = jnp.int32(0)
    for index, ref in enumerate(got_refs):
        for group, count in enumerate(source_counts(ref)):
            start_ref[MARKS * index + group] = start
            place = pl.ds(pl.multiple_of(start, SUBLANES), rows)
            kv_room[place] = ref[group * rows : (group + 1) * rows]
            live = live_rows(count, rows, slot_rows, time_dev, lanes)
            live_room[place] = live.astype(jnp.float32).astype(jnp.bfloat16)
            base = 2 * rows + group * half
            pair = ref[base : base + half].astype(jnp.float32)
            query_ref[pl.ds(pl.multiple_of(start, SUBLANES), half)] = jnp.where(left, pair, 0.0).astype(
                jnp.bfloat16
            )
            query_ref[pl.ds(pl.multiple_of(start + half, SUBLANES), half)] = jnp.where(
                plain, pltpu.roll(pair, head_size, 1), 0.0
            ).astype(jnp.bfloat16)
            start = start + packed_rows(count, slot_rows)
    start_ref[MARKS * len(got_refs)] = start
    case_ref[0] = sum((start > size).astype(jnp.int32) for size in sizes[:-1])


def pack(got, sizes, slot_rows, time_dev):
    message, lanes = got[0].shape
    rows = message // 3
    sources = MARKS * len(got)
    room = jax.ShapeDtypeStruct((sizes[-1] + rows, lanes), jnp.bfloat16)
    queries = up_to(sources * rows, QUERY_TILE) + rows
    return pl.pallas_call(
        functools.partial(pack_kernel, slot_rows, time_dev, tuple(sizes)),
        out_shape=(
            room,
            room,
            jax.ShapeDtypeStruct((queries, lanes), jnp.bfloat16),
            jax.ShapeDtypeStruct((sources + 1,), jnp.int32),
            jax.ShapeDtypeStruct((1,), jnp.int32),
        ),
        in_specs=[VMEM] * len(got),
        out_specs=(VMEM, VMEM, VMEM, SMEM, SMEM),
        compiler_params=params(),
        name="pack",
    )(*got)


def attend_kernel(first, last, size, lengths, *refs):
    start_ref, query_ref, live_ref = refs[:3]
    block_refs = refs[3 : 3 + len(lengths)]
    rest = list(refs[3 + len(lengths) :])
    side_ref = rest.pop()
    if not first:
        best_in, sum_in, flag_in = rest[:3]
        rest = rest[3:]
    if last:
        sum_out = rest.pop()
        out_ref = rest[0]
    else:
        best_out, sum_out, flag_out = rest
    lanes = live_ref.shape[1]
    head_size = lanes // 2
    total = start_ref[start_ref.shape[0] - 1]
    blocks = []
    begin = 0
    widest = jnp.zeros((1, lanes), jnp.float32)
    for length, ref in zip(lengths, block_refs):
        left = lax.broadcasted_iota(jnp.int32, (length, lanes), 1) < head_size
        rows = slice(begin, begin + length)
        place = begin % size
        side_ref[rows] = jnp.where(left, live_ref[place : place + length], ref[0:length])
        reach = jnp.max(jnp.abs(ref[0:length].astype(jnp.float32)), axis=0, keepdims=True)
        widest = jnp.maximum(widest, reach)
        blocks.append((ref, length, rows))
        begin = begin + length
    lane = lax.broadcasted_iota(jnp.int32, (1, lanes), 1)
    keys_square = jnp.sum(jnp.where(lane < head_size, widest * widest, 0.0))
    if first:
        queries = query_ref[0 : query_ref.shape[0] // QUERY_TILE * QUERY_TILE].astype(jnp.float32)
        query_square = jnp.max(jnp.sum(queries * queries, axis=-1, keepdims=True))
        small = jnp.bool_(True)
    else:
        query_square = flag_in[0]
        small = flag_in[1] > 0.5
    before_small = small
    small = jnp.logical_and(small, query_square * keys_square <= SCORE_BOUND * SCORE_BOUND)
    if not last:
        flag_out[0] = query_square
        flag_out[1] = jnp.where(small, 1.0, 0.0)

    def score(query, ref, length):
        return lax.dot_general(
            query, ref[0:length], (((1,), (1,)), ((), ())), preferred_element_type=jnp.float32
        )

    def total_of(weights):
        return sum(
            jnp.dot(weight, side_ref[rows], preferred_element_type=jnp.float32)
            for weight, (ref, length, rows) in zip(weights, blocks)
        )

    def finish(place, sums):
        if last:
            sums = sums / pltpu.roll(sums, head_size, 1)
        sum_out[place] = sums

    def unshifted(start, tile):
        place = pl.ds(pl.multiple_of(start, QUERY_TILE), tile)
        query = query_ref[place]
        sums = total_of(
            [
                jnp.exp(score(query, ref, length)).astype(jnp.bfloat16)
                for ref, length, rows in blocks
            ]
        )
        if not first:
            sums = sums + sum_in[place]
        finish(place, sums)

    def shifted(start, tile):
        place = pl.ds(pl.multiple_of(start, tile), tile)
        query = query_ref[place]
        scores = [score(query, ref, length) for ref, length, rows in blocks]
        best = functools.reduce(
            jnp.maximum, [jnp.max(part, axis=-1, keepdims=True) for part in scores]
        )
        if not first:
            before = jnp.where(before_small, 0.0, best_in[place][:, 0:1])
            best = jnp.maximum(best, before)
        sums = total_of([jnp.exp(part - best).astype(jnp.bfloat16) for part in scores])
        if not first:
            sums = sums + sum_in[place] * jnp.exp(before - best)
        if not last:
            best_out[place] = jnp.broadcast_to(best, (tile, lanes))
        finish(place, sums)

    @pl.when(small)
    def _():
        def step(index, carry):
            unshifted(index * QUERY_BIG, QUERY_BIG)
            return carry

        bigs = (total + QUERY_BIG - QUERY_TILE - 1) // QUERY_BIG
        lax.fori_loop(0, bigs, step, 0)

        @pl.when(total > bigs * QUERY_BIG)
        def _():
            unshifted(bigs * QUERY_BIG, QUERY_TILE)

    @pl.when(jnp.logical_not(small))
    def _():
        def step(index, carry):
            shifted(index * QUERY_SMALL, QUERY_SMALL)
            return carry

        lax.fori_loop(0, (total + QUERY_SMALL - 1) // QUERY_SMALL, step, 0)

    if last:
        half = out_ref.shape[1] // MARKS
        left_half = lax.broadcasted_iota(jnp.int32, (half, lanes), 1) < head_size
        for source in range(MARKS * out_ref.shape[0]):
            start = start_ref[source]
            top = sum_out[pl.ds(pl.multiple_of(start, SUBLANES), half)]
            low = sum_out[pl.ds(pl.multiple_of(start + half, SUBLANES), half)]
            base = source % MARKS * half
            out_ref[source // MARKS, base : base + half] = jnp.where(
                left_half, pltpu.roll(top, head_size, 1), low
            ).astype(jnp.bfloat16)


def run_stage(stage, stages, size, starts, query, live, blocks, lengths, state, half):
    lanes = query.shape[1]
    queries = query.shape[0]
    outs = (starts.shape[0] - 1) // MARKS
    first, last = stage == 0, stage == stages - 1
    held = jax.ShapeDtypeStruct((queries, lanes), jnp.float32)
    flags = jax.ShapeDtypeStruct((2,), jnp.float32)
    keys = sum(lengths)
    scratch = [pltpu.VMEM((keys, lanes), jnp.bfloat16)]
    if last:
        out_shape = (jax.ShapeDtypeStruct((outs, MARKS * half, lanes), jnp.bfloat16),)
        out_specs = (VMEM,)
        scratch = [pltpu.VMEM((queries, lanes), jnp.float32)] + scratch
    else:
        out_shape = (held, held, flags)
        out_specs = (VMEM, VMEM, SMEM)
    places = 3 + len(blocks)
    return pl.pallas_call(
        functools.partial(attend_kernel, first, last, size, lengths),
        out_shape=out_shape,
        in_specs=[SMEM]
        + [VMEM] * (2 + len(blocks))
        + ([] if first else [VMEM, VMEM, SMEM]),
        out_specs=out_specs,
        scratch_shapes=scratch,
        input_output_aliases={} if first or last else {places: 0, places + 1: 1},
        compiler_params=params(),
        cost_estimate=pl.CostEstimate(
            flops=4 * keys * keys * lanes, bytes_accessed=keys * lanes * 8, transcendentals=0
        ),
    )(starts, query, live, *blocks, *state)


def tie(value, *after):
    return lax.optimization_barrier((value, *after))


def attend_size(size, half, *packed):
    return exchange_and_attend(size, half, *packed)


def exchange_and_attend(size, half, kv, live, query, starts):
    late = size // 2 // SIZE_STEP * SIZE_STEP
    early = size - late
    first, second, both = tie(kv[:early], kv[early:size], kv[:size])
    far_early = lax.ppermute(first, "far", SWAP)
    far_late = lax.ppermute(second, "far", SWAP)
    near = lax.ppermute(both, "near", SWAP)
    run = lambda stage, blocks, lengths, state: run_stage(
        stage, 3, size, starts, query, live, blocks, lengths, state, half
    )
    state = run(0, (both,), (size,), ())
    far_early, *state = tie(far_early, *state)
    both_early = lax.ppermute(far_early, "near", SWAP)
    both_late = lax.ppermute(far_late, "near", SWAP)
    state = run(1, (near, far_early, far_late), (size, early, late), state)
    both_early, both_late, *state = tie(both_early, both_late, *state)
    return run(2, (both_early, both_late), (early, late), state)[0]


def mix_kernel(core_ref, chip_ref, count_ref, got_ref, other_ref, x_ref, w_ref, out_ref, held_ref):
    chips, half, lanes = got_ref.shape
    time_dev, slots, width = x_ref.shape
    slot_rows = 2 * half // slots
    head_size = lanes // 2
    core = core_ref[0]
    chip = chip_ref[0]
    flipped = lax.rem(chip, 2) == 1
    left = lax.broadcasted_iota(jnp.int32, (half, lanes), 1) < head_size
    count = scalar(count_ref)
    live = live_rows(count, 2 * half, slot_rows, time_dev, lanes)
    for slot in range(chips // 2):
        block = (slot + chip // 2) % (chips // 2) if chips == 4 else slot
        for side in range(2):
            if side == 0:
                owner = core
                first = got_ref[2 * slot]
                second = got_ref[2 * slot + 1]
            else:
                owner = 1 - core
                first = other_ref[2 * slot]
                second = other_ref[2 * slot + 1]
            first = first.astype(jnp.float32)
            second = second.astype(jnp.float32)
            even = jnp.where(flipped, second, first)
            odd = jnp.where(flipped, first, second)
            top = jnp.where(left, even, pltpu.roll(odd, head_size, 1))
            low = jnp.where(left, pltpu.roll(even, head_size, 1), odd)
            pair = jnp.where(live, jnp.concatenate([top, low], axis=0), 0.0)
            place = pl.multiple_of((owner * (chips // 2) + block) * lanes, lanes)
            held_ref[:, pl.ds(place, lanes)] = pair.astype(jnp.bfloat16)
    hot = one_hot((time_dev * slots, 2 * half), slots, slot_rows, 1)
    attended = jnp.dot(hot, held_ref[...], preferred_element_type=jnp.float32).astype(jnp.bfloat16)
    mixed = jnp.dot(attended, w_ref[...], preferred_element_type=jnp.float32)
    full = x_ref[...].astype(jnp.float32) + mixed.reshape(time_dev, slots, width)
    slot = lax.broadcasted_iota(jnp.int32, full.shape, 1)
    out_ref[...] = jnp.where(slot < count, full, 0.0).astype(jnp.bfloat16)


def mix(core, chip, count, got, other, tokens, w_out):
    half, _ = got.shape[1:]
    return pl.pallas_call(
        mix_kernel,
        out_shape=jax.ShapeDtypeStruct(tokens.shape, jnp.bfloat16),
        in_specs=[SMEM] * 2 + [VMEM] * 5,
        out_specs=VMEM,
        scratch_shapes=[pltpu.VMEM((2 * half, w_out.shape[0]), jnp.bfloat16)],
        compiler_params=params(),
        cost_estimate=pl.CostEstimate(
            flops=4 * half * w_out.size, bytes_accessed=2 * w_out.size, transcendentals=0
        ),
        name="mix",
    )(core, chip, count, got, other, tokens, w_out)


def spread(arrays, chips):
    return [arrays[0]] + [
        lax.ppermute(arrays[hop], "chip", [(i, i ^ hop) for i in range(chips)])
        for hop in range(1, chips)
    ]


def head_per_device(tokens, tube_count, ln_gain, ln_bias, w_qkv, w_out):
    slots, time_dev, _ = tokens.shape
    slot_rows = up_to(time_dev, SUBLANES)
    rows = slots * slot_rows
    half = rows // 2
    chips = lax.axis_size("chip")
    core = lax.axis_index("core").reshape(1)
    chip = lax.axis_index("chip").reshape(1)
    by_time = jnp.transpose(tokens, (1, 0, 2))
    other_tokens = lax.ppermute(by_time, "core", SWAP)
    tube_count = tube_count.reshape(1, 1)
    other_count = lax.ppermute(tube_count, "core", SWAP)
    fetched = fetch(core, by_time, ln_gain, ln_bias, w_qkv, rows)
    rows_in, gain, bias, weights = fetched
    messages = project(
        chip, tube_count, other_count, rows_in, other_tokens, gain, bias, weights
    )
    got = spread(messages, chips)
    least = up_to((HEADS - 1) * slot_rows + rows, SIZE_STEP // 2)
    most = up_to((HEADS - 1) * rows + slot_rows, SIZE_STEP)
    sizes = [least + more for more in SIZES_ABOVE if least + more < most] + [most]
    kv, live, query, starts, case = pack(got, sizes, slot_rows, time_dev)
    branches = [functools.partial(attend_size, size, half) for size in sizes]
    returned = lax.switch(case[0], branches, kv, live, query, starts)
    back = jnp.stack(spread(returned, chips))
    other = lax.ppermute(back[:, half:], "core", SWAP)
    mixed = mix(core, chip, tube_count, back[:, :half], other, by_time, w_out)
    return jnp.transpose(mixed, (1, 0, 2))


def layer_norm(flat, ln_gain, ln_bias):
    values32 = flat.astype(jnp.float32)
    center = values32 - jnp.mean(values32, axis=-1, keepdims=True)
    spread = jnp.mean(center * center, axis=-1, keepdims=True)
    return (center * lax.rsqrt(spread + EPSILON) * ln_gain + ln_bias).astype(jnp.bfloat16)


def live_mask(counts, slots_dev, time_dev):
    slot_ids = jnp.arange(slots_dev)[None, :, None]
    marks = jnp.broadcast_to(
        slot_ids < counts[:, None, None], (counts.shape[0], slots_dev, time_dev)
    )
    return marks.reshape(-1)


def attend(carry, query_heads, key_block, value_block, live_keys, scaling):
    best_now, total_now, accum = carry
    heads = query_heads.shape[1]
    key_heads = key_block.reshape(key_block.shape[0], heads, -1)
    value_heads = value_block.reshape(value_block.shape[0], heads, -1)
    scores = (
        jnp.einsum("qhd,khd->hqk", query_heads, key_heads, preferred_element_type=jnp.float32)
        * scaling
    )
    scores = jnp.where(live_keys[None, None, :], scores, NEG_FILL)
    best_next = jnp.maximum(best_now, jnp.max(scores, axis=-1))
    fading = jnp.exp(best_now - best_next)
    weights = jnp.exp(scores - best_next[..., None])
    total_next = total_now * fading + jnp.sum(weights, axis=-1)
    accum = accum * fading[..., None] + jnp.einsum(
        "hqk,khd->hqd",
        weights.astype(jnp.bfloat16),
        value_heads,
        preferred_element_type=jnp.float32,
    )
    return (best_next, total_next, accum)


def make_fold(query_heads, vis_dev, time_dev, scaling):
    rows_dev = vis_dev * time_dev

    def fold_masked(carry, piece, start):
        key_all, value_all, count_all = piece
        width_in = key_all.shape[1]
        shards = count_all.shape[0]
        group = 1
        for _ in range(6):
            if shards % (group * 2) == 0 and group * rows_dev < 2048:
                group = group * 2
        blocks = shards // group
        key_groups = key_all.reshape(blocks, group * rows_dev, width_in)
        value_groups = value_all.reshape(blocks, group * rows_dev, width_in)
        count_groups = count_all.reshape(blocks, group)

        def step_group(state, item):
            key_group, value_group, count_group = item
            marks = live_mask(count_group, vis_dev, time_dev)
            return (attend(state, query_heads, key_group, value_group, marks, scaling), None)

        carry, _ = lax.scan(step_group, carry, (key_groups, value_groups, count_groups))
        return carry

    return fold_masked


def start_state(heads, rows, head_size):
    return (
        jnp.full((heads, rows), NEG_FILL, jnp.float32),
        jnp.zeros((heads, rows), jnp.float32),
        jnp.zeros((heads, rows, head_size), jnp.float32),
    )


def on_device(tokens, tube_count, ln_gain, ln_bias, w_qkv, w_out):
    vis_dev, time_dev, width = tokens.shape
    rows_dev = vis_dev * time_dev
    inner = w_out.shape[0]
    head_size = inner // HEADS
    flat = tokens.reshape(rows_dev, width)
    normed = layer_norm(flat, ln_gain, ln_bias)
    projected = jnp.dot(normed, w_qkv, preferred_element_type=jnp.float32).astype(jnp.bfloat16)
    scaling = head_size ** (-0.5)
    frames = lax.axis_size("frame")
    local_heads = HEADS // frames
    stacked = projected.reshape(rows_dev, 3, HEADS, head_size)
    regrouped = lax.all_to_all(stacked, "frame", split_axis=2, concat_axis=0, tiled=True)
    all_rows = regrouped.shape[0]
    query_local = regrouped[:, 0]
    key_local = regrouped[:, 1].reshape(all_rows, local_heads * head_size)
    value_local = regrouped[:, 2].reshape(all_rows, local_heads * head_size)
    counts_rep = jnp.tile(tube_count, frames)
    fold_fn = make_fold(query_local, vis_dev, time_dev, scaling)
    state = fold_fn(
        start_state(local_heads, all_rows, head_size),
        (
            lax.all_gather(key_local, "space", axis=0, tiled=True),
            lax.all_gather(value_local, "space", axis=0, tiled=True),
            lax.all_gather(counts_rep, "space", axis=0, tiled=True),
        ),
        jnp.int32(0),
    )
    _, total_final, accum_final = state
    attended = (accum_final / total_final[..., None]).astype(jnp.bfloat16)
    attended = jnp.transpose(attended, (1, 0, 2))
    returned = lax.all_to_all(attended, "frame", split_axis=0, concat_axis=1, tiled=True)
    attended = returned.reshape(rows_dev, inner)
    mixed = flat.astype(jnp.float32) + jnp.dot(attended, w_out, preferred_element_type=jnp.float32)
    own_live = live_mask(tube_count, vis_dev, time_dev)
    mixed = jnp.where(own_live[:, None], mixed, 0.0)
    return mixed.astype(jnp.bfloat16).reshape(vis_dev, time_dev, width)


def solution(mesh):
    frames, spaces = mesh.shape["frame"], mesh.shape["space"]
    parts = (2, frames // 2, spaces // 2, 2)

    def layer(tokens, tube_count, ln_gain, ln_bias, w_qkv, w_out):
        slots = tokens.shape[0] // spaces
        time_dev = tokens.shape[1] // frames
        rows = slots * up_to(time_dev, SUBLANES)
        pairs = 2 * w_out.shape[0] == HEADS * LANES and rows % (2 * PACK) == 0
        padded = up_to(time_dev, SUBLANES) >= time_dev + MARKS
        split = parts[1] == 2 and parts[2] == 4 and spaces == HEADS
        if split and pairs and padded:
            run, over = head_per_device, Mesh(
                mesh.devices.reshape(parts), ("far", "near", "chip", "core")
            )
            frame, space = ("far", "near"), ("chip", "core")
        else:
            run, over, frame, space = on_device, mesh, "frame", "space"
        mapped = jax.shard_map(
            run,
            mesh=over,
            in_specs=(P(space, frame, None), P(space), P(), P(), P(), P()),
            out_specs=P(space, frame, None),
            check_vma=False,
        )
        return mapped(tokens, tube_count, ln_gain, ln_bias, w_qkv, w_out)

    return layer
```

```python
import functools
import jax
import jax.numpy as jnp
from jax import lax
from jax.experimental import pallas as pl
from jax.experimental.pallas import tpu as pltpu
from jax.sharding import Mesh, PartitionSpec as P

HEADS = 8


EPSILON = 1e-06
NEG_FILL = -1e30
LANES = 128
SUBLANES = 8
PACK = 16
SIZE_STEP = 128
MARKS = 2
SIZES_ABOVE = (128, 192, 320, 448)
SCORE_BOUND = 60.0
QUERY_SMALL = 128
QUERY_TILE = 256
QUERY_BIG = 512
VMEM_BYTES = 20 * 2**20

VMEM = pl.BlockSpec(memory_space=pltpu.VMEM)
SMEM = pl.BlockSpec(memory_space=pltpu.SMEM)
SWAP = [(0, 1), (1, 0)]


def up_to(value, unit):
    return -(-value // unit) * unit


def params():
    return pltpu.CompilerParams(vmem_limit_bytes=VMEM_BYTES)


def packed_rows(count, slot_rows):
    return count * slot_rows


def slot_of(row, slots, slot_rows):
    slot = row * 0
    for edge in range(1, slots):
        slot = slot + (row >= edge * slot_rows).astype(jnp.int32)
    return slot


def live_rows(count, rows, slot_rows, time_dev, width):
    row = lax.broadcasted_iota(jnp.int32, (rows, width), 0)
    slot = slot_of(row, rows // slot_rows, slot_rows)
    return (slot < count) & (row - slot * slot_rows < time_dev)


def one_hot(shape, slots, slot_rows, padded_dim):
    padded = lax.broadcasted_iota(jnp.int32, shape, padded_dim)
    plain = lax.broadcasted_iota(jnp.int32, shape, 1 - padded_dim)
    slot = slot_of(padded, slots, slot_rows)
    hot = plain == (padded - slot * slot_rows) * slots + slot
    return hot.astype(jnp.float32).astype(jnp.bfloat16)


def scalar(ref):
    return jnp.max(ref[...].astype(jnp.float32)).astype(jnp.int32)


def read(ref, row):
    return jnp.max(ref[row : row + 1])


def write(ref, row, value):
    ref[row : row + 1] = jnp.full((1, ref.shape[1]), value, ref.dtype)


def normalise(x_ref, gain_ref, bias_ref, rows):
    time_dev, slots, width = x_ref.shape
    x = x_ref[...].astype(jnp.float32).reshape(time_dev * slots, width)
    center = x - jnp.mean(x, axis=-1, keepdims=True)
    spread = jnp.mean(center * center, axis=-1, keepdims=True)
    normed = center * lax.rsqrt(spread + EPSILON) * gain_ref[...] + bias_ref[...]
    hot = one_hot((rows, time_dev * slots), slots, rows // slots, 0)
    return jnp.dot(
        hot, normed.astype(jnp.bfloat16), preferred_element_type=jnp.float32
    ).astype(jnp.bfloat16)


def fetch_kernel(
    x_hbm,
    gain_hbm,
    bias_hbm,
    w_hbm,
    rows_ref,
    gain_ref,
    bias_ref,
    w_ref,
    x_ref,
    sems,
):
    kinds, _, wide = w_ref.shape
    pairs = [(x_hbm, x_ref), (gain_hbm, gain_ref), (bias_hbm, bias_ref)]
    for kind in range(kinds):
        start = pl.multiple_of(2 * wide * kind + wide * lax.axis_index("core"), wide)
        pairs.append((w_hbm.at[:, pl.ds(start, wide)], w_ref.at[kind]))
    copies = [
        pltpu.make_async_copy(source, target, sems.at[place])
        for place, (source, target) in enumerate(pairs)
    ]
    for copy in copies:
        copy.start()
    for copy in copies[:-kinds]:
        copy.wait()
    rows_ref[...] = normalise(x_ref, gain_ref, bias_ref, rows_ref.shape[0])
    for copy in copies[-kinds:]:
        copy.wait()


def fetch(tokens, ln_gain, ln_bias, w_qkv, rows):
    width = tokens.shape[-1]
    wide = w_qkv.shape[1] // 6
    gain = ln_gain.reshape(1, width)
    bias = ln_bias.reshape(1, width)
    inputs = [pltpu.with_memory_space_constraint(a, pltpu.HBM) for a in (tokens, gain, bias, w_qkv)]
    hbm = pl.BlockSpec(memory_space=pltpu.HBM)
    return pl.pallas_call(
        fetch_kernel,
        out_shape=(
            jax.ShapeDtypeStruct((rows, width), jnp.bfloat16),
            jax.ShapeDtypeStruct(gain.shape, gain.dtype),
            jax.ShapeDtypeStruct(bias.shape, bias.dtype),
            jax.ShapeDtypeStruct((3, width, wide), w_qkv.dtype),
        ),
        in_specs=[hbm] * 4,
        out_specs=(VMEM,) * 4,
        scratch_shapes=[
            pltpu.VMEM(tokens.shape, tokens.dtype),
            pltpu.SemaphoreType.DMA((6,)),
        ],
        compiler_params=params(),
        cost_estimate=pl.CostEstimate(
            flops=2 * rows * w_qkv.size, bytes_accessed=w_qkv.size, transcendentals=0
        ),
        name="fetch",
    )(*inputs)


def project_kernel(
    count_ref,
    other_count_ref,
    rows_ref,
    other_ref,
    gain_ref,
    bias_ref,
    w_ref,
    *refs,
):
    chips = len(refs) - 3
    outs = refs[:chips]
    query_ref, key_ref, value_ref = refs[chips:]
    time_dev, slots, _ = other_ref.shape
    message, lanes = outs[0].shape
    rows = message // 3
    slot_rows = rows // slots
    half = rows // 2
    head_size = lanes // 2
    scaling = head_size ** (-0.5)
    chip = lax.axis_index("chip")
    rows_in = jnp.concatenate(
        [rows_ref[...], normalise(other_ref, gain_ref, bias_ref, rows)], axis=0
    )
    for kind, target in enumerate((query_ref, key_ref, value_ref)):
        target[...] = jnp.dot(rows_in, w_ref[kind], preferred_element_type=jnp.float32)
    left = lax.broadcasted_iota(jnp.int32, (rows, lanes), 1) < head_size
    left_half = left[:half]
    row_half = lax.broadcasted_iota(jnp.int32, (half, lanes), 0)
    counts = (scalar(count_ref), scalar(other_count_ref))
    flipped = lax.rem(chip, 2) == 1
    for slot in range(chips // 2):
        block = (slot + chip // 2) % (chips // 2) if chips == 4 else slot
        cols = pl.ds(pl.multiple_of(block * lanes, lanes), lanes)
        for group, count in enumerate(counts):
            base = group * rows
            key_pair = key_ref[base : base + rows, cols]
            value_pair = value_ref[base : base + rows, cols]
            live = live_rows(count, rows, slot_rows, time_dev, lanes)
            key_pair = jnp.where(live, key_pair, key_pair[0:1])
            value_pair = jnp.where(live, value_pair, 0.0)
            even = jnp.where(left, key_pair, pltpu.roll(value_pair, head_size, 1))
            odd = jnp.where(left, pltpu.roll(key_pair, head_size, 1), value_pair)
            first = jnp.where(flipped, odd, even).astype(jnp.bfloat16)
            second = jnp.where(flipped, even, odd).astype(jnp.bfloat16)
            outs[2 * slot][base : base + rows] = first
            outs[2 * slot + 1][base : base + rows] = second
            top = query_ref[base : base + half, cols] * scaling
            low = query_ref[base + half : base + rows, cols] * scaling
            even = jnp.where(left_half, top, pltpu.roll(low, head_size, 1))
            odd = jnp.where(left_half, pltpu.roll(top, head_size, 1), low)
            first = jnp.where(flipped, odd, even)
            second = jnp.where(flipped, even, odd)
            if group == 1:
                for index, mark in enumerate(counts):
                    here = (row_half == half - MARKS + index) & jnp.logical_not(left_half)
                    first = jnp.where(here, mark.astype(jnp.float32), first)
                    second = jnp.where(here, mark.astype(jnp.float32), second)
            place = 2 * rows + group * half
            outs[2 * slot][place : place + half] = first.astype(jnp.bfloat16)
            outs[2 * slot + 1][place : place + half] = second.astype(jnp.bfloat16)


def project(count, other_count, rows_in, other_tokens, gain, bias, weights):
    chips = HEADS // 2
    rows = rows_in.shape[0]
    wide = weights.shape[-1]
    held = pltpu.VMEM((2 * rows, wide), jnp.float32)
    message = jax.ShapeDtypeStruct((3 * rows, LANES), jnp.bfloat16)
    return pl.pallas_call(
        project_kernel,
        out_shape=(message,) * chips,
        in_specs=[VMEM] * 7,
        out_specs=(VMEM,) * chips,
        scratch_shapes=[held] * 3,
        compiler_params=params(),
        cost_estimate=pl.CostEstimate(
            flops=4 * rows * weights.size, bytes_accessed=2 * weights.size, transcendentals=0
        ),
        name="project",
    )(count, other_count, rows_in, other_tokens, gain, bias, weights)


def source_counts(ref):
    message = ref.shape[0]
    tail = ref[message - PACK : message].astype(jnp.float32)
    return [
        jnp.max(tail[PACK - MARKS + index : PACK - MARKS + index + 1, LANES // 2 :]).astype(jnp.int32)
        for index in range(MARKS)
    ]


def pack_kernel(slot_rows, sizes, *refs):
    got_refs = refs[:-3]
    kv_room, start_ref, case_ref = refs[-3:]
    message, lanes = got_refs[0].shape
    rows = message // 3
    head_size = lanes // 2
    lane = lax.broadcasted_iota(jnp.int32, (PACK, lanes), 1)
    first = got_refs[0][0:PACK].astype(jnp.float32)[0:1]
    fill = jnp.where(lane < head_size, jnp.broadcast_to(first, (PACK, lanes)), 0.0)
    fill = fill.astype(jnp.bfloat16)
    for start in range(0, kv_room.shape[0] - rows, PACK):
        kv_room[start : start + PACK] = fill
    start = jnp.int32(0)
    for index, ref in enumerate(got_refs):
        for group, count in enumerate(source_counts(ref)):
            source = MARKS * index + group
            write(start_ref, source, start.astype(jnp.float32))
            write(start_ref, HEADS + source, count.astype(jnp.float32))
            kv_room[pl.ds(pl.multiple_of(start, SUBLANES), rows)] = ref[
                group * rows : (group + 1) * rows
            ]
            start = start + packed_rows(count, slot_rows)
    write(start_ref, 2 * HEADS, start.astype(jnp.float32))
    case_ref[0] = sum((start > size).astype(jnp.int32) for size in sizes[:-1])


def pack(got, sizes, slot_rows):
    message, lanes = got[0].shape
    rows = message // 3
    return pl.pallas_call(
        functools.partial(pack_kernel, slot_rows, tuple(sizes)),
        out_shape=(
            jax.ShapeDtypeStruct((sizes[-1] + rows, lanes), jnp.bfloat16),
            jax.ShapeDtypeStruct((up_to(2 * HEADS + 1, SUBLANES), lanes), jnp.float32),
            jax.ShapeDtypeStruct((1,), jnp.int32),
        ),
        in_specs=[VMEM] * len(got),
        out_specs=(VMEM, VMEM, SMEM),
        compiler_params=params(),
        name="pack",
    )(*got)


def prepare_kernel(slot_rows, time_dev, start_ref, *refs):
    got_refs = refs[:-2]
    live_room, query_ref = refs[-2:]
    message, lanes = got_refs[0].shape
    rows = message // 3
    half = rows // 2
    head_size = lanes // 2
    blank = jnp.zeros((PACK, lanes), jnp.bfloat16)
    for start in range(0, live_room.shape[0] - rows, PACK):
        live_room[start : start + PACK] = blank
    for start in range(0, query_ref.shape[0], PACK):
        query_ref[start : start + PACK] = blank
    left = lax.broadcasted_iota(jnp.int32, (half, lanes), 1) < head_size
    plain = left & (lax.broadcasted_iota(jnp.int32, (half, lanes), 0) < half - MARKS)
    for index, ref in enumerate(got_refs):
        for group in range(MARKS):
            source = MARKS * index + group
            start = read(start_ref, source).astype(jnp.int32)
            count = read(start_ref, HEADS + source).astype(jnp.int32)
            live = live_rows(count, rows, slot_rows, time_dev, lanes)
            live_room[pl.ds(pl.multiple_of(start, SUBLANES), rows)] = live.astype(
                jnp.float32
            ).astype(jnp.bfloat16)
            base = 2 * rows + group * half
            pair = ref[base : base + half].astype(jnp.float32)
            query_ref[pl.ds(pl.multiple_of(start, SUBLANES), half)] = jnp.where(
                left, pair, 0.0
            ).astype(jnp.bfloat16)
            query_ref[pl.ds(pl.multiple_of(start + half, SUBLANES), half)] = jnp.where(
                plain, pltpu.roll(pair, head_size, 1), 0.0
            ).astype(jnp.bfloat16)


def prepare(starts, got, room, slot_rows, time_dev):
    message, lanes = got[0].shape
    rows = message // 3
    queries = up_to(HEADS * rows, QUERY_TILE) + rows
    return pl.pallas_call(
        functools.partial(prepare_kernel, slot_rows, time_dev),
        out_shape=(
            jax.ShapeDtypeStruct((room, lanes), jnp.bfloat16),
            jax.ShapeDtypeStruct((queries, lanes), jnp.bfloat16),
        ),
        in_specs=[VMEM] * (1 + len(got)),
        out_specs=(VMEM, VMEM),
        compiler_params=params(),
        cost_estimate=pl.CostEstimate(
            flops=2 * queries * lanes * lanes, bytes_accessed=queries * lanes * 4, transcendentals=0
        ),
        name="prepare",
    )(starts, *got)


def attend_kernel(first, last, size, lengths, *refs):
    start_ref, query_ref, live_ref = refs[:3]
    block_refs = refs[3 : 3 + len(lengths)]
    rest = list(refs[3 + len(lengths) :])
    side_ref = rest.pop()
    if not first:
        best_in, sum_in, flag_in = rest[:3]
        rest = rest[3:]
    if last:
        sum_out = rest.pop()
        out_ref = rest[0]
    else:
        best_out, sum_out, flag_out = rest
    lanes = live_ref.shape[1]
    head_size = lanes // 2
    total = read(start_ref, 2 * HEADS).astype(jnp.int32)
    blocks = []
    begin = 0
    widest = jnp.zeros((1, lanes), jnp.float32)
    for length, ref in zip(lengths, block_refs):
        left = lax.broadcasted_iota(jnp.int32, (length, lanes), 1) < head_size
        rows = slice(begin, begin + length)
        place = begin % size
        side_ref[rows] = jnp.where(left, live_ref[place : place + length], ref[0:length])
        reach = jnp.max(jnp.abs(ref[0:length].astype(jnp.float32)), axis=0, keepdims=True)
        widest = jnp.maximum(widest, reach)
        blocks.append((ref, length, rows))
        begin = begin + length
    lane = lax.broadcasted_iota(jnp.int32, (1, lanes), 1)
    keys_square = jnp.sum(jnp.where(lane < head_size, widest * widest, 0.0))
    if first:
        queries = query_ref[0 : query_ref.shape[0] // QUERY_TILE * QUERY_TILE].astype(jnp.float32)
        query_square = jnp.max(jnp.sum(queries * queries, axis=-1, keepdims=True))
        small = jnp.bool_(True)
    else:
        query_square = read(flag_in, 0)
        small = read(flag_in, 1) > 0.5
    before_small = small
    small = jnp.logical_and(small, query_square * keys_square <= SCORE_BOUND * SCORE_BOUND)
    if not last:
        write(flag_out, 0, query_square)
        write(flag_out, 1, jnp.where(small, 1.0, 0.0))

    def score(query, ref, length):
        return lax.dot_general(
            query, ref[0:length], (((1,), (1,)), ((), ())), preferred_element_type=jnp.float32
        )

    def total_of(weights):
        return sum(
            jnp.dot(weight, side_ref[rows], preferred_element_type=jnp.float32)
            for weight, (ref, length, rows) in zip(weights, blocks)
        )

    def finish(place, sums):
        if last:
            sums = sums / pltpu.roll(sums, head_size, 1)
        sum_out[place] = sums

    def unshifted(start, tile):
        place = pl.ds(pl.multiple_of(start, QUERY_TILE), tile)
        query = query_ref[place]
        sums = total_of(
            [
                jnp.exp(score(query, ref, length)).astype(jnp.bfloat16)
                for ref, length, rows in blocks
            ]
        )
        if not first:
            sums = sums + sum_in[place]
        finish(place, sums)

    def shifted(start, tile):
        place = pl.ds(pl.multiple_of(start, tile), tile)
        query = query_ref[place]
        scores = [score(query, ref, length) for ref, length, rows in blocks]
        best = functools.reduce(
            jnp.maximum, [jnp.max(part, axis=-1, keepdims=True) for part in scores]
        )
        if not first:
            before = jnp.where(before_small, 0.0, best_in[place][:, 0:1])
            best = jnp.maximum(best, before)
        sums = total_of([jnp.exp(part - best).astype(jnp.bfloat16) for part in scores])
        if not first:
            sums = sums + sum_in[place] * jnp.exp(before - best)
        if not last:
            best_out[place] = jnp.broadcast_to(best, (tile, lanes))
        finish(place, sums)

    @pl.when(small)
    def _():
        def step(index, carry):
            unshifted(index * QUERY_BIG, QUERY_BIG)
            return carry

        bigs = (total + QUERY_BIG - QUERY_TILE - 1) // QUERY_BIG
        lax.fori_loop(0, bigs, step, 0)

        @pl.when(total > bigs * QUERY_BIG)
        def _():
            unshifted(bigs * QUERY_BIG, QUERY_TILE)

    @pl.when(jnp.logical_not(small))
    def _():
        def step(index, carry):
            shifted(index * QUERY_SMALL, QUERY_SMALL)
            return carry

        lax.fori_loop(0, (total + QUERY_SMALL - 1) // QUERY_SMALL, step, 0)

    if last:
        half = out_ref.shape[1] // MARKS
        left_half = lax.broadcasted_iota(jnp.int32, (half, lanes), 1) < head_size
        for source in range(MARKS * out_ref.shape[0]):
            start = read(start_ref, source).astype(jnp.int32)
            top = sum_out[pl.ds(pl.multiple_of(start, SUBLANES), half)]
            low = sum_out[pl.ds(pl.multiple_of(start + half, SUBLANES), half)]
            base = source % MARKS * half
            out_ref[source // MARKS, base : base + half] = jnp.where(
                left_half, pltpu.roll(top, head_size, 1), low
            ).astype(jnp.bfloat16)


def run_stage(stage, stages, size, starts, query, live, blocks, lengths, state, half):
    lanes = query.shape[1]
    queries = query.shape[0]
    outs = HEADS // MARKS
    first, last = stage == 0, stage == stages - 1
    held = jax.ShapeDtypeStruct((queries, lanes), jnp.float32)
    flags = jax.ShapeDtypeStruct((SUBLANES, lanes), jnp.float32)
    keys = sum(lengths)
    scratch = [pltpu.VMEM((keys, lanes), jnp.bfloat16)]
    if last:
        out_shape = (jax.ShapeDtypeStruct((outs, MARKS * half, lanes), jnp.bfloat16),)
        out_specs = (VMEM,)
        scratch = [pltpu.VMEM((queries, lanes), jnp.float32)] + scratch
    else:
        out_shape = (held, held, flags)
        out_specs = (VMEM,) * 3
    places = 3 + len(blocks)
    return pl.pallas_call(
        functools.partial(attend_kernel, first, last, size, lengths),
        out_shape=out_shape,
        in_specs=[VMEM] * (3 + len(blocks) + len(state)),
        out_specs=out_specs,
        scratch_shapes=scratch,
        input_output_aliases={} if first or last else {places: 0, places + 1: 1},
        compiler_params=params(),
        cost_estimate=pl.CostEstimate(
            flops=4 * keys * keys * lanes, bytes_accessed=keys * lanes * 8, transcendentals=0
        ),
    )(starts, query, live, *blocks, *state)


def tie(value, *after):
    return lax.optimization_barrier((value, *after))


def attend_size(size, slot_rows, time_dev, *packed):
    return exchange_and_attend(size, slot_rows, time_dev, *packed)


def exchange_and_attend(size, slot_rows, time_dev, kv, starts, *got):
    half = got[0].shape[0] // 6
    late = size // 2 // SIZE_STEP * SIZE_STEP
    early = size - late
    first, second, both = tie(kv[:early], kv[early:size], kv[:size])
    far_early = lax.ppermute(first, "far", SWAP)
    far_late = lax.ppermute(second, "far", SWAP)
    near = lax.ppermute(both, "near", SWAP)
    run = lambda stage, blocks, lengths, state: run_stage(
        stage, 3, size, starts, query, live, blocks, lengths, state, half
    )
    live, query = prepare(starts, got, kv.shape[0], slot_rows, time_dev)
    state = run(0, (both,), (size,), ())
    far_early, *state = tie(far_early, *state)
    both_early = lax.ppermute(far_early, "near", SWAP)
    both_late = lax.ppermute(far_late, "near", SWAP)
    state = run(1, (near, far_early, far_late), (size, early, late), state)
    both_early, both_late, *state = tie(both_early, both_late, *state)
    return run(2, (both_early, both_late), (early, late), state)[0]


def mix_kernel(count_ref, got_ref, other_ref, x_ref, w_ref, out_ref, held_ref):
    chips, half, lanes = got_ref.shape
    time_dev, slots, width = x_ref.shape
    slot_rows = 2 * half // slots
    head_size = lanes // 2
    core = lax.axis_index("core")
    chip = lax.axis_index("chip")
    flipped = lax.rem(chip, 2) == 1
    left = lax.broadcasted_iota(jnp.int32, (half, lanes), 1) < head_size
    count = scalar(count_ref)
    live = live_rows(count, 2 * half, slot_rows, time_dev, lanes)
    for slot in range(chips // 2):
        block = (slot + chip // 2) % (chips // 2) if chips == 4 else slot
        for side in range(2):
            if side == 0:
                owner = core
                first = got_ref[2 * slot]
                second = got_ref[2 * slot + 1]
            else:
                owner = 1 - core
                first = other_ref[2 * slot]
                second = other_ref[2 * slot + 1]
            first = first.astype(jnp.float32)
            second = second.astype(jnp.float32)
            even = jnp.where(flipped, second, first)
            odd = jnp.where(flipped, first, second)
            top = jnp.where(left, even, pltpu.roll(odd, head_size, 1))
            low = jnp.where(left, pltpu.roll(even, head_size, 1), odd)
            pair = jnp.where(live, jnp.concatenate([top, low], axis=0), 0.0)
            place = pl.multiple_of((owner * (chips // 2) + block) * lanes, lanes)
            held_ref[:, pl.ds(place, lanes)] = pair.astype(jnp.bfloat16)
    hot = one_hot((time_dev * slots, 2 * half), slots, slot_rows, 1)
    attended = jnp.dot(hot, held_ref[...], preferred_element_type=jnp.float32).astype(jnp.bfloat16)
    mixed = jnp.dot(attended, w_ref[...], preferred_element_type=jnp.float32)
    full = x_ref[...].astype(jnp.float32) + mixed.reshape(time_dev, slots, width)
    slot = lax.broadcasted_iota(jnp.int32, full.shape, 1)
    out_ref[...] = jnp.where(slot < count, full, 0.0).astype(jnp.bfloat16)


def mix(count, got, other, tokens, w_out):
    half, _ = got.shape[1:]
    return pl.pallas_call(
        mix_kernel,
        out_shape=jax.ShapeDtypeStruct(tokens.shape, jnp.bfloat16),
        in_specs=[VMEM] * 5,
        out_specs=VMEM,
        scratch_shapes=[pltpu.VMEM((2 * half, w_out.shape[0]), jnp.bfloat16)],
        compiler_params=params(),
        cost_estimate=pl.CostEstimate(
            flops=4 * half * w_out.size, bytes_accessed=2 * w_out.size, transcendentals=0
        ),
        name="mix",
    )(count, got, other, tokens, w_out)


def spread(arrays, chips):
    out = [arrays[0]]
    for hop in range(1, chips):
        out.append(lax.ppermute(arrays[hop], "chip", [(i, i ^ hop) for i in range(chips)]))
    return out


def head_per_device(tokens, tube_count, ln_gain, ln_bias, w_qkv, w_out):
    slots, time_dev, _ = tokens.shape
    slot_rows = up_to(time_dev, SUBLANES)
    rows = slots * slot_rows
    half = rows // 2
    chips = lax.axis_size("chip")
    by_time = jnp.transpose(tokens, (1, 0, 2))
    other_tokens = lax.ppermute(by_time, "core", SWAP)
    tube_count = tube_count.reshape(1, 1)
    other_count = lax.ppermute(tube_count, "core", SWAP)
    fetched = fetch(by_time, ln_gain, ln_bias, w_qkv, rows)
    rows_in, gain, bias, weights = fetched
    messages = project(
        tube_count, other_count, rows_in, other_tokens, gain, bias, weights
    )
    got = spread(messages, chips)
    least = up_to((HEADS - 1) * slot_rows + rows, SIZE_STEP // 2)
    most = up_to((HEADS - 1) * rows + slot_rows, SIZE_STEP)
    sizes = [least + more for more in SIZES_ABOVE if least + more < most] + [most]
    kv, starts, case = pack(got, sizes, slot_rows)
    branches = [functools.partial(attend_size, size, slot_rows, time_dev) for size in sizes]
    returned = lax.switch(case[0], branches, kv, starts, *got)
    back = jnp.stack(spread(returned, chips))
    other = lax.ppermute(back[:, half:], "core", SWAP)
    mixed = mix(tube_count, back[:, :half], other, by_time, w_out)
    return jnp.transpose(mixed, (1, 0, 2))


def layer_norm(flat, ln_gain, ln_bias):
    values32 = flat.astype(jnp.float32)
    center = values32 - jnp.mean(values32, axis=-1, keepdims=True)
    spread = jnp.mean(center * center, axis=-1, keepdims=True)
    return (center * lax.rsqrt(spread + EPSILON) * ln_gain + ln_bias).astype(jnp.bfloat16)


def live_mask(counts, slots_dev, time_dev):
    slot_ids = jnp.arange(slots_dev)[None, :, None]
    marks = jnp.broadcast_to(
        slot_ids < counts[:, None, None], (counts.shape[0], slots_dev, time_dev)
    )
    return marks.reshape(-1)


def attend(carry, query_heads, key_block, value_block, live_keys, scaling):
    best_now, total_now, accum = carry
    heads = query_heads.shape[1]
    key_heads = key_block.reshape(key_block.shape[0], heads, -1)
    value_heads = value_block.reshape(value_block.shape[0], heads, -1)
    scores = (
        jnp.einsum("qhd,khd->hqk", query_heads, key_heads, preferred_element_type=jnp.float32)
        * scaling
    )
    scores = jnp.where(live_keys[None, None, :], scores, NEG_FILL)
    best_next = jnp.maximum(best_now, jnp.max(scores, axis=-1))
    fading = jnp.exp(best_now - best_next)
    weights = jnp.exp(scores - best_next[..., None])
    total_next = total_now * fading + jnp.sum(weights, axis=-1)
    accum = accum * fading[..., None] + jnp.einsum(
        "hqk,khd->hqd",
        weights.astype(jnp.bfloat16),
        value_heads,
        preferred_element_type=jnp.float32,
    )
    return (best_next, total_next, accum)


def make_fold(query_heads, vis_dev, time_dev, scaling):
    rows_dev = vis_dev * time_dev

    def fold_masked(carry, piece, start):
        key_all, value_all, count_all = piece
        width_in = key_all.shape[1]
        shards = count_all.shape[0]
        group = 1
        for _ in range(6):
            if shards % (group * 2) == 0 and group * rows_dev < 2048:
                group = group * 2
        blocks = shards // group
        key_groups = key_all.reshape(blocks, group * rows_dev, width_in)
        value_groups = value_all.reshape(blocks, group * rows_dev, width_in)
        count_groups = count_all.reshape(blocks, group)

        def step_group(state, item):
            key_group, value_group, count_group = item
            marks = live_mask(count_group, vis_dev, time_dev)
            return (attend(state, query_heads, key_group, value_group, marks, scaling), None)

        carry, _ = lax.scan(step_group, carry, (key_groups, value_groups, count_groups))
        return carry

    return fold_masked


def start_state(heads, rows, head_size):
    return (
        jnp.full((heads, rows), NEG_FILL, jnp.float32),
        jnp.zeros((heads, rows), jnp.float32),
        jnp.zeros((heads, rows, head_size), jnp.float32),
    )


def on_device(tokens, tube_count, ln_gain, ln_bias, w_qkv, w_out):
    vis_dev, time_dev, width = tokens.shape
    rows_dev = vis_dev * time_dev
    inner = w_out.shape[0]
    head_size = inner // HEADS
    flat = tokens.reshape(rows_dev, width)
    normed = layer_norm(flat, ln_gain, ln_bias)
    projected = jnp.dot(normed, w_qkv, preferred_element_type=jnp.float32).astype(jnp.bfloat16)
    scaling = head_size ** (-0.5)
    frames = lax.axis_size("frame")
    local_heads = HEADS // frames
    stacked = projected.reshape(rows_dev, 3, HEADS, head_size)
    regrouped = lax.all_to_all(stacked, "frame", split_axis=2, concat_axis=0, tiled=True)
    all_rows = regrouped.shape[0]
    query_local = regrouped[:, 0]
    key_local = regrouped[:, 1].reshape(all_rows, local_heads * head_size)
    value_local = regrouped[:, 2].reshape(all_rows, local_heads * head_size)
    counts_rep = jnp.tile(tube_count, frames)
    fold_fn = make_fold(query_local, vis_dev, time_dev, scaling)
    state = fold_fn(
        start_state(local_heads, all_rows, head_size),
        (
            lax.all_gather(key_local, "space", axis=0, tiled=True),
            lax.all_gather(value_local, "space", axis=0, tiled=True),
            lax.all_gather(counts_rep, "space", axis=0, tiled=True),
        ),
        jnp.int32(0),
    )
    _, total_final, accum_final = state
    attended = (accum_final / total_final[..., None]).astype(jnp.bfloat16)
    attended = jnp.transpose(attended, (1, 0, 2))
    returned = lax.all_to_all(attended, "frame", split_axis=0, concat_axis=1, tiled=True)
    attended = returned.reshape(rows_dev, inner)
    mixed = flat.astype(jnp.float32) + jnp.dot(attended, w_out, preferred_element_type=jnp.float32)
    own_live = live_mask(tube_count, vis_dev, time_dev)
    mixed = jnp.where(own_live[:, None], mixed, 0.0)
    return mixed.astype(jnp.bfloat16).reshape(vis_dev, time_dev, width)


def solution(mesh):
    frames, spaces = mesh.shape["frame"], mesh.shape["space"]
    parts = (2, frames // 2, spaces // 2, 2)

    def layer(tokens, tube_count, ln_gain, ln_bias, w_qkv, w_out):
        slots = tokens.shape[0] // spaces
        time_dev = tokens.shape[1] // frames
        rows = slots * up_to(time_dev, SUBLANES)
        pairs = 2 * w_out.shape[0] == HEADS * LANES and rows % (2 * PACK) == 0
        padded = up_to(time_dev, SUBLANES) >= time_dev + MARKS
        split = parts[1] == 2 and parts[2] == 4 and spaces == HEADS
        if split and pairs and padded:
            run, over = head_per_device, Mesh(
                mesh.devices.reshape(parts), ("far", "near", "chip", "core")
            )
            frame, space = ("far", "near"), ("chip", "core")
        else:
            run, over, frame, space = on_device, mesh, "frame", "space"
        mapped = jax.shard_map(
            run,
            mesh=over,
            in_specs=(P(space, frame, None), P(space), P(), P(), P(), P()),
            out_specs=P(space, frame, None),
            check_vma=False,
        )
        return mapped(tokens, tube_count, ln_gain, ln_bias, w_qkv, w_out)

    return layer
```

```python
import functools
import jax
import jax.numpy as jnp
from jax import lax
from jax.experimental import pallas as pl
from jax.experimental.pallas import tpu as pltpu
from jax.sharding import Mesh, PartitionSpec as P

HEADS = 8


EPSILON = 1e-06
NEG_FILL = -1e30
LANES = 128
SUBLANES = 8
PACK = 16
SIZE_STEP = 128
MARKS = 2
SIZES_ABOVE = (128, 192, 320, 448)
SCORE_BOUND = 60.0
QUERY_SMALL = 128
QUERY_TILE = 256
QUERY_BIG = 512
VMEM_BYTES = 20 * 2**20

VMEM = pl.BlockSpec(memory_space=pltpu.VMEM)
SMEM = pl.BlockSpec(memory_space=pltpu.SMEM)
SWAP = [(0, 1), (1, 0)]


def up_to(value, unit):
    return -(-value // unit) * unit


def params():
    return pltpu.CompilerParams(vmem_limit_bytes=VMEM_BYTES)


def packed_rows(count, slot_rows):
    return count * slot_rows


def slot_of(row, slots, slot_rows):
    slot = row * 0
    for edge in range(1, slots):
        slot = slot + (row >= edge * slot_rows).astype(jnp.int32)
    return slot


def live_rows(count, rows, slot_rows, time_dev, width):
    row = lax.broadcasted_iota(jnp.int32, (rows, width), 0)
    slot = slot_of(row, rows // slot_rows, slot_rows)
    return (slot < count) & (row - slot * slot_rows < time_dev)


def one_hot(shape, slots, slot_rows, padded_dim):
    padded = lax.broadcasted_iota(jnp.int32, shape, padded_dim)
    plain = lax.broadcasted_iota(jnp.int32, shape, 1 - padded_dim)
    slot = slot_of(padded, slots, slot_rows)
    hot = plain == (padded - slot * slot_rows) * slots + slot
    return hot.astype(jnp.float32).astype(jnp.bfloat16)


def scalar(ref):
    return jnp.max(ref[...].astype(jnp.float32)).astype(jnp.int32)


def read(ref, row):
    return jnp.max(ref[row : row + 1])


def write(ref, row, value):
    ref[row : row + 1] = jnp.full((1, ref.shape[1]), value, ref.dtype)


def normalise(x_ref, gain_ref, bias_ref, rows):
    time_dev, slots, width = x_ref.shape
    x = x_ref[...].astype(jnp.float32).reshape(time_dev * slots, width)
    center = x - jnp.mean(x, axis=-1, keepdims=True)
    spread = jnp.mean(center * center, axis=-1, keepdims=True)
    normed = center * lax.rsqrt(spread + EPSILON) * gain_ref[...] + bias_ref[...]
    hot = one_hot((rows, time_dev * slots), slots, rows // slots, 0)
    return jnp.dot(
        hot, normed.astype(jnp.bfloat16), preferred_element_type=jnp.float32
    ).astype(jnp.bfloat16)


def fetch_kernel(
    x_hbm,
    gain_hbm,
    bias_hbm,
    w_hbm,
    rows_ref,
    gain_ref,
    bias_ref,
    w_ref,
    x_ref,
    sems,
):
    kinds, _, wide = w_ref.shape
    pairs = [(x_hbm, x_ref), (gain_hbm, gain_ref), (bias_hbm, bias_ref)]
    for kind in range(kinds):
        start = pl.multiple_of(2 * wide * kind + wide * lax.axis_index("core"), wide)
        pairs.append((w_hbm.at[:, pl.ds(start, wide)], w_ref.at[kind]))
    copies = [
        pltpu.make_async_copy(source, target, sems.at[place])
        for place, (source, target) in enumerate(pairs)
    ]
    for copy in copies:
        copy.start()
    for copy in copies[:-kinds]:
        copy.wait()
    rows_ref[...] = normalise(x_ref, gain_ref, bias_ref, rows_ref.shape[0])
    for copy in copies[-kinds:]:
        copy.wait()


def fetch(tokens, ln_gain, ln_bias, w_qkv, rows):
    width = tokens.shape[-1]
    wide = w_qkv.shape[1] // 6
    gain = ln_gain.reshape(1, width)
    bias = ln_bias.reshape(1, width)
    inputs = [pltpu.with_memory_space_constraint(a, pltpu.HBM) for a in (tokens, gain, bias, w_qkv)]
    hbm = pl.BlockSpec(memory_space=pltpu.HBM)
    return pl.pallas_call(
        fetch_kernel,
        out_shape=(
            jax.ShapeDtypeStruct((rows, width), jnp.bfloat16),
            jax.ShapeDtypeStruct(gain.shape, gain.dtype),
            jax.ShapeDtypeStruct(bias.shape, bias.dtype),
            jax.ShapeDtypeStruct((3, width, wide), w_qkv.dtype),
        ),
        in_specs=[hbm] * 4,
        out_specs=(VMEM,) * 4,
        scratch_shapes=[
            pltpu.VMEM(tokens.shape, tokens.dtype),
            pltpu.SemaphoreType.DMA((6,)),
        ],
        compiler_params=params(),
        cost_estimate=pl.CostEstimate(
            flops=2 * rows * w_qkv.size, bytes_accessed=w_qkv.size, transcendentals=0
        ),
        name="fetch",
    )(*inputs)


def project_kernel(
    count_ref,
    other_count_ref,
    rows_ref,
    other_ref,
    gain_ref,
    bias_ref,
    w_ref,
    *refs,
):
    chips = len(refs) - 3
    outs = refs[:chips]
    query_ref, key_ref, value_ref = refs[chips:]
    time_dev, slots, _ = other_ref.shape
    message, lanes = outs[0].shape
    rows = message // 3
    slot_rows = rows // slots
    half = rows // 2
    head_size = lanes // 2
    scaling = head_size ** (-0.5)
    chip = lax.axis_index("chip")
    rows_in = jnp.concatenate(
        [rows_ref[...], normalise(other_ref, gain_ref, bias_ref, rows)], axis=0
    )
    for kind, target in enumerate((query_ref, key_ref, value_ref)):
        target[...] = jnp.dot(rows_in, w_ref[kind], preferred_element_type=jnp.float32)
    left = lax.broadcasted_iota(jnp.int32, (rows, lanes), 1) < head_size
    left_half = left[:half]
    row_half = lax.broadcasted_iota(jnp.int32, (half, lanes), 0)
    counts = (scalar(count_ref), scalar(other_count_ref))
    flipped = lax.rem(chip, 2) == 1
    for slot in range(chips // 2):
        block = (slot + chip // 2) % (chips // 2) if chips == 4 else slot
        cols = pl.ds(pl.multiple_of(block * lanes, lanes), lanes)
        for group, count in enumerate(counts):
            base = group * rows
            key_pair = key_ref[base : base + rows, cols]
            value_pair = value_ref[base : base + rows, cols]
            live = live_rows(count, rows, slot_rows, time_dev, lanes)
            key_pair = jnp.where(live, key_pair, key_pair[0:1])
            value_pair = jnp.where(live, value_pair, 0.0)
            even = jnp.where(left, key_pair, pltpu.roll(value_pair, head_size, 1))
            odd = jnp.where(left, pltpu.roll(key_pair, head_size, 1), value_pair)
            first = jnp.where(flipped, odd, even).astype(jnp.bfloat16)
            second = jnp.where(flipped, even, odd).astype(jnp.bfloat16)
            outs[2 * slot][base : base + rows] = first
            outs[2 * slot + 1][base : base + rows] = second
            top = query_ref[base : base + half, cols] * scaling
            low = query_ref[base + half : base + rows, cols] * scaling
            even = jnp.where(left_half, top, pltpu.roll(low, head_size, 1))
            odd = jnp.where(left_half, pltpu.roll(top, head_size, 1), low)
            first = jnp.where(flipped, odd, even)
            second = jnp.where(flipped, even, odd)
            if group == 1:
                for index, mark in enumerate(counts):
                    here = (row_half == half - MARKS + index) & jnp.logical_not(left_half)
                    first = jnp.where(here, mark.astype(jnp.float32), first)
                    second = jnp.where(here, mark.astype(jnp.float32), second)
            place = 2 * rows + group * half
            outs[2 * slot][place : place + half] = first.astype(jnp.bfloat16)
            outs[2 * slot + 1][place : place + half] = second.astype(jnp.bfloat16)


def project(count, other_count, rows_in, other_tokens, gain, bias, weights):
    chips = HEADS // 2
    rows = rows_in.shape[0]
    wide = weights.shape[-1]
    held = pltpu.VMEM((2 * rows, wide), jnp.float32)
    message = jax.ShapeDtypeStruct((3 * rows, LANES), jnp.bfloat16)
    return pl.pallas_call(
        project_kernel,
        out_shape=(message,) * chips,
        in_specs=[VMEM] * 7,
        out_specs=(VMEM,) * chips,
        scratch_shapes=[held] * 3,
        compiler_params=params(),
        cost_estimate=pl.CostEstimate(
            flops=4 * rows * weights.size, bytes_accessed=2 * weights.size, transcendentals=0
        ),
        name="project",
    )(count, other_count, rows_in, other_tokens, gain, bias, weights)


def source_counts(ref):
    message = ref.shape[0]
    tail = ref[message - PACK : message].astype(jnp.float32)
    return [
        jnp.max(tail[PACK - MARKS + index : PACK - MARKS + index + 1, LANES // 2 :]).astype(jnp.int32)
        for index in range(MARKS)
    ]


def pack_kernel(slot_rows, time_dev, sizes, *refs):
    got_refs = refs[:-5]
    kv_room, live_room, query_ref, start_ref, case_ref = refs[-5:]
    message, lanes = got_refs[0].shape
    rows = message // 3
    half = rows // 2
    head_size = lanes // 2
    size = live_room.shape[0] - rows
    lane = lax.broadcasted_iota(jnp.int32, (PACK, lanes), 1)
    first = got_refs[0][0:PACK].astype(jnp.float32)[0:1]
    fill = jnp.where(lane < head_size, jnp.broadcast_to(first, (PACK, lanes)), 0.0)
    fill = fill.astype(jnp.bfloat16)
    blank = jnp.zeros((PACK, lanes), jnp.bfloat16)
    for start in range(0, size, PACK):
        kv_room[start : start + PACK] = fill
        live_room[start : start + PACK] = blank
    for start in range(0, query_ref.shape[0], PACK):
        query_ref[start : start + PACK] = blank
    left = lax.broadcasted_iota(jnp.int32, (half, lanes), 1) < head_size
    plain = left & (lax.broadcasted_iota(jnp.int32, (half, lanes), 0) < half - MARKS)
    start = jnp.int32(0)
    for index, ref in enumerate(got_refs):
        for group, count in enumerate(source_counts(ref)):
            write(start_ref, MARKS * index + group, start.astype(jnp.float32))
            place = pl.ds(pl.multiple_of(start, SUBLANES), rows)
            kv_room[place] = ref[group * rows : (group + 1) * rows]
            live = live_rows(count, rows, slot_rows, time_dev, lanes)
            live_room[place] = live.astype(jnp.float32).astype(jnp.bfloat16)
            base = 2 * rows + group * half
            pair = ref[base : base + half].astype(jnp.float32)
            query_ref[pl.ds(pl.multiple_of(start, SUBLANES), half)] = jnp.where(left, pair, 0.0).astype(
                jnp.bfloat16
            )
            query_ref[pl.ds(pl.multiple_of(start + half, SUBLANES), half)] = jnp.where(
                plain, pltpu.roll(pair, head_size, 1), 0.0
            ).astype(jnp.bfloat16)
            start = start + packed_rows(count, slot_rows)
    write(start_ref, MARKS * len(got_refs), start.astype(jnp.float32))
    case_ref[0] = sum((start > size).astype(jnp.int32) for size in sizes[:-1])


def pack(got, sizes, slot_rows, time_dev):
    message, lanes = got[0].shape
    rows = message // 3
    sources = MARKS * len(got)
    room = jax.ShapeDtypeStruct((sizes[-1] + rows, lanes), jnp.bfloat16)
    queries = up_to(sources * rows, QUERY_TILE) + rows
    return pl.pallas_call(
        functools.partial(pack_kernel, slot_rows, time_dev, tuple(sizes)),
        out_shape=(
            room,
            room,
            jax.ShapeDtypeStruct((queries, lanes), jnp.bfloat16),
            jax.ShapeDtypeStruct((up_to(sources + 1, SUBLANES), lanes), jnp.float32),
            jax.ShapeDtypeStruct((1,), jnp.int32),
        ),
        in_specs=[VMEM] * len(got),
        out_specs=(VMEM, VMEM, VMEM, VMEM, SMEM),
        compiler_params=params(),
        name="pack",
    )(*got)


def attend_kernel(first, last, size, lengths, *refs):
    start_ref, query_ref, live_ref = refs[:3]
    block_refs = refs[3 : 3 + len(lengths)]
    rest = list(refs[3 + len(lengths) :])
    side_ref = rest.pop()
    if not first:
        best_in, sum_in, flag_in = rest[:3]
        rest = rest[3:]
    if last:
        sum_out = rest.pop()
        out_ref = rest[0]
    else:
        best_out, sum_out, flag_out = rest
    lanes = live_ref.shape[1]
    head_size = lanes // 2
    total = read(start_ref, HEADS).astype(jnp.int32)
    blocks = []
    begin = 0
    widest = jnp.zeros((1, lanes), jnp.float32)
    for length, ref in zip(lengths, block_refs):
        left = lax.broadcasted_iota(jnp.int32, (length, lanes), 1) < head_size
        rows = slice(begin, begin + length)
        place = begin % size
        side_ref[rows] = jnp.where(left, live_ref[place : place + length], ref[0:length])
        reach = jnp.max(jnp.abs(ref[0:length].astype(jnp.float32)), axis=0, keepdims=True)
        widest = jnp.maximum(widest, reach)
        blocks.append((ref, length, rows))
        begin = begin + length
    lane = lax.broadcasted_iota(jnp.int32, (1, lanes), 1)
    keys_square = jnp.sum(jnp.where(lane < head_size, widest * widest, 0.0))
    if first:
        queries = query_ref[0 : query_ref.shape[0] // QUERY_TILE * QUERY_TILE].astype(jnp.float32)
        query_square = jnp.max(jnp.sum(queries * queries, axis=-1, keepdims=True))
        small = jnp.bool_(True)
    else:
        query_square = read(flag_in, 0)
        small = read(flag_in, 1) > 0.5
    before_small = small
    small = jnp.logical_and(small, query_square * keys_square <= SCORE_BOUND * SCORE_BOUND)
    if not last:
        write(flag_out, 0, query_square)
        write(flag_out, 1, jnp.where(small, 1.0, 0.0))

    def score(query, ref, length):
        return lax.dot_general(
            query, ref[0:length], (((1,), (1,)), ((), ())), preferred_element_type=jnp.float32
        )

    def total_of(weights):
        return sum(
            jnp.dot(weight, side_ref[rows], preferred_element_type=jnp.float32)
            for weight, (ref, length, rows) in zip(weights, blocks)
        )

    def finish(place, sums):
        if last:
            sums = sums / pltpu.roll(sums, head_size, 1)
        sum_out[place] = sums

    def unshifted(start, tile):
        place = pl.ds(pl.multiple_of(start, QUERY_TILE), tile)
        query = query_ref[place]
        sums = total_of(
            [
                jnp.exp(score(query, ref, length)).astype(jnp.bfloat16)
                for ref, length, rows in blocks
            ]
        )
        if not first:
            sums = sums + sum_in[place]
        finish(place, sums)

    def shifted(start, tile):
        place = pl.ds(pl.multiple_of(start, tile), tile)
        query = query_ref[place]
        scores = [score(query, ref, length) for ref, length, rows in blocks]
        best = functools.reduce(
            jnp.maximum, [jnp.max(part, axis=-1, keepdims=True) for part in scores]
        )
        if not first:
            before = jnp.where(before_small, 0.0, best_in[place][:, 0:1])
            best = jnp.maximum(best, before)
        sums = total_of([jnp.exp(part - best).astype(jnp.bfloat16) for part in scores])
        if not first:
            sums = sums + sum_in[place] * jnp.exp(before - best)
        if not last:
            best_out[place] = jnp.broadcast_to(best, (tile, lanes))
        finish(place, sums)

    @pl.when(small)
    def _():
        def step(index, carry):
            unshifted(index * QUERY_BIG, QUERY_BIG)
            return carry

        bigs = (total + QUERY_BIG - QUERY_TILE - 1) // QUERY_BIG
        lax.fori_loop(0, bigs, step, 0)

        @pl.when(total > bigs * QUERY_BIG)
        def _():
            unshifted(bigs * QUERY_BIG, QUERY_TILE)

    @pl.when(jnp.logical_not(small))
    def _():
        def step(index, carry):
            shifted(index * QUERY_SMALL, QUERY_SMALL)
            return carry

        lax.fori_loop(0, (total + QUERY_SMALL - 1) // QUERY_SMALL, step, 0)

    if last:
        half = out_ref.shape[1] // MARKS
        left_half = lax.broadcasted_iota(jnp.int32, (half, lanes), 1) < head_size
        for source in range(MARKS * out_ref.shape[0]):
            start = read(start_ref, source).astype(jnp.int32)
            top = sum_out[pl.ds(pl.multiple_of(start, SUBLANES), half)]
            low = sum_out[pl.ds(pl.multiple_of(start + half, SUBLANES), half)]
            base = source % MARKS * half
            out_ref[source // MARKS, base : base + half] = jnp.where(
                left_half, pltpu.roll(top, head_size, 1), low
            ).astype(jnp.bfloat16)


def run_stage(stage, stages, size, starts, query, live, blocks, lengths, state, half):
    lanes = query.shape[1]
    queries = query.shape[0]
    outs = HEADS // MARKS
    first, last = stage == 0, stage == stages - 1
    held = jax.ShapeDtypeStruct((queries, lanes), jnp.float32)
    flags = jax.ShapeDtypeStruct((SUBLANES, lanes), jnp.float32)
    keys = sum(lengths)
    scratch = [pltpu.VMEM((keys, lanes), jnp.bfloat16)]
    if last:
        out_shape = (jax.ShapeDtypeStruct((outs, MARKS * half, lanes), jnp.bfloat16),)
        out_specs = (VMEM,)
        scratch = [pltpu.VMEM((queries, lanes), jnp.float32)] + scratch
    else:
        out_shape = (held, held, flags)
        out_specs = (VMEM,) * 3
    places = 3 + len(blocks)
    return pl.pallas_call(
        functools.partial(attend_kernel, first, last, size, lengths),
        out_shape=out_shape,
        in_specs=[VMEM] * (3 + len(blocks) + len(state)),
        out_specs=out_specs,
        scratch_shapes=scratch,
        input_output_aliases={} if first or last else {places: 0, places + 1: 1},
        compiler_params=params(),
        cost_estimate=pl.CostEstimate(
            flops=4 * keys * keys * lanes, bytes_accessed=keys * lanes * 8, transcendentals=0
        ),
    )(starts, query, live, *blocks, *state)


def tie(value, *after):
    return lax.optimization_barrier((value, *after))


def attend_size(size, half, *packed):
    return exchange_and_attend(size, half, *packed)


def exchange_and_attend(size, half, kv, live, query, starts):
    late = size // 2 // SIZE_STEP * SIZE_STEP
    early = size - late
    first, second, both = tie(kv[:early], kv[early:size], kv[:size])
    far_early = lax.ppermute(first, "far", SWAP)
    far_late = lax.ppermute(second, "far", SWAP)
    near = lax.ppermute(both, "near", SWAP)
    run = lambda stage, blocks, lengths, state: run_stage(
        stage, 3, size, starts, query, live, blocks, lengths, state, half
    )
    state = run(0, (both,), (size,), ())
    far_early, *state = tie(far_early, *state)
    both_early = lax.ppermute(far_early, "near", SWAP)
    both_late = lax.ppermute(far_late, "near", SWAP)
    state = run(1, (near, far_early, far_late), (size, early, late), state)
    both_early, both_late, *state = tie(both_early, both_late, *state)
    return run(2, (both_early, both_late), (early, late), state)[0]


def mix_kernel(count_ref, got_ref, other_ref, x_ref, w_ref, out_ref, held_ref):
    chips, half, lanes = got_ref.shape
    time_dev, slots, width = x_ref.shape
    slot_rows = 2 * half // slots
    head_size = lanes // 2
    core = lax.axis_index("core")
    chip = lax.axis_index("chip")
    flipped = lax.rem(chip, 2) == 1
    left = lax.broadcasted_iota(jnp.int32, (half, lanes), 1) < head_size
    count = scalar(count_ref)
    live = live_rows(count, 2 * half, slot_rows, time_dev, lanes)
    for slot in range(chips // 2):
        block = (slot + chip // 2) % (chips // 2) if chips == 4 else slot
        for side in range(2):
            if side == 0:
                owner = core
                first = got_ref[2 * slot]
                second = got_ref[2 * slot + 1]
            else:
                owner = 1 - core
                first = other_ref[2 * slot]
                second = other_ref[2 * slot + 1]
            first = first.astype(jnp.float32)
            second = second.astype(jnp.float32)
            even = jnp.where(flipped, second, first)
            odd = jnp.where(flipped, first, second)
            top = jnp.where(left, even, pltpu.roll(odd, head_size, 1))
            low = jnp.where(left, pltpu.roll(even, head_size, 1), odd)
            pair = jnp.where(live, jnp.concatenate([top, low], axis=0), 0.0)
            place = pl.multiple_of((owner * (chips // 2) + block) * lanes, lanes)
            held_ref[:, pl.ds(place, lanes)] = pair.astype(jnp.bfloat16)
    hot = one_hot((time_dev * slots, 2 * half), slots, slot_rows, 1)
    attended = jnp.dot(hot, held_ref[...], preferred_element_type=jnp.float32).astype(jnp.bfloat16)
    mixed = jnp.dot(attended, w_ref[...], preferred_element_type=jnp.float32)
    full = x_ref[...].astype(jnp.float32) + mixed.reshape(time_dev, slots, width)
    slot = lax.broadcasted_iota(jnp.int32, full.shape, 1)
    out_ref[...] = jnp.where(slot < count, full, 0.0).astype(jnp.bfloat16)


def mix(count, got, other, tokens, w_out):
    half, _ = got.shape[1:]
    return pl.pallas_call(
        mix_kernel,
        out_shape=jax.ShapeDtypeStruct(tokens.shape, jnp.bfloat16),
        in_specs=[VMEM] * 5,
        out_specs=VMEM,
        scratch_shapes=[pltpu.VMEM((2 * half, w_out.shape[0]), jnp.bfloat16)],
        compiler_params=params(),
        cost_estimate=pl.CostEstimate(
            flops=4 * half * w_out.size, bytes_accessed=2 * w_out.size, transcendentals=0
        ),
        name="mix",
    )(count, got, other, tokens, w_out)


def spread(arrays, chips):
    out = [arrays[0]]
    for hop in range(1, chips):
        out.append(lax.ppermute(arrays[hop], "chip", [(i, i ^ hop) for i in range(chips)]))
    return out


def head_per_device(tokens, tube_count, ln_gain, ln_bias, w_qkv, w_out):
    slots, time_dev, _ = tokens.shape
    slot_rows = up_to(time_dev, SUBLANES)
    rows = slots * slot_rows
    half = rows // 2
    chips = lax.axis_size("chip")
    by_time = jnp.transpose(tokens, (1, 0, 2))
    other_tokens = lax.ppermute(by_time, "core", SWAP)
    tube_count = tube_count.reshape(1, 1)
    other_count = lax.ppermute(tube_count, "core", SWAP)
    fetched = fetch(by_time, ln_gain, ln_bias, w_qkv, rows)
    rows_in, gain, bias, weights = fetched
    messages = project(
        tube_count, other_count, rows_in, other_tokens, gain, bias, weights
    )
    got = spread(messages, chips)
    least = up_to((HEADS - 1) * slot_rows + rows, SIZE_STEP // 2)
    most = up_to((HEADS - 1) * rows + slot_rows, SIZE_STEP)
    sizes = [least + more for more in SIZES_ABOVE if least + more < most] + [most]
    kv, live, query, starts, case = pack(got, sizes, slot_rows, time_dev)
    branches = [functools.partial(attend_size, size, half) for size in sizes]
    returned = lax.switch(case[0], branches, kv, live, query, starts)
    back = jnp.stack(spread(returned, chips))
    other = lax.ppermute(back[:, half:], "core", SWAP)
    mixed = mix(tube_count, back[:, :half], other, by_time, w_out)
    return jnp.transpose(mixed, (1, 0, 2))


def layer_norm(flat, ln_gain, ln_bias):
    values32 = flat.astype(jnp.float32)
    center = values32 - jnp.mean(values32, axis=-1, keepdims=True)
    spread = jnp.mean(center * center, axis=-1, keepdims=True)
    return (center * lax.rsqrt(spread + EPSILON) * ln_gain + ln_bias).astype(jnp.bfloat16)


def live_mask(counts, slots_dev, time_dev):
    slot_ids = jnp.arange(slots_dev)[None, :, None]
    marks = jnp.broadcast_to(
        slot_ids < counts[:, None, None], (counts.shape[0], slots_dev, time_dev)
    )
    return marks.reshape(-1)


def attend(carry, query_heads, key_block, value_block, live_keys, scaling):
    best_now, total_now, accum = carry
    heads = query_heads.shape[1]
    key_heads = key_block.reshape(key_block.shape[0], heads, -1)
    value_heads = value_block.reshape(value_block.shape[0], heads, -1)
    scores = (
        jnp.einsum("qhd,khd->hqk", query_heads, key_heads, preferred_element_type=jnp.float32)
        * scaling
    )
    scores = jnp.where(live_keys[None, None, :], scores, NEG_FILL)
    best_next = jnp.maximum(best_now, jnp.max(scores, axis=-1))
    fading = jnp.exp(best_now - best_next)
    weights = jnp.exp(scores - best_next[..., None])
    total_next = total_now * fading + jnp.sum(weights, axis=-1)
    accum = accum * fading[..., None] + jnp.einsum(
        "hqk,khd->hqd",
        weights.astype(jnp.bfloat16),
        value_heads,
        preferred_element_type=jnp.float32,
    )
    return (best_next, total_next, accum)


def make_fold(query_heads, vis_dev, time_dev, scaling):
    rows_dev = vis_dev * time_dev

    def fold_masked(carry, piece, start):
        key_all, value_all, count_all = piece
        width_in = key_all.shape[1]
        shards = count_all.shape[0]
        group = 1
        for _ in range(6):
            if shards % (group * 2) == 0 and group * rows_dev < 2048:
                group = group * 2
        blocks = shards // group
        key_groups = key_all.reshape(blocks, group * rows_dev, width_in)
        value_groups = value_all.reshape(blocks, group * rows_dev, width_in)
        count_groups = count_all.reshape(blocks, group)

        def step_group(state, item):
            key_group, value_group, count_group = item
            marks = live_mask(count_group, vis_dev, time_dev)
            return (attend(state, query_heads, key_group, value_group, marks, scaling), None)

        carry, _ = lax.scan(step_group, carry, (key_groups, value_groups, count_groups))
        return carry

    return fold_masked


def start_state(heads, rows, head_size):
    return (
        jnp.full((heads, rows), NEG_FILL, jnp.float32),
        jnp.zeros((heads, rows), jnp.float32),
        jnp.zeros((heads, rows, head_size), jnp.float32),
    )


def on_device(tokens, tube_count, ln_gain, ln_bias, w_qkv, w_out):
    vis_dev, time_dev, width = tokens.shape
    rows_dev = vis_dev * time_dev
    inner = w_out.shape[0]
    head_size = inner // HEADS
    flat = tokens.reshape(rows_dev, width)
    normed = layer_norm(flat, ln_gain, ln_bias)
    projected = jnp.dot(normed, w_qkv, preferred_element_type=jnp.float32).astype(jnp.bfloat16)
    scaling = head_size ** (-0.5)
    frames = lax.axis_size("frame")
    local_heads = HEADS // frames
    stacked = projected.reshape(rows_dev, 3, HEADS, head_size)
    regrouped = lax.all_to_all(stacked, "frame", split_axis=2, concat_axis=0, tiled=True)
    all_rows = regrouped.shape[0]
    query_local = regrouped[:, 0]
    key_local = regrouped[:, 1].reshape(all_rows, local_heads * head_size)
    value_local = regrouped[:, 2].reshape(all_rows, local_heads * head_size)
    counts_rep = jnp.tile(tube_count, frames)
    fold_fn = make_fold(query_local, vis_dev, time_dev, scaling)
    state = fold_fn(
        start_state(local_heads, all_rows, head_size),
        (
            lax.all_gather(key_local, "space", axis=0, tiled=True),
            lax.all_gather(value_local, "space", axis=0, tiled=True),
            lax.all_gather(counts_rep, "space", axis=0, tiled=True),
        ),
        jnp.int32(0),
    )
    _, total_final, accum_final = state
    attended = (accum_final / total_final[..., None]).astype(jnp.bfloat16)
    attended = jnp.transpose(attended, (1, 0, 2))
    returned = lax.all_to_all(attended, "frame", split_axis=0, concat_axis=1, tiled=True)
    attended = returned.reshape(rows_dev, inner)
    mixed = flat.astype(jnp.float32) + jnp.dot(attended, w_out, preferred_element_type=jnp.float32)
    own_live = live_mask(tube_count, vis_dev, time_dev)
    mixed = jnp.where(own_live[:, None], mixed, 0.0)
    return mixed.astype(jnp.bfloat16).reshape(vis_dev, time_dev, width)


def solution(mesh):
    frames, spaces = mesh.shape["frame"], mesh.shape["space"]
    parts = (2, frames // 2, spaces // 2, 2)

    def layer(tokens, tube_count, ln_gain, ln_bias, w_qkv, w_out):
        slots = tokens.shape[0] // spaces
        time_dev = tokens.shape[1] // frames
        rows = slots * up_to(time_dev, SUBLANES)
        pairs = 2 * w_out.shape[0] == HEADS * LANES and rows % (2 * PACK) == 0
        padded = up_to(time_dev, SUBLANES) >= time_dev + MARKS
        split = parts[1] == 2 and parts[2] == 4 and spaces == HEADS
        if split and pairs and padded:
            run, over = head_per_device, Mesh(
                mesh.devices.reshape(parts), ("far", "near", "chip", "core")
            )
            frame, space = ("far", "near"), ("chip", "core")
        else:
            run, over, frame, space = on_device, mesh, "frame", "space"
        mapped = jax.shard_map(
            run,
            mesh=over,
            in_specs=(P(space, frame, None), P(space), P(), P(), P(), P()),
            out_specs=P(space, frame, None),
            check_vma=False,
        )
        return mapped(tokens, tube_count, ln_gain, ln_bias, w_qkv, w_out)

    return layer
```
